32 devices in a mesh: gx: 4 (over y, x), gy: 8 (over z, core).
Axes of the slice: x: 2, y: 2, z: 4, core: 2. Of those that a mesh axis runs over, the one named last changes fastest.
Arguments:
- primal: float32 [4, 27, 16384], P(None, None, ('gx', 'gy')), may hold values from -6 to 6
- adjoint: float32 [4, 27, 16384], P(None, None, ('gx', 'gy')), may hold values from -6 to 6
- source: float32 [4, 27, 16384], P(None, None, ('gx', 'gy')), may hold values from -6 to 6
- coefficient: float32 [16384], P(('gx', 'gy')), may hold values from 0.3 to 3
- levels: int32 [16384], P(('gx', 'gy')), may hold values from 0 to 3
- recon: float32 [7, 125, 27], replicated, may hold values from -0.4375 to 0.4375
- stiffness: float32 [125, 27], replicated, may hold values from -1.25 to 1.25
- interp: float32 [125, 27], replicated, may hold values from -1.25 to 1.25
- flux: float32 [6, 25, 27], replicated, may hold values from -1.25 to 1.25
- face_eval: float32 [6, 25, 125], replicated, may hold values from -0.5 to 0.5
- child_interp: float32 [4, 25, 25], replicated, may hold values from -1.25 to 1.25
- ghost_send: int32 [32, 8, 32], P(('gx', 'gy')), may hold values from -1 to 511, as said below
- edge_send: int32 [32, 2, 16], P(('gx', 'gy')), may hold values from -1 to 511, as said below
- neighbor_slot: int32 [6, 16384], P(None, ('gx', 'gy')), may hold values from -1 to 799, as said below
- neighbor_child: int32 [6, 16384], P(None, ('gx', 'gy')), may hold values from 0 to 4, as said below
- hang_send: int32 [2, 32, 8, 8], P(None, ('gx', 'gy')), may hold values from -1 to 511, as said below
- hang_recv: int32 [3, 32, 8, 8], P(None, ('gx', 'gy')), may hold values from -1 to 511, as said below
Outputs:
- cell_indicator: float32 [4, 16384], P(None, ('gx', 'gy'))
- face_indicator: float32 [4, 16384], P(None, ('gx', 'gy'))
The draws below stay inside these ranges and needn't reach their ends.
Inputs may be any that keep to these rules, and one draw needn't show every extreme that they name: `ghost_send`: the gy index of a device numbers a block of a cube of blocks with side S, the cube root of 8: index = G(c0) + S * G(c1) + S * S * G(c2) for block coordinates c0, c1, c2, where G(p) = p xor (p // 2) is the Gray code, so face-adjacent blocks differ in one bit of the index. Row [r, p] lists the local cells that device r sends to the device with its gx index and gy index p, live ids first, then -1. Only the up to six blocks face-adjacent to r's block get live ids, between 16 and 32 of them, and exactly 32 go to the neighbour one step up along coordinate 0 wherever it exists. `edge_send`: row [r, 0] lists the local cells sent to the device one gx index lower with the same gy index, row [r, 1] those sent to the one higher, live ids first, then -1; where that device exists there are 8 to 16 live ids, and exactly 16 towards the lower one; otherwise the row is all -1. `neighbor_slot`: every slot that is not -1 points at a live entry: a cell of the device itself, a live entry of a gy peer's ghost_send row for this device, or a live entry of a gx neighbour's edge_send row towards this device. `neighbor_child`: 4 means a neighbour of the same level. `hang_send`: [0, r, p, t] is a local cell of device r and [1, r, p, t] one of its faces, both -1 after the live slots; live slots go only to face-adjacent gy peers (as for ghost_send), at most 8 to one peer, and the device with gy index 0 sends exactly 8 to each of its face-adjacent peers. `hang_recv`: [:, q, p, t] describes what device q receives in slot t from the device with its gx index and gy index p: a local coarse cell, its face (the opposite of the sender's fine face) and a child position 0 to 3; all three are -1 exactly where the sender's slot is empty.
All inputs are finite; a program needn't handle non-finite values.
Results may differ from the reference program's by a relative error of at most 0.0003.
Values sent between devices are 32-bit elements; how exact they have to be, the bound alone decides.
A program may use at most 128 MiB of HBM per device.

```python
import math
import jax
import jax.numpy as jnp
from jax import lax

F = 4
DOFS = 27
QUADS = 125
FACEPTS = 25
CELL_DEV = 512
GSLOT = 32
XSLOT = 16
HSLOT = 8
CELLS = 16384
N_GY = 8
DEVICES = 32


def gray_encode(position):
    return jnp.bitwise_xor(position, position >> 1)


def gray_decode(code, side_log):
    position = code
    for shift_by in range(1, max(side_log, 1)):
        position = jnp.bitwise_xor(position, code >> shift_by)
    return position


def block_table():
    side_log = (N_GY.bit_length() - 1) // 3
    length = 1 << side_log
    own_rows = jnp.arange(N_GY, dtype=jnp.int32)
    coords = [gray_decode(own_rows >> side_log * axis_dim & length - 1, side_log) for axis_dim in range(3)]
    columns = []
    for axis_dim in range(3):
        for direction in (1, -1):
            moved = [coords[other] + (direction if other == axis_dim else 0) for other in range(3)]
            inside = (moved[axis_dim] >= 0) & (moved[axis_dim] < length)
            block_index = jnp.zeros((N_GY,), jnp.int32)
            for other in range(3):
                block_index = block_index + (gray_encode(moved[other] & length - 1) << side_log * other)
            columns.append(jnp.where(inside, block_index, -1))
    return jnp.stack(columns, 1)


def mesh_layout(key):
    segments = DEVICES // N_GY
    table = block_table()
    device = jnp.arange(DEVICES, dtype=jnp.int32)
    own_row = device % N_GY
    segment = device // N_GY
    peer_rows = jnp.arange(N_GY, dtype=jnp.int32)
    row_table = table[own_row]
    near = jnp.any(row_table[:, :, None] == peer_rows[None, None, :], axis=1)
    full = row_table[:, 0:1] == peer_rows[None, :]
    count = jax.random.randint(jax.random.fold_in(key, 11), (DEVICES, N_GY), GSLOT // 2, GSLOT + 1)
    count = jnp.where(full, GSLOT, count)
    count = jnp.where(near, count, 0)
    ghost_ids = jax.random.randint(jax.random.fold_in(key, 12), (DEVICES, N_GY, GSLOT), 0, CELL_DEV)
    ghost = jnp.where(jnp.arange(GSLOT)[None, None, :] < count[:, :, None], ghost_ids, -1)
    has_side = jnp.stack([segment > 0, segment < segments - 1], 1)
    edge_count = jax.random.randint(jax.random.fold_in(key, 13), (DEVICES, 2), XSLOT // 2, XSLOT + 1)
    edge_count = jnp.where(jnp.arange(2)[None, :] == 0, XSLOT, edge_count)
    edge_count = jnp.where(has_side, edge_count, 0)
    edge_ids = jax.random.randint(jax.random.fold_in(key, 14), (DEVICES, 2, XSLOT), 0, CELL_DEV)
    edge = jnp.where(jnp.arange(XSLOT)[None, None, :] < edge_count[:, :, None], edge_ids, -1)
    shape = (DEVICES, 6, CELL_DEV)
    kind_draw = jax.random.randint(jax.random.fold_in(key, 15), shape, 0, 20)
    local_cell = jax.random.randint(jax.random.fold_in(key, 16), shape, 0, CELL_DEV)
    direction = jax.random.randint(jax.random.fold_in(key, 17), shape, 0, 6)
    row_wide = jnp.broadcast_to(own_row[:, None, None], shape)
    first_peer = table[row_wide, direction]
    other_peer = table[row_wide, jnp.bitwise_xor(direction, 1)]
    source_row = jnp.where(first_peer >= 0, first_peer, other_peer)
    sender = segment[:, None, None] * N_GY + source_row
    live_count = jnp.maximum(count[sender, row_wide], 1)
    draw_bits = jax.random.randint(jax.random.fold_in(key, 18), shape, 0, 1 << 20)
    via_segment = CELL_DEV + source_row * GSLOT + draw_bits % live_count
    side_draw = jax.random.randint(jax.random.fold_in(key, 19), shape, 0, 2)
    low_ok = (segment > 0)[:, None, None]
    high_ok = (segment < segments - 1)[:, None, None]
    side_pick = jnp.where(side_draw == 0, jnp.where(low_ok, 0, 1), jnp.where(high_ok, 1, 0))
    side_ok = jnp.where(side_pick == 0, low_ok, high_ok)
    edge_sender = jnp.clip(device[:, None, None] + (2 * side_pick - 1) * N_GY, 0, DEVICES - 1)
    edge_live = jnp.maximum(edge_count[edge_sender, 1 - side_pick], 1)
    via_edges = CELL_DEV + N_GY * GSLOT + side_pick * XSLOT + draw_bits % edge_live
    chosen = jnp.where(kind_draw < 10, local_cell, jnp.where(kind_draw < 17, via_segment, jnp.where((kind_draw < 19) & side_ok, via_edges, -1)))
    neighbours = jnp.transpose(chosen, (1, 0, 2)).reshape(6, DEVICES * CELL_DEV)
    heavy = (jax.random.randint(jax.random.fold_in(key, 20), (DEVICES,), 0, 4) == 0) | (own_row == 0)
    light = jax.random.randint(jax.random.fold_in(key, 21), (DEVICES, N_GY), 0, HSLOT // 2 + 1)
    hang_count = jnp.where(heavy[:, None], HSLOT, light)
    hang_count = jnp.where(near, hang_count, 0)
    hang_live = jnp.arange(HSLOT)[None, None, :] < hang_count[:, :, None]
    hang_shape = (DEVICES, N_GY, HSLOT)
    fine_cell = jax.random.randint(jax.random.fold_in(key, 22), hang_shape, 0, CELL_DEV)
    fine_face = jax.random.randint(jax.random.fold_in(key, 23), hang_shape, 0, 6)
    coarse_cell = jax.random.randint(jax.random.fold_in(key, 24), hang_shape, 0, CELL_DEV)
    child_pos = jax.random.randint(jax.random.fold_in(key, 25), hang_shape, 0, 4)

    def turned(values):
        masked = jnp.where(hang_live, values, -1)
        return masked.reshape(segments, N_GY, N_GY, HSLOT).transpose(0, 2, 1, 3).reshape(DEVICES, N_GY, HSLOT)
    sent = jnp.stack([jnp.where(hang_live, fine_cell, -1), jnp.where(hang_live, fine_face, -1)])
    received = jnp.stack([turned(coarse_cell), turned(jnp.bitwise_xor(fine_face, 1)), turned(child_pos)])
    return (ghost, edge, neighbours, sent, received)


def draw_ghost_send(key, part):
    return mesh_layout(key)[0].astype(jnp.int32)


def draw_edge_send(key, part):
    return mesh_layout(key)[1].astype(jnp.int32)


def draw_neighbor_slot(key, part):
    return mesh_layout(key)[2].astype(jnp.int32)


def draw_hang_send(key, part):
    return mesh_layout(key)[3].astype(jnp.int32)


def draw_hang_recv(key, part):
    return mesh_layout(key)[4].astype(jnp.int32)


def draw_neighbor_child(key, part):
    child_draw = jax.random.randint(jax.random.fold_in(key, 31), (6, CELLS), 0, 20)
    return jnp.where(child_draw < 16, 4, child_draw - 16).astype(jnp.int32)


def touch_ends(entries, stream_key, least, top_value):
    spot = [jax.random.randint(jax.random.fold_in(stream_key, axis), (), 0, length) for axis, length in enumerate(entries.shape)]
    longest = entries.shape.index(max(entries.shape))
    beside = spot[:longest] + [(spot[longest] + 1) % entries.shape[longest]] + spot[longest + 1:]
    return entries.at[tuple(spot)].set(least).at[tuple(beside)].set(top_value)


def block_levels(key, dims, shards, smallest, high):
    def one(dim, parts):
        heights = jax.random.uniform(jax.random.fold_in(jax.random.fold_in(key, 6), dim), (parts,), jnp.float32, smallest / len(shards), high / len(shards))
        return jnp.repeat(jnp.exp(heights), dims[dim] // parts).reshape((-1,) + (1,) * (len(dims) - dim - 1))

    gain = one(*shards[0])
    for cut in shards[1:]:
        gain = gain * one(*cut)
    return gain


def noise(own_key, dims, spread, limit, split=(), kind=jnp.bfloat16):
    values = spread * jax.random.normal(own_key, dims, jnp.float32)
    if split:
        values = values * block_levels(own_key, dims, split, -0.22, 0.18)
    return jnp.clip(values, -limit, limit).astype(kind)


def setup_inputs(seed: int = 0) -> dict:
    arg_keys = jax.random.split(jax.random.key(seed), 18)
    primal = noise(arg_keys[0], (F, DOFS, CELLS), 1.0, 6.0, ((2, 32),), jnp.float32)
    adjoint = noise(arg_keys[1], (F, DOFS, CELLS), 1.0, 6.0, ((2, 32),), jnp.float32)
    source = noise(arg_keys[2], (F, DOFS, CELLS), 1.0, 6.0, ((2, 32),), jnp.float32)
    coefficient = jnp.clip(jnp.exp(math.log(3.0) - 2.3025851 * jax.random.uniform(arg_keys[3], (CELLS,), jnp.float32) ** block_levels(arg_keys[3], (CELLS,), ((0, 32),), -0.2, 0.2)), 0.3, 3.0)
    levels = touch_ends(jax.random.randint(arg_keys[4], (CELLS,), 0, 4), jax.random.fold_in(arg_keys[4], 1), 0, 3).astype(jnp.int32)
    recon = noise(arg_keys[5], (7, QUADS, DOFS), (7 * DOFS) ** -0.5, 0.4375, (), jnp.float32)
    stiffness = noise(arg_keys[6], (QUADS, DOFS), DOFS ** -0.5, 1.25, (), jnp.float32)
    interp = noise(arg_keys[7], (QUADS, DOFS), DOFS ** -0.5, 1.25, (), jnp.float32)
    flux = noise(arg_keys[8], (6, FACEPTS, DOFS), DOFS ** -0.5, 1.25, (), jnp.float32)
    face_eval = noise(arg_keys[9], (6, FACEPTS, QUADS), QUADS ** -0.5, 0.5, (), jnp.float32)
    child_interp = noise(arg_keys[10], (4, FACEPTS, FACEPTS), FACEPTS ** -0.5, 1.25, (), jnp.float32)
    ghost_send = draw_ghost_send(jax.random.fold_in(arg_keys[17], 71), 0)
    edge_send = draw_edge_send(jax.random.fold_in(arg_keys[17], 71), 0)
    neighbor_slot = draw_neighbor_slot(jax.random.fold_in(arg_keys[17], 71), 0)
    neighbor_child = draw_neighbor_child(jax.random.fold_in(arg_keys[17], 71), 0)
    hang_send = draw_hang_send(jax.random.fold_in(arg_keys[17], 71), 0)
    hang_recv = draw_hang_recv(jax.random.fold_in(arg_keys[17], 71), 0)
    return dict(primal=primal, adjoint=adjoint, source=source, coefficient=coefficient, levels=levels, recon=recon, stiffness=stiffness, interp=interp, flux=flux, face_eval=face_eval, child_interp=child_interp, ghost_send=ghost_send, edge_send=edge_send, neighbor_slot=neighbor_slot, neighbor_child=neighbor_child, hang_send=hang_send, hang_recv=hang_recv)


PRECISE = lax.Precision.HIGHEST
OPPOSITE = (1, 0, 3, 2, 5, 4)

def collect(blocks, cell_ids):
    safe_cells = jnp.maximum(cell_ids, 0)
    taken = jnp.take(blocks, safe_cells.reshape(-1), axis=2)
    taken = taken.reshape(blocks.shape[:2] + cell_ids.shape)
    return jnp.where(cell_ids >= 0, taken, 0.0)

def face_traces(flux, primal, cell_ids, face_ids):
    fine_u = collect(primal, cell_ids)
    flat_u = fine_u.reshape(fine_u.shape[0], fine_u.shape[1], -1)
    flat_faces = face_ids.reshape(-1)
    chosen = jnp.zeros((flat_u.shape[0], flux.shape[1], flat_u.shape[2]), jnp.float32)
    for face_idx in range(6):
        term = jnp.einsum('pj,kjs->kps', flux[face_idx], flat_u, precision=PRECISE)
        chosen = chosen + jnp.where(flat_faces == face_idx, term, 0.0)
    return chosen.reshape(chosen.shape[:2] + cell_ids.shape)

def take_back(face_total, traces_in, recv_maps, face_weight, child_interp):
    flat_trace = traces_in.reshape(traces_in.shape[0], traces_in.shape[1], -1)
    coarse = recv_maps[0].reshape(-1)
    coarse_face = recv_maps[1].reshape(-1)
    child_pos = recv_maps[2].reshape(-1)
    lifted = jnp.zeros_like(flat_trace)
    for position in range(4):
        term = jnp.einsum('qp,kqs->kps', child_interp[position], flat_trace, precision=PRECISE)
        lifted = lifted + jnp.where(child_pos == position, term, 0.0)
    target = jnp.maximum(coarse, 0)
    chosen = jnp.zeros_like(flat_trace)
    for face_idx in range(6):
        chosen = chosen + jnp.where(coarse_face == face_idx, jnp.take(face_weight[face_idx], target, axis=2), 0.0)
    contrib = jnp.where(coarse >= 0, lax.optimization_barrier(jnp.sum(lifted * chosen, axis=1)), 0.0)
    return face_total.at[:, target].add(contrib)

def local_terms(primal, adjoint, source, coefficient, recon, stiffness, interp, flux, face_eval, child_interp, primal_near, adjoint_near, buffer_slots, neighbor_child):
    is_live = buffer_slots >= 0
    safe_cells = jnp.maximum(buffer_slots, 0)
    weight = jnp.einsum('qj,kjc->kqc', recon[0], adjoint, precision=PRECISE)
    for face_idx in range(6):
        near_z = jnp.where(is_live[face_idx], jnp.take(adjoint_near, safe_cells[face_idx], axis=2), 0.0)
        weight = weight + jnp.einsum('qj,kjc->kqc', recon[face_idx + 1], near_z, precision=PRECISE)
    residual_q = jnp.einsum('qj,kjc->kqc', interp, source, precision=PRECISE) - coefficient * jnp.einsum('qj,kjc->kqc', stiffness, primal, precision=PRECISE)
    cell_part = lax.optimization_barrier(jnp.sum(residual_q * weight, axis=1))
    face_weight = jnp.einsum('fpq,kqc->fkpc', face_eval, weight, precision=PRECISE)
    face_total = jnp.zeros(cell_part.shape, jnp.float32)
    for face_idx in range(6):
        near_u = jnp.where(is_live[face_idx], jnp.take(primal_near, safe_cells[face_idx], axis=2), 0.0)
        outer_trace = jnp.einsum('pj,kjc->kpc', flux[OPPOSITE[face_idx]], near_u, precision=PRECISE)
        child_here = neighbor_child[face_idx]
        mapped = jnp.where(child_here == 4, outer_trace, 0.0)
        for position in range(4):
            term = jnp.einsum('pq,kqc->kpc', child_interp[position], outer_trace, precision=PRECISE)
            mapped = mapped + jnp.where(child_here == position, term, 0.0)
        inner_trace = jnp.einsum('pj,kjc->kpc', flux[face_idx], primal, precision=PRECISE)
        face_total = face_total + lax.optimization_barrier(jnp.sum((inner_trace + mapped) * face_weight[face_idx], axis=1))
    return (cell_part, face_total, face_weight)

def finish(cell_part, face_total, levels, quad_count, point_count):
    cell_size = jnp.exp2(-levels.astype(jnp.float32))
    return (cell_size * cell_part / math.sqrt(quad_count), cell_size * face_total / math.sqrt(6 * point_count))

def reference(primal, adjoint, source, coefficient, levels, recon, stiffness, interp, flux, face_eval, child_interp, ghost_send, edge_send, neighbor_slot, neighbor_child, hang_send, hang_recv):
    fields = primal.shape[0]

    def device(device_id):
        own_row = device_id % N_GY
        segment = device_id // N_GY
        first_cell = (device_id * CELL_DEV).astype(jnp.int32)
        own_u = lax.dynamic_slice_in_dim(primal, first_cell, CELL_DEV, 2)
        own_z = lax.dynamic_slice_in_dim(adjoint, first_cell, CELL_DEV, 2)
        own_src = lax.dynamic_slice_in_dim(source, first_cell, CELL_DEV, 2)
        coeff_cells = lax.dynamic_slice_in_dim(coefficient, first_cell, CELL_DEV, 0)
        level_cells = lax.dynamic_slice_in_dim(levels, first_cell, CELL_DEV, 0)
        slot_rows = lax.dynamic_slice_in_dim(neighbor_slot, first_cell, CELL_DEV, 1)
        child_rows = lax.dynamic_slice_in_dim(neighbor_child, first_cell, CELL_DEV, 1)
        shifted = slot_rows - CELL_DEV
        source_peer = jnp.clip(shifted // GSLOT, 0, N_GY - 1)
        ghost_pos = jnp.clip(shifted - source_peer * GSLOT, 0, GSLOT - 1)
        sender = segment * N_GY + source_peer
        via_segment = sender * CELL_DEV + ghost_send[sender, own_row, ghost_pos]
        edge_rel = shifted - N_GY * GSLOT
        side_pick = jnp.clip(edge_rel // XSLOT, 0, 1)
        edge_pos = jnp.clip(edge_rel - side_pick * XSLOT, 0, XSLOT - 1)
        edge_sender = jnp.clip(device_id + (2 * side_pick - 1) * N_GY, 0, DEVICES - 1)
        via_edges = edge_sender * CELL_DEV + edge_send[edge_sender, 1 - side_pick, edge_pos]
        global_ids = jnp.where(slot_rows < 0, -1, jnp.where(slot_rows < CELL_DEV, first_cell + slot_rows, jnp.where(shifted < N_GY * GSLOT, via_segment, via_edges)))
        global_ids = global_ids.astype(jnp.int32)
        cell_part, face_total, face_weight = local_terms(own_u, own_z, own_src, coeff_cells, recon, stiffness, interp, flux, face_eval, child_interp, primal, adjoint, global_ids, child_rows)
        senders = segment * N_GY + jnp.arange(N_GY, dtype=jnp.int32)
        fine_cell = hang_send[0][senders, own_row]
        fine_face = hang_send[1][senders, own_row]
        fine_ids = jnp.where(fine_cell >= 0, senders[:, None] * CELL_DEV + fine_cell, -1).astype(jnp.int32)
        traces_in = face_traces(flux, primal, fine_ids, fine_face)
        recv_maps = hang_recv[:, device_id]
        face_total = take_back(face_total, traces_in, recv_maps, face_weight, child_interp)
        return finish(cell_part, face_total, level_cells, recon.shape[1], flux.shape[1])
    cell_parts, face_parts = lax.map(device, jnp.arange(DEVICES, dtype=jnp.int32))
    cell_indicator = jnp.transpose(cell_parts, (1, 0, 2)).reshape(fields, DEVICES * CELL_DEV)
    face_indicator = jnp.transpose(face_parts, (1, 0, 2)).reshape(fields, DEVICES * CELL_DEV)
    return (cell_indicator, face_indicator)
```

```python
import functools
import math

import jax
import jax.numpy as jnp
from jax import lax
from jax.experimental import pallas as pl
from jax.experimental.pallas import tpu as pltpu
from jax.sharding import PartitionSpec as P

LANES = 128
F32 = jnp.float32
BF16 = jnp.bfloat16
MESH = pl.DeviceIdType.MESH


def round_up(value, unit):
    return -(-value // unit) * unit


def split(x):
    hi = x.astype(BF16)
    lo = (x - hi.astype(F32)).astype(BF16)
    return hi, lo


def both(x):
    return jnp.concatenate(split(x), 0)


def mm(a, b):
    return jnp.dot(a, b, preferred_element_type=F32)


def mm_nt(a, b):
    return lax.dot_general(a, b, (((1,), (1,)), ((), ())), preferred_element_type=F32)


def dot3(a_both, b_hi, b_lo, dot=mm):
    rows = a_both.shape[0] // 2
    first = dot(a_both, b_hi)
    return first[:rows] + first[rows:] + dot(a_both[:rows], b_lo)


def fill_flat(flat, refs, width):
    for at, ref in enumerate(refs):
        dofs, fields, cells = ref.shape
        used = dofs * fields
        for i in range(cells // LANES):
            for j in range(dofs):
                row = at * width + j * fields
                flat[i, row : row + fields, :] = ref[j, :, i * LANES : (i + 1) * LANES]
            flat[i, at * width + used : (at + 1) * width, :] = jnp.zeros((width - used, LANES), F32)


def lane_gather(blocks, lane, block_id):
    total = jnp.zeros(blocks[0].shape, F32)
    for i, block in enumerate(blocks):
        got = jnp.take_along_axis(block, lane, axis=1)
        total = jnp.where(block_id == i, got, total)
    return total


def one_hot(index, rows):
    parts = []
    for first in range(0, rows, 256):
        count = min(256, rows - first)
        wide = jnp.broadcast_to((index - first).astype(F32), (count, index.shape[1])).astype(BF16)
        ids = lax.broadcasted_iota(jnp.int32, wide.shape, 0).astype(F32).astype(BF16)
        parts.append(jnp.where(wide == ids, jnp.ones_like(wide), jnp.zeros_like(wide)))
    return parts[0] if len(parts) == 1 else jnp.concatenate(parts, 0)


def compute_kernel(dims, n_args, *refs):
    n_gx, n_gy, bits, ghosts, edges, hangs, fields, rows, hang_rows, chunk_lanes = dims
    hbm = refs[:n_args]
    out_ref = refs[n_args]
    local = refs[n_args + 1 : 2 * n_args + 1]
    (
        op_recon,
        op_left,
        op_flux_rows,
        op_child,
        child_flat,
        op_flux,
        op_rep,
        op_z,
        op_u,
        op_trace,
        op_back,
        maps,
        z_hi,
        z_lo,
        u_all,
        sources,
        flat,
        source_flat,
        hang_flat,
        near,
        hot,
        scatter,
        part_z,
        from_gy,
        from_gx,
        to_gy,
        to_gx,
        ids,
        packed,
        in_sems,
        send_gy,
        recv_gy,
        send_gx,
        recv_gx,
    ) = refs[2 * n_args + 1 :]
    (
        primal_ref,
        adjoint_ref,
        source_ref,
        coef_ref,
        levels_ref,
        recon_ref,
        stiffness_ref,
        interp_ref,
        flux_ref,
        face_eval_ref,
        child_interp_ref,
        slot_ref,
        child_ref,
        hang_ref,
        ghost_ref,
        edge_ref,
        hang_send_ref,
    ) = local
    gx = lax.axis_index("gx")
    gy = lax.axis_index("gy")
    dofs, _, cells = primal_ref.shape
    width = fields * rows
    wide = 2 * width
    partners = [jnp.bitwise_xor(gy, 1 << b) for b in range(bits)]

    order = [14, 15, 16, 0, 1, 11, 5, 6, 7, 8, 9, 10, 13, 12, 3, 4, 2]
    loads = [pltpu.make_async_copy(hbm[i], local[i], in_sems.at[i]) for i in range(n_args)]
    for i in order[:5]:
        loads[i].start()

    barrier = pltpu.get_barrier_semaphore()
    for partner in partners:
        pl.semaphore_signal(barrier, inc=1, device_id=(gx, partner), device_id_type=MESH)

    @pl.when(gx > 0)
    def _():
        pl.semaphore_signal(barrier, inc=1, device_id=(gx - 1, gy), device_id_type=MESH)

    @pl.when(gx < n_gx - 1)
    def _():
        pl.semaphore_signal(barrier, inc=1, device_id=(gx + 1, gy), device_id_type=MESH)

    for i in order[5:]:
        loads[i].start()
    for i in order[:5]:
        loads[i].wait()

    main = bits * ghosts + 2 * edges
    main_pad = round_up(main, LANES)
    hang_pad = round_up(bits * hangs, LANES)
    ids[...] = jnp.zeros_like(ids)
    for b, partner in enumerate(partners):
        ids[0:1, b * ghosts : (b + 1) * ghosts] = ghost_ref[0, pl.ds(partner, 1), :]
        at = main_pad + b * hangs
        ids[0:1, at : at + hangs] = hang_send_ref[0, 0, pl.ds(partner, 1), :]
    for side in range(2):
        at = bits * ghosts + side * edges
        ids[0:1, at : at + edges] = edge_ref[0, side : side + 1, :]
    fill_flat(flat, (primal_ref, adjoint_ref), width)
    chosen = jnp.maximum(ids[0:1, :], 0)
    for at in range(0, main_pad + hang_pad, LANES):
        part = jnp.broadcast_to(chosen[:, at : at + LANES], (rows, LANES))
        lane = jnp.bitwise_and(part, LANES - 1)
        block_id = jnp.right_shift(part, 7)
        count = 2 * fields if at < main_pad else fields
        for group in range(count):
            blocks = [flat[i, group * rows : (group + 1) * rows, :] for i in range(cells // LANES)]
            packed[group * rows : (group + 1) * rows, :] = lane_gather(blocks, lane, block_id)
        if at < main_pad:
            turned = packed[...].T
            for first in range(at, min(at + LANES, main), edges):
                chunk = turned[first - at : first - at + edges]
                if first < bits * ghosts:
                    inner = first % ghosts
                    to_gy[first // ghosts, inner : inner + edges, :] = chunk
                else:
                    to_gx[(first - bits * ghosts) // edges] = chunk
        else:
            turned = packed[0:width, :].T
            for b in range(bits):
                at_slot = b * hangs - (at - main_pad)
                if 0 <= at_slot < LANES:
                    to_gy[b, ghosts : ghosts + hangs, 0:width] = turned[at_slot : at_slot + hangs]
                    to_gy[b, ghosts : ghosts + hangs, width:] = jnp.zeros(
                        (hangs, to_gy.shape[2] - width), F32
                    )

    def low_copy():
        return pltpu.make_async_remote_copy(
            src_ref=to_gx.at[0],
            dst_ref=from_gx.at[1],
            send_sem=send_gx.at[0],
            recv_sem=recv_gx.at[1],
            device_id=(gx - 1, gy),
            device_id_type=MESH,
        )

    def high_copy():
        return pltpu.make_async_remote_copy(
            src_ref=to_gx.at[1],
            dst_ref=from_gx.at[0],
            send_sem=send_gx.at[1],
            recv_sem=recv_gx.at[0],
            device_id=(gx + 1, gy),
            device_id_type=MESH,
        )

    @pl.when((gx > 0) & (gx < n_gx - 1))
    def _():
        pl.semaphore_wait(barrier, bits + 2)

    @pl.when((gx == 0) | (gx == n_gx - 1))
    def _():
        pl.semaphore_wait(barrier, bits + (1 if n_gx > 1 else 0))

    copies = []
    for b in reversed(range(bits)):
        copy = pltpu.make_async_remote_copy(
            src_ref=to_gy.at[b],
            dst_ref=from_gy.at[b],
            send_sem=send_gy.at[b],
            recv_sem=recv_gy.at[b],
            device_id=(gx, partners[b]),
            device_id_type=MESH,
        )
        copy.start()
        copies.append(copy)

    @pl.when(gx > 0)
    def _():
        low_copy().start()

    @pl.when(gx == 0)
    def _():
        from_gx[0] = jnp.zeros(from_gx.shape[1:], F32)

    @pl.when(gx < n_gx - 1)
    def _():
        high_copy().start()

    @pl.when(gx == n_gx - 1)
    def _():
        from_gx[1] = jnp.zeros(from_gx.shape[1:], F32)

    quads = recon_ref.shape[2]
    own_blocks = cells // LANES
    points = flux_ref.shape[1]
    remote = bits * ghosts + 2 * edges
    remote_pad = round_up(remote, LANES)
    hang_count = bits * hangs
    children = 4

    for i in order[5:]:
        loads[i].wait()

    for i in range(own_blocks):
        for group in range(2 * fields):
            first = group // fields * width + group % fields
            sources[group * rows : (group + 1) * rows, i * LANES : (i + 1) * LANES] = flat[
                i, pl.ds(first, rows, stride=fields), :
            ]
    own_both = both(sources[...])
    slot = slot_ref[...]
    shifted = slot - cells
    log_ghosts = ghosts.bit_length() - 1
    peer = jnp.right_shift(shifted, log_ghosts)
    within = jnp.bitwise_and(shifted, ghosts - 1)
    differing = jnp.bitwise_xor(peer, gy)
    place_of = jnp.zeros_like(slot)
    for b in range(1, bits):
        place_of = jnp.where(differing == (1 << b), b, place_of)
    far = jnp.where(
        shifted < n_gy * ghosts, place_of * ghosts + within, shifted - (n_gy - bits) * ghosts
    )
    far = jnp.where(shifted < 0, -1, far)
    for f in range(6):
        for at in range(0, cells, chunk_lanes):
            cols = slice(at, at + chunk_lanes)
            got = mm(own_both, one_hot(slot[f : f + 1, cols], cells))
            near[f, :, cols] = got[:wide] + got[wide:]
    for f in range(6):
        for at in range(0, cells, chunk_lanes):
            cols = slice(at, at + chunk_lanes)
            hot_part = one_hot(far[f : f + 1, cols], remote_pad)
            hot[f, 0:remote_pad, cols] = hot_part
            hot[f, remote_pad : 2 * remote_pad, cols] = hot_part

    op_recon[...] = jnp.zeros_like(op_recon)
    op_left[...] = jnp.zeros_like(op_left)
    op_flux_rows[...] = jnp.zeros_like(op_flux_rows)
    child_flat[...] = jnp.zeros_like(child_flat)
    op_flux[...] = jnp.zeros_like(op_flux)
    for j in range(dofs):
        op_recon[8 * j : 8 * j + 7, 0:quads] = recon_ref[j]
    op_left[0:dofs, 0:quads] = interp_ref[...]
    op_left[rows : rows + dofs, 0:quads] = stiffness_ref[...]
    for f in range(6):
        at = (3 + f) * rows
        op_left[at : at + points, 0:quads] = face_eval_ref[f]
        op_flux_rows[f * rows : f * rows + points, 0:dofs] = flux_ref[f]
        op_flux[0:points, f * rows : f * rows + dofs] = flux_ref[f]
    for p in range(points):
        child_flat[children * p : children * (p + 1), 0:points] = child_interp_ref[p]
    for h in range(children):
        op_child[h * rows : (h + 1) * rows, :] = child_flat[pl.ds(h, rows, stride=children), :]
    flux_turned = op_flux_rows[...].T[0:rows]
    face_eval = op_left[3 * rows : 9 * rows, :]
    op_left[2 * rows : 3 * rows, :] = dot3(both(flux_turned), *split(face_eval))
    recon_turned = jnp.concatenate([op_recon[pl.ds(f, rows, stride=8), :] for f in range(7)], 0)
    op_z[...] = both(dot3(both(op_left[...]), *split(recon_turned), dot=mm_nt))
    for f in range(6):
        single = op_flux_rows[f * rows : (f + 1) * rows, :]
        thrice = single + pltpu.roll(single, rows, 1) + pltpu.roll(single, 2 * rows, 1)
        op_rep[:, (f ^ 1) * LANES : ((f ^ 1) + 1) * LANES] = thrice
    child_both = both(op_child[...])
    mapped_ops = dot3(child_both[:, 0:rows], *split(op_rep[...]))
    high_lanes = lax.broadcasted_iota(jnp.int32, (5 * rows, LANES), 1) < 2 * rows
    for f in range(6):
        cols = slice(f * LANES, (f + 1) * LANES)
        maps_f = jnp.concatenate([mapped_ops[:, cols], op_rep[:, cols]], 0)
        hi, lo = split(maps_f)
        op_u[f] = jnp.where(high_lanes, hi.astype(F32), lo.astype(F32)).astype(BF16)
    op_trace[...] = both(op_flux[...])
    op_back[...] = both(op_child[...].T[0:rows])

    maps[...] = jnp.full(maps.shape, -1, jnp.int32)
    for b in range(bits):
        partner = jnp.bitwise_xor(gy, 1 << b)
        for i in range(3):
            maps[i : i + 1, b * hangs : (b + 1) * hangs] = hang_ref[i, 0, pl.ds(partner, 1), :]
    live = maps[0:1, :] >= 0
    place = jnp.where(live, maps[0:1, :] + maps[1:2, :] * cells, -1).astype(F32)
    place_rows = jnp.broadcast_to(place, (LANES, hang_pad)).T[0:hang_rows, 0:1]
    column = lax.broadcasted_iota(jnp.int32, (hang_rows, cells), 1).astype(F32)
    place_wide = jnp.broadcast_to(place_rows, (hang_rows, cells))
    for f in range(6):
        hit = jnp.where(place_wide == column + float(f * cells), 1.0, 0.0).astype(BF16)
        scatter[f, 0:hang_rows] = hit
        scatter[f, hang_rows : 2 * hang_rows] = hit

    def spread(x):
        outs = []
        for first in range(0, fields * hang_rows, LANES):
            total = None
            for k in range(fields):
                at = k * hang_rows - first
                if 0 <= at < LANES:
                    piece = x[k][:, 0:LANES]
                    piece = pltpu.roll(piece, at, 1) if at else piece
                    total = piece if total is None else total + piece
            outs.append(total)
        return outs[0] if len(outs) == 1 else jnp.concatenate(outs, 1)

    maps_all = spread([maps[...] + 1] * fields) - 1
    hang_lanes = fields * hang_rows
    face_wide = jnp.broadcast_to(maps_all[1:2, :], (rows, hang_lanes))
    child_wide = jnp.broadcast_to(maps_all[2:3, :], (rows, hang_lanes))
    hang_zero = jnp.zeros((rows, hang_lanes), BF16)

    fill_flat(source_flat, (source_ref,), width)
    for k in range(fields):
        own_hi, own_lo = split(sources[(fields + k) * rows : (fields + k + 1) * rows, :])
        z_hi[k, 0:rows, :] = own_hi
        z_lo[k, 0:rows, :] = own_lo
    coef = coef_ref[...]
    size = jnp.exp2(-levels_ref[...].astype(F32))

    for copy in copies:
        copy.wait()

    @pl.when(gx > 0)
    def _():
        low_copy().wait_send()
        high_copy().wait_recv()

    @pl.when(gx < n_gx - 1)
    def _():
        high_copy().wait_send()
        low_copy().wait_recv()

    parts = [from_gy[b, 0:ghosts, :] for b in range(bits)] + [from_gx[0], from_gx[1]]
    if remote_pad > remote:
        parts.append(jnp.zeros((remote_pad - remote, parts[0].shape[1]), F32))
    arrived = jnp.concatenate(parts, 0).T
    blocks = []
    for i in range(remote_pad // LANES):
        flat[i] = arrived[:, i * LANES : (i + 1) * LANES]
        blocks.append(
            jnp.concatenate(
                [
                    flat[i, pl.ds(group // fields * width + group % fields, rows, stride=fields), :]
                    for group in range(2 * fields)
                ],
                0,
            )
        )
    halves = [split(block) for block in blocks]
    far_both = jnp.concatenate([h[0] for h in halves] + [h[1] for h in halves], 1)

    parts = [from_gy[b, ghosts : ghosts + hangs, 0:width] for b in range(bits)]
    parts.append(jnp.zeros((hang_pad - hang_count, width), F32))
    hang_flat[...] = jnp.concatenate(parts, 0).T
    live_lanes = lax.broadcasted_iota(jnp.int32, (rows, LANES), 1) < hang_rows
    hang_all = spread([hang_flat[pl.ds(k, rows, stride=fields), :] for k in range(fields)])
    hang_hi, hang_lo = [
        jnp.concatenate([jnp.where(face_wide == (f ^ 1), x, hang_zero) for f in range(6)], 0)
        for x in split(hang_all)
    ]
    trace_parts = split(dot3(op_trace[:, 0 : 6 * rows], hang_hi, hang_lo))
    trace_hi, trace_lo = [
        jnp.concatenate([jnp.where(child_wide == h, x, hang_zero) for h in range(children)], 0)
        for x in trace_parts
    ]
    lifted = dot3(op_back[...], trace_hi, trace_lo)
    lifts = []
    for k in range(fields):
        at = k * hang_rows
        block = lifted[:, at // LANES * LANES : at // LANES * LANES + LANES]
        if at % LANES:
            block = pltpu.roll(block, LANES - at % LANES, 1)
        hi, lo = split(jnp.where(live_lanes, block, 0.0))
        if 2 * hang_rows <= LANES:
            lo = pltpu.roll(lo.astype(F32), hang_rows, 1)
            lifts.append((hi.astype(F32) + lo).astype(BF16)[:, 0 : 2 * hang_rows])
        else:
            lifts.append(jnp.concatenate([hi, lo], 1))
    lift = jnp.concatenate(lifts, 0)

    for at in range(0, cells, chunk_lanes):
        cols = slice(at, at + chunk_lanes)
        for f in range(6):
            total = near[f, :, cols] + mm(far_both, hot[f, :, cols])
            hi, lo = split(total)
            for k in range(fields):
                u_rows = slice(k * rows, (k + 1) * rows)
                z_rows = slice((fields + k) * rows, (fields + k + 1) * rows)
                u_all[k, f, 0:rows, cols] = hi[u_rows]
                u_all[k, f, rows : 2 * rows, cols] = lo[u_rows]
                u_all[k, f, 2 * rows : 3 * rows, cols] = hi[u_rows]
                z_hi[k, (1 + f) * rows : (2 + f) * rows, cols] = hi[z_rows]
                z_lo[k, (1 + f) * rows : (2 + f) * rows, cols] = lo[z_rows]
        totals = []
        for k in range(fields):
            forms = dot3(op_z[...], z_hi[k, :, cols], z_lo[k, :, cols])
            own_u = sources[k * rows : (k + 1) * rows, cols]
            src = jnp.concatenate(
                [
                    source_flat[i, pl.ds(k, rows, stride=fields), :]
                    for i in range(at // LANES, (at + chunk_lanes) // LANES)
                ],
                1,
            )
            cell_part = src * forms[0:rows] - coef[:, cols] * own_u * forms[rows : 2 * rows]
            cell_sum = jnp.sum(cell_part, axis=0, keepdims=True)
            out_ref[k : k + 1, cols] = size[:, cols] * cell_sum * (1.0 / math.sqrt(quads))
            part_z[k] = forms[3 * rows :]
            totals.append(own_u * forms[2 * rows : 3 * rows])
        for f in range(6):
            child = jnp.broadcast_to(child_ref[f : f + 1, cols], (rows, chunk_lanes))
            masks = [child == h for h in range(children)]
            returned = mm(lift, scatter[f, :, cols])
            for k in range(fields):
                jumps = mm(op_u[f, :, 0 : 3 * rows], u_all[k, f, :, cols])
                jump = jumps[children * rows :]
                for h in range(children):
                    jump = jnp.where(masks[h], jumps[h * rows : (h + 1) * rows], jump)
                jump = jump + returned[k * rows : (k + 1) * rows]
                totals[k] = totals[k] + jump * part_z[k, f * rows : (f + 1) * rows]
        for k in range(fields):
            face_sum = jnp.sum(totals[k], axis=0, keepdims=True)
            row = fields + k
            out_ref[row : row + 1, cols] = size[:, cols] * face_sum * (1.0 / math.sqrt(6 * points))


def solution(mesh):
    n_gx, n_gy = mesh.shape["gx"], mesh.shape["gy"]
    bits = n_gy.bit_length() - 1

    def shards(
        primal,
        adjoint,
        source,
        coefficient,
        levels,
        recon,
        stiffness,
        interp,
        flux,
        face_eval,
        child_interp,
        ghost_send,
        edge_send,
        neighbor_slot,
        neighbor_child,
        hang_send,
        hang_recv,
    ):
        fields, dofs, cells = primal.shape
        ghosts, edges, hangs = ghost_send.shape[2], edge_send.shape[2], hang_send.shape[3]
        rows = round_up(dofs, 32)
        quads = recon.shape[1]
        quad_rows = round_up(quads, LANES)
        hang_rows = max(32, 1 << (bits * hangs - 1).bit_length())
        chunk = min(cells, 256)
        dims = (n_gx, n_gy, bits, ghosts, edges, hangs, fields, rows, hang_rows, chunk)
        primal, adjoint, source = [x.transpose(1, 0, 2) for x in (primal, adjoint, source)]
        main_pad = round_up(bits * ghosts + 2 * edges, LANES)
        hang_pad = round_up(bits * hangs, LANES)
        wide = 2 * fields * rows
        args = (
            primal,
            adjoint,
            source,
            coefficient.reshape(1, cells),
            levels.reshape(1, cells),
            recon.transpose(2, 0, 1),
            stiffness.T,
            interp.T,
            flux,
            face_eval,
            child_interp.transpose(1, 0, 2),
            neighbor_slot,
            neighbor_child,
            hang_recv,
            ghost_send,
            edge_send,
            hang_send,
        )
        raw = pl.pallas_call(
            functools.partial(compute_kernel, dims, len(args)),
            out_shape=pltpu.VMEM((2 * fields, cells), F32),
            in_specs=[pl.BlockSpec(memory_space=pltpu.MemorySpace.HBM)] * len(args),
            out_specs=pl.BlockSpec(memory_space=pltpu.VMEM),
            scratch_shapes=[pltpu.VMEM(x.shape, x.dtype) for x in args]
            + [
                pltpu.VMEM((8 * rows, quad_rows), F32),
                pltpu.VMEM((9 * rows, quad_rows), F32),
                pltpu.VMEM((6 * rows, LANES), F32),
                pltpu.VMEM((4 * rows, LANES), F32),
                pltpu.VMEM((4 * rows, LANES), F32),
                pltpu.VMEM((rows, round_up(6 * rows, LANES)), F32),
                pltpu.VMEM((rows, 6 * LANES), F32),
                pltpu.VMEM((18 * rows, 7 * rows), BF16),
                pltpu.VMEM((6, 5 * rows, LANES), BF16),
                pltpu.VMEM((2 * rows, round_up(6 * rows, LANES)), BF16),
                pltpu.VMEM((2 * rows, 4 * rows), BF16),
                pltpu.VMEM((8, hang_pad), jnp.int32),
                pltpu.VMEM((fields, 7 * rows, cells), BF16),
                pltpu.VMEM((fields, 7 * rows, cells), BF16),
                pltpu.VMEM((fields, 6, 3 * rows, cells), BF16),
                pltpu.VMEM((wide, cells), F32),
                pltpu.VMEM((max(cells, main_pad) // LANES, wide, LANES), F32),
                pltpu.VMEM((cells // LANES, fields * rows, LANES), F32),
                pltpu.VMEM((fields * rows, hang_pad), F32),
                pltpu.VMEM((6, wide, cells), F32),
                pltpu.VMEM((6, 2 * main_pad, cells), BF16),
                pltpu.VMEM((6, 2 * hang_rows, cells), BF16),
                pltpu.VMEM((fields, 6 * rows, chunk), F32),
                pltpu.VMEM((bits, ghosts + hangs, wide), F32),
                pltpu.VMEM((2, edges, wide), F32),
                pltpu.VMEM((bits, ghosts + hangs, wide), F32),
                pltpu.VMEM((2, edges, wide), F32),
                pltpu.VMEM((8, main_pad + hang_pad), jnp.int32),
                pltpu.VMEM((wide, LANES), F32),
                pltpu.SemaphoreType.DMA((len(args),)),
                pltpu.SemaphoreType.DMA((bits,)),
                pltpu.SemaphoreType.DMA((bits,)),
                pltpu.SemaphoreType.DMA((2,)),
                pltpu.SemaphoreType.DMA((2,)),
            ],
            compiler_params=pltpu.CompilerParams(collective_id=0, has_side_effects=True),
            name="indicators",
        )(*args)
        return raw[:fields], raw[fields:]

    split_all = ("gx", "gy")
    placed = (
        P(None, None, split_all),
        P(None, None, split_all),
        P(None, None, split_all),
        P(split_all),
        P(split_all),
        P(),
        P(),
        P(),
        P(),
        P(),
        P(),
        P(split_all, None, None),
        P(split_all, None, None),
        P(None, split_all),
        P(None, split_all),
        P(None, split_all, None, None),
        P(None, split_all, None, None),
    )
    return jax.shard_map(
        shards,
        mesh=mesh,
        in_specs=placed,
        out_specs=(P(None, split_all), P(None, split_all)),
        check_vma=False,
    )
```

```python
import functools
import math

import jax
import jax.numpy as jnp
from jax import lax
from jax.experimental import pallas as pl
from jax.experimental.pallas import tpu as pltpu
from jax.sharding import PartitionSpec as P

LANES = 128
F32 = jnp.float32
BF16 = jnp.bfloat16
MESH = pl.DeviceIdType.MESH
DOT_FACES = 4
FAR_DOT_FACES = 3


def round_up(value, unit):
    return -(-value // unit) * unit


def split(x):
    hi = x.astype(BF16)
    lo = (x - hi.astype(F32)).astype(BF16)
    return hi, lo


def both(x):
    return jnp.concatenate(split(x), 0)


def mm(a, b):
    return jnp.dot(a, b, preferred_element_type=F32)


def mm_nt(a, b):
    return lax.dot_general(a, b, (((1,), (1,)), ((), ())), preferred_element_type=F32)


def dot3(a_both, b_hi, b_lo, dot=mm):
    rows = a_both.shape[0] // 2
    first = dot(a_both, b_hi)
    return first[:rows] + first[rows:] + dot(a_both[:rows], b_lo)


def fill_flat(flat, refs, width):
    for at, ref in enumerate(refs):
        dofs, fields, cells = ref.shape
        used = dofs * fields
        for i in range(cells // LANES):
            for j in range(dofs):
                row = at * width + j * fields
                flat[i, row : row + fields, :] = ref[j, :, i * LANES : (i + 1) * LANES]
            flat[i, at * width + used : (at + 1) * width, :] = jnp.zeros((width - used, LANES), F32)


def lane_gather(blocks, lane, block_id):
    total = jnp.zeros(blocks[0].shape, F32)
    for i, block in enumerate(blocks):
        got = jnp.take_along_axis(block, lane, axis=1)
        total = jnp.where(block_id == i, got, total)
    return total


def one_hot(index, rows):
    parts = []
    for first in range(0, rows, 256):
        count = min(256, rows - first)
        wide = jnp.broadcast_to((index - first).astype(F32), (count, index.shape[1])).astype(BF16)
        ids = lax.broadcasted_iota(jnp.int32, wide.shape, 0).astype(F32).astype(BF16)
        parts.append(jnp.where(wide == ids, jnp.ones_like(wide), jnp.zeros_like(wide)))
    return parts[0] if len(parts) == 1 else jnp.concatenate(parts, 0)


def compute_kernel(dims, n_args, *refs):
    n_gx, n_gy, bits, ghosts, edges, hangs, fields, rows, hang_rows, chunk_lanes = dims
    hbm = refs[:n_args]
    out_ref = refs[n_args]
    local = refs[n_args + 1 : 2 * n_args + 1]
    (
        op_recon,
        op_left,
        op_flux_rows,
        op_face_rows,
        op_child,
        op_child_tight,
        child_flat,
        op_flux,
        op_rep,
        op_z,
        op_u,
        op_trace,
        op_back,
        maps,
        z_hi,
        z_lo,
        u_all,
        sources,
        flat,
        source_flat,
        hang_flat,
        near,
        hot,
        scatter,
        part_z,
        part_x,
        from_gy_u,
        from_gx_u,
        from_gy_z,
        from_gx_z,
        to_gy_u,
        to_gx_u,
        to_gy_z,
        to_gx_z,
        ids,
        packed,
        in_sems,
        send_gy,
        recv_gy,
        send_gx,
        recv_gx,
    ) = refs[2 * n_args + 1 :]
    (
        primal_ref,
        adjoint_ref,
        source_ref,
        coef_ref,
        levels_ref,
        recon_ref,
        stiffness_ref,
        interp_ref,
        flux_ref,
        face_eval_ref,
        child_interp_ref,
        slot_ref,
        child_ref,
        hang_ref,
        ghost_ref,
        edge_ref,
        hang_send_ref,
    ) = local
    gx = lax.axis_index("gx")
    gy = lax.axis_index("gy")
    dofs, _, cells = primal_ref.shape
    width = fields * rows
    wide = 2 * width
    partners = [jnp.bitwise_xor(gy, 1 << b) for b in range(bits)]

    order = [14, 15, 16, 0, 1, 11, 5, 6, 7, 8, 9, 10, 13, 12, 3, 4, 2]
    loads = [pltpu.make_async_copy(hbm[i], local[i], in_sems.at[i]) for i in range(n_args)]
    for i in order[:5]:
        loads[i].start()

    barrier = pltpu.get_barrier_semaphore()
    for partner in partners:
        pl.semaphore_signal(barrier, inc=1, device_id=(gx, partner), device_id_type=MESH)

    @pl.when(gx > 0)
    def _():
        pl.semaphore_signal(barrier, inc=1, device_id=(gx - 1, gy), device_id_type=MESH)

    @pl.when(gx < n_gx - 1)
    def _():
        pl.semaphore_signal(barrier, inc=1, device_id=(gx + 1, gy), device_id_type=MESH)

    for i in order[5:]:
        loads[i].start()
    for i in order[:5]:
        loads[i].wait()

    main = bits * ghosts + 2 * edges
    main_pad = round_up(main, LANES)
    hang_pad = round_up(bits * hangs, LANES)
    ids[...] = jnp.zeros_like(ids)
    for b, partner in enumerate(partners):
        ids[0:1, b * ghosts : (b + 1) * ghosts] = ghost_ref[0, pl.ds(partner, 1), :]
        at = main_pad + b * hangs
        ids[0:1, at : at + hangs] = hang_send_ref[0, 0, pl.ds(partner, 1), :]
    for side in range(2):
        at = bits * ghosts + side * edges
        ids[0:1, at : at + edges] = edge_ref[0, side : side + 1, :]
    fill_flat(flat, (primal_ref, adjoint_ref), width)
    chosen = jnp.maximum(ids[0:1, :], 0)
    for at in range(0, main_pad + hang_pad, LANES):
        part = jnp.broadcast_to(chosen[:, at : at + LANES], (rows, LANES))
        lane = jnp.bitwise_and(part, LANES - 1)
        block_id = jnp.right_shift(part, 7)
        count = 2 * fields if at < main_pad else fields
        for group in range(count):
            blocks = [flat[i, group * rows : (group + 1) * rows, :] for i in range(cells // LANES)]
            packed[group * rows : (group + 1) * rows, :] = lane_gather(blocks, lane, block_id)
        if at < main_pad:
            turned = packed[...].T
            for first in range(at, min(at + LANES, main), edges):
                chunk = turned[first - at : first - at + edges]
                if first < bits * ghosts:
                    span = slice(first % ghosts, first % ghosts + edges)
                    to_gy_u[first // ghosts, span, :] = chunk[:, 0:width]
                    to_gy_z[first // ghosts, span, :] = chunk[:, width:]
                else:
                    side = (first - bits * ghosts) // edges
                    to_gx_u[side] = chunk[:, 0:width]
                    to_gx_z[side] = chunk[:, width:]
        else:
            turned = packed[0:width, :].T
            for b in range(bits):
                at_slot = b * hangs - (at - main_pad)
                if 0 <= at_slot < LANES:
                    to_gy_u[b, ghosts : ghosts + hangs, :] = turned[at_slot : at_slot + hangs]

    stages = [(to_gy_z, from_gy_z, to_gx_z, from_gx_z), (to_gy_u, from_gy_u, to_gx_u, from_gx_u)]

    def low_copy(stage):
        _, _, src, dst = stages[stage]
        return pltpu.make_async_remote_copy(
            src_ref=src.at[0],
            dst_ref=dst.at[1],
            send_sem=send_gx.at[stage, 0],
            recv_sem=recv_gx.at[stage, 1],
            device_id=(gx - 1, gy),
            device_id_type=MESH,
        )

    def high_copy(stage):
        _, _, src, dst = stages[stage]
        return pltpu.make_async_remote_copy(
            src_ref=src.at[1],
            dst_ref=dst.at[0],
            send_sem=send_gx.at[stage, 1],
            recv_sem=recv_gx.at[stage, 0],
            device_id=(gx + 1, gy),
            device_id_type=MESH,
        )

    @pl.when((gx > 0) & (gx < n_gx - 1))
    def _():
        pl.semaphore_wait(barrier, bits + 2)

    @pl.when((gx == 0) | (gx == n_gx - 1))
    def _():
        pl.semaphore_wait(barrier, bits + (1 if n_gx > 1 else 0))

    copies = []
    for stage in range(2):
        src, dst, _, far_gx = stages[stage]
        copies.append([])
        for b in reversed(range(bits)):
            copy = pltpu.make_async_remote_copy(
                src_ref=src.at[b],
                dst_ref=dst.at[b],
                send_sem=send_gy.at[stage, b],
                recv_sem=recv_gy.at[stage, b],
                device_id=(gx, partners[b]),
                device_id_type=MESH,
            )
            copy.start()
            copies[stage].append(copy)

        @pl.when(gx > 0)
        def _():
            low_copy(stage).start()

        @pl.when(gx == 0)
        def _():
            far_gx[0] = jnp.zeros(far_gx.shape[1:], F32)

        @pl.when(gx < n_gx - 1)
        def _():
            high_copy(stage).start()

        @pl.when(gx == n_gx - 1)
        def _():
            far_gx[1] = jnp.zeros(far_gx.shape[1:], F32)

    def receive(stage):
        for copy in copies[stage]:
            copy.wait()

        @pl.when(gx > 0)
        def _():
            low_copy(stage).wait_send()
            high_copy(stage).wait_recv()

        @pl.when(gx < n_gx - 1)
        def _():
            high_copy(stage).wait_send()
            low_copy(stage).wait_recv()

    quads = recon_ref.shape[2]
    own_blocks = cells // LANES
    points = flux_ref.shape[1]
    remote = bits * ghosts + 2 * edges
    remote_pad = round_up(remote, LANES)
    hang_count = bits * hangs
    children = 4
    tight = points // 8 * 8
    tails = points - tight
    form_rows = op_z.shape[0] // 2
    tail_at = 5 * tight

    for i in order[5:]:
        loads[i].wait()

    for i in range(own_blocks):
        for group in range(2 * fields):
            first = group // fields * width + group % fields
            sources[group * rows : (group + 1) * rows, i * LANES : (i + 1) * LANES] = flat[
                i, pl.ds(first, rows, stride=fields), :
            ]
    own_both = both(sources[...])
    slot = slot_ref[...]
    shifted = slot - cells
    log_ghosts = ghosts.bit_length() - 1
    peer = jnp.right_shift(shifted, log_ghosts)
    within = jnp.bitwise_and(shifted, ghosts - 1)
    differing = jnp.bitwise_xor(peer, gy)
    place_of = jnp.zeros_like(slot)
    for b in range(1, bits):
        place_of = jnp.where(differing == (1 << b), b, place_of)
    far = jnp.where(
        shifted < n_gy * ghosts, place_of * ghosts + within, shifted - (n_gy - bits) * ghosts
    )
    far = jnp.where(shifted < 0, -1, far)
    for f in range(DOT_FACES):
        for at in range(0, cells, chunk_lanes):
            cols = slice(at, at + chunk_lanes)
            got = mm(own_both, one_hot(slot[f : f + 1, cols], cells))
            near[f, :, cols] = got[:wide] + got[wide:]
    for f in range(DOT_FACES, 6):
        for at in range(0, cells, LANES):
            cols = slice(at, at + LANES)
            part = jnp.broadcast_to(slot[f : f + 1, cols], (rows, LANES))
            lane = jnp.bitwise_and(part, LANES - 1)
            block_id = jnp.right_shift(part, 7)
            for group in range(2 * fields):
                span = slice(group * rows, (group + 1) * rows)
                blocks = [sources[span, i * LANES : (i + 1) * LANES] for i in range(own_blocks)]
                near[f, span, cols] = lane_gather(blocks, lane, block_id)
    for f in range(FAR_DOT_FACES):
        for at in range(0, cells, chunk_lanes):
            cols = slice(at, at + chunk_lanes)
            hot_part = one_hot(far[f : f + 1, cols], remote_pad)
            hot[f, 0:remote_pad, cols] = hot_part
            hot[f, remote_pad : 2 * remote_pad, cols] = hot_part

    op_recon[...] = jnp.zeros_like(op_recon)
    op_left[...] = jnp.zeros_like(op_left)
    op_flux_rows[...] = jnp.zeros_like(op_flux_rows)
    op_face_rows[...] = jnp.zeros_like(op_face_rows)
    op_child_tight[...] = jnp.zeros_like(op_child_tight)
    child_flat[...] = jnp.zeros_like(child_flat)
    op_flux[...] = jnp.zeros_like(op_flux)
    for j in range(dofs):
        op_recon[8 * j : 8 * j + 7, 0:quads] = recon_ref[j]
    op_left[0:dofs, 0:quads] = interp_ref[...]
    op_left[rows : rows + dofs, 0:quads] = stiffness_ref[...]
    for f in range(6):
        at = 3 * rows + f * tight
        op_left[at : at + tight, 0:quads] = face_eval_ref[f, 0:tight, :]
        for e in range(points - tight):
            at = 3 * rows + 6 * tight + 8 * e + f
            op_left[at : at + 1, 0:quads] = face_eval_ref[f, tight + e : tight + e + 1, :]
        op_face_rows[f * rows : f * rows + points, 0:quads] = face_eval_ref[f]
        op_flux_rows[f * rows : f * rows + points, 0:dofs] = flux_ref[f]
        op_flux[0:points, f * rows : f * rows + dofs] = flux_ref[f]
    for p in range(points):
        child_flat[children * p : children * (p + 1), 0:points] = child_interp_ref[p]
    for h in range(children):
        op_child[h * rows : (h + 1) * rows, :] = child_flat[pl.ds(h, rows, stride=children), :]
    flux_turned = op_flux_rows[...].T[0:rows]
    op_left[2 * rows : 3 * rows, :] = dot3(both(flux_turned), *split(op_face_rows[...]))
    recon_turned = jnp.concatenate([op_recon[pl.ds(f, rows, stride=8), :] for f in range(7)], 0)
    op_z[...] = both(dot3(both(op_left[...]), *split(recon_turned), dot=mm_nt))
    for f in range(6):
        single = op_flux_rows[f * rows : (f + 1) * rows, :]
        thrice = single + pltpu.roll(single, rows, 1) + pltpu.roll(single, 2 * rows, 1)
        op_rep[:, (f ^ 1) * LANES : ((f ^ 1) + 1) * LANES] = thrice
    for h in range(children):
        op_child_tight[h * tight : (h + 1) * tight, :] = op_child[h * rows : h * rows + tight, :]
        for e in range(tails):
            at = tail_at + 8 * e + h
            op_child_tight[at : at + 1, :] = op_child[h * rows + tight + e : h * rows + tight + e + 1, :]
    same = (tight, LANES)
    op_child_tight[children * tight : 5 * tight, :] = jnp.where(
        lax.broadcasted_iota(jnp.int32, same, 0) == lax.broadcasted_iota(jnp.int32, same, 1), 1.0, 0.0
    )
    for e in range(tails):
        at = tail_at + 8 * e + children
        op_child_tight[at : at + 1, :] = jnp.where(
            lax.broadcasted_iota(jnp.int32, (1, LANES), 1) == tight + e, 1.0, 0.0
        )
    mapped_ops = dot3(both(op_child_tight[...])[:, 0:rows], *split(op_rep[...]))
    high_lanes = lax.broadcasted_iota(jnp.int32, (op_u.shape[1], LANES), 1) < 2 * rows
    for f in range(6):
        hi, lo = split(mapped_ops[:, f * LANES : (f + 1) * LANES])
        op_u[f] = jnp.where(high_lanes, hi.astype(F32), lo.astype(F32)).astype(BF16)
    op_trace[...] = both(op_flux[...])
    op_back[...] = both(op_child[...].T[0:rows])

    maps[...] = jnp.full(maps.shape, -1, jnp.int32)
    for b in range(bits):
        partner = jnp.bitwise_xor(gy, 1 << b)
        for i in range(3):
            maps[i : i + 1, b * hangs : (b + 1) * hangs] = hang_ref[i, 0, pl.ds(partner, 1), :]
    live = maps[0:1, :] >= 0
    place = jnp.where(live, maps[0:1, :] + maps[1:2, :] * cells, -1).astype(F32)
    place_rows = jnp.broadcast_to(place, (LANES, hang_pad)).T[0:hang_rows, 0:1]
    column = lax.broadcasted_iota(jnp.int32, (hang_rows, cells), 1).astype(F32)
    place_wide = jnp.broadcast_to(place_rows, (hang_rows, cells))
    for f in range(6):
        hit = jnp.where(place_wide == column + float(f * cells), 1.0, 0.0).astype(BF16)
        scatter[f, 0:hang_rows] = hit
        scatter[f, hang_rows : 2 * hang_rows] = hit

    def spread(x):
        outs = []
        for first in range(0, fields * hang_rows, LANES):
            total = None
            for k in range(fields):
                at = k * hang_rows - first
                if 0 <= at < LANES:
                    piece = x[k][:, 0:LANES]
                    piece = pltpu.roll(piece, at, 1) if at else piece
                    total = piece if total is None else total + piece
            outs.append(total)
        return outs[0] if len(outs) == 1 else jnp.concatenate(outs, 1)

    maps_all = spread([maps[...] + 1] * fields) - 1
    hang_lanes = fields * hang_rows
    face_wide = jnp.broadcast_to(maps_all[1:2, :], (rows, hang_lanes))
    child_wide = jnp.broadcast_to(maps_all[2:3, :], (rows, hang_lanes))
    hang_zero = jnp.zeros((rows, hang_lanes), BF16)

    fill_flat(source_flat, (source_ref,), width)
    for k in range(fields):
        own_hi, own_lo = split(sources[(fields + k) * rows : (fields + k + 1) * rows, :])
        z_hi[k, 0:rows, :] = own_hi
        z_lo[k, 0:rows, :] = own_lo
    coef = coef_ref[...]
    size = jnp.exp2(-levels_ref[...].astype(F32))

    far_lane = jnp.bitwise_and(far, LANES - 1)
    far_block = jnp.right_shift(far, 7)

    def turn(from_gy, from_gx):
        parts = [from_gy[b, 0:ghosts, :] for b in range(bits)] + [from_gx[0], from_gx[1]]
        if remote_pad > remote:
            parts.append(jnp.zeros((remote_pad - remote, width), F32))
        arrived = jnp.concatenate(parts, 0).T
        blocks = []
        for i in range(remote_pad // LANES):
            flat[i, 0:width, :] = arrived[:, i * LANES : (i + 1) * LANES]
            blocks.append(
                jnp.concatenate(
                    [flat[i, pl.ds(k, rows, stride=fields), :] for k in range(fields)], 0
                )
            )
        return blocks

    def far_gather(blocks, base, f, at):
        cols = slice(at, at + LANES)
        lane = jnp.broadcast_to(far_lane[f : f + 1, cols], (rows, LANES))
        block_id = jnp.broadcast_to(far_block[f : f + 1, cols], (rows, LANES))
        outs = []
        for k in range(fields):
            span = slice(base + k * rows, base + (k + 1) * rows)
            total = near[f, span, cols]
            for i, block in enumerate(blocks):
                got = jnp.take_along_axis(block[k * rows : (k + 1) * rows], lane, axis=1)
                total = jnp.where(block_id == i, got, total)
            outs.append(total)
        return jnp.concatenate(outs, 0)

    def put_z(f, cols, total):
        hi, lo = split(total)
        for k in range(fields):
            span = slice(k * rows, (k + 1) * rows)
            z_hi[k, (1 + f) * rows : (2 + f) * rows, cols] = hi[span]
            z_lo[k, (1 + f) * rows : (2 + f) * rows, cols] = lo[span]

    receive(0)
    blocks_z = turn(from_gy_z, from_gx_z)
    halves = [split(block) for block in blocks_z]
    far_both = jnp.concatenate([h[0] for h in halves] + [h[1] for h in halves], 1)
    for f in range(FAR_DOT_FACES):
        for at in range(0, cells, chunk_lanes):
            cols = slice(at, at + chunk_lanes)
            put_z(f, cols, near[f, width:, cols] + mm(far_both, hot[f, :, cols]))
    for f in range(FAR_DOT_FACES, 6):
        for at in range(0, cells, LANES):
            put_z(f, slice(at, at + LANES), far_gather(blocks_z, width, f, at))

    receive(1)
    blocks_u = turn(from_gy_u, from_gx_u)
    parts = [from_gy_u[b, ghosts : ghosts + hangs, :] for b in range(bits)]
    parts.append(jnp.zeros((hang_pad - hang_count, width), F32))
    hang_flat[...] = jnp.concatenate(parts, 0).T
    live_lanes = lax.broadcasted_iota(jnp.int32, (rows, LANES), 1) < hang_rows
    hang_all = spread([hang_flat[pl.ds(k, rows, stride=fields), :] for k in range(fields)])
    hang_hi, hang_lo = [
        jnp.concatenate([jnp.where(face_wide == (f ^ 1), x, hang_zero) for f in range(6)], 0)
        for x in split(hang_all)
    ]
    trace_parts = split(dot3(op_trace[:, 0 : 6 * rows], hang_hi, hang_lo))
    trace_hi, trace_lo = [
        jnp.concatenate([jnp.where(child_wide == h, x, hang_zero) for h in range(children)], 0)
        for x in trace_parts
    ]
    lifted = dot3(op_back[...], trace_hi, trace_lo)
    mains, ends = [], []
    for k in range(fields):
        at = k * hang_rows
        block = lifted[:, at // LANES * LANES : at // LANES * LANES + LANES]
        if at % LANES:
            block = pltpu.roll(block, LANES - at % LANES, 1)
        block = jnp.where(live_lanes, block, 0.0)
        mains.append(block[0:tight])
        ends.append(block[tight:rows])
    lift_hi, lift_lo = split(jnp.concatenate(mains + ends, 0))
    if 2 * hang_rows <= LANES:
        lift_lo = pltpu.roll(lift_lo.astype(F32), hang_rows, 1)
        lift = (lift_hi.astype(F32) + lift_lo).astype(BF16)[:, 0 : 2 * hang_rows]
    else:
        lift = jnp.concatenate([lift_hi[:, 0:hang_rows], lift_lo[:, 0:hang_rows]], 1)
    end_rows = rows - tight

    for f in range(6):
        for at in range(0, cells, LANES):
            cols = slice(at, at + LANES)
            hi, lo = split(far_gather(blocks_u, 0, f, at))
            for k in range(fields):
                span = slice(k * rows, (k + 1) * rows)
                u_all[k, f, 0:rows, cols] = hi[span]
                u_all[k, f, rows : 2 * rows, cols] = lo[span]
                u_all[k, f, 2 * rows : 3 * rows, cols] = hi[span]
    for at in range(0, cells, chunk_lanes):
        cols = slice(at, at + chunk_lanes)
        totals, end_totals = [], []
        for k in range(fields):
            forms = dot3(op_z[...], z_hi[k, :, cols], z_lo[k, :, cols])
            own_u = sources[k * rows : (k + 1) * rows, cols]
            src = jnp.concatenate(
                [
                    source_flat[i, pl.ds(k, rows, stride=fields), :]
                    for i in range(at // LANES, (at + chunk_lanes) // LANES)
                ],
                1,
            )
            cell_part = src * forms[0:rows] - coef[:, cols] * own_u * forms[rows : 2 * rows]
            cell_sum = jnp.sum(cell_part, axis=0, keepdims=True)
            out_ref[k : k + 1, cols] = size[:, cols] * cell_sum * (1.0 / math.sqrt(quads))
            part_z[k] = forms[3 * rows : 3 * rows + 6 * tight]
            part_x[k] = forms[3 * rows + 6 * tight : 3 * rows + 6 * tight + 8 * tails]
            own_part = own_u * forms[2 * rows : 3 * rows]
            end_totals.append(sum(own_part[i : i + 8] for i in range(8, rows, 8)) + own_part[0:8])
            totals.append(jnp.zeros((tight, chunk_lanes), F32))
        for f in range(6):
            child = jnp.broadcast_to(child_ref[f : f + 1, cols], (tight, chunk_lanes))
            masks = [child == h for h in range(children)]
            sub = lax.broadcasted_iota(jnp.int32, (8, chunk_lanes), 0)
            end_mask = sub == child[0:8]
            returned = mm(lift, scatter[f, :, cols])
            for k in range(fields):
                jumps = mm(op_u[f, :, 0 : 3 * rows], u_all[k, f, :, cols])
                jump = jumps[children * tight : 5 * tight]
                for h in range(children):
                    jump = jnp.where(masks[h], jumps[h * tight : (h + 1) * tight], jump)
                jump = jump + returned[k * tight : (k + 1) * tight]
                totals[k] = totals[k] + jump * part_z[k, f * tight : (f + 1) * tight]
                end_at = fields * tight + k * end_rows
                for e in range(tails):
                    block = jumps[tail_at + 8 * e : tail_at + 8 * (e + 1)]
                    back = returned[end_at + 8 * (e // 8) : end_at + 8 * (e // 8) + 8]
                    if tails > 1:
                        back = jnp.where(sub == e % 8, back, 0.0)
                    block = jnp.where(end_mask, block, 0.0) + back
                    weight = jnp.broadcast_to(part_x[k, 8 * e + f : 8 * e + f + 1, :], block.shape)
                    end_totals[k] = end_totals[k] + block * weight
        for k in range(fields):
            face_sum = jnp.sum(jnp.concatenate([totals[k], end_totals[k]], 0), axis=0, keepdims=True)
            row = fields + k
            out_ref[row : row + 1, cols] = size[:, cols] * face_sum * (1.0 / math.sqrt(6 * points))


def solution(mesh):
    n_gx, n_gy = mesh.shape["gx"], mesh.shape["gy"]
    bits = n_gy.bit_length() - 1

    def shards(
        primal,
        adjoint,
        source,
        coefficient,
        levels,
        recon,
        stiffness,
        interp,
        flux,
        face_eval,
        child_interp,
        ghost_send,
        edge_send,
        neighbor_slot,
        neighbor_child,
        hang_send,
        hang_recv,
    ):
        fields, dofs, cells = primal.shape
        ghosts, edges, hangs = ghost_send.shape[2], edge_send.shape[2], hang_send.shape[3]
        rows = round_up(dofs, 32)
        quads = recon.shape[1]
        quad_rows = round_up(quads, LANES)
        hang_rows = max(32, 1 << (bits * hangs - 1).bit_length())
        chunk = min(cells, 256)
        dims = (n_gx, n_gy, bits, ghosts, edges, hangs, fields, rows, hang_rows, chunk)
        primal, adjoint, source = [x.transpose(1, 0, 2) for x in (primal, adjoint, source)]
        main_pad = round_up(bits * ghosts + 2 * edges, LANES)
        hang_pad = round_up(bits * hangs, LANES)
        wide = 2 * fields * rows
        points = flux.shape[1]
        tight, tails = points // 8 * 8, points % 8
        form_rows = round_up(3 * rows + 6 * tight + 8 * tails, 16)
        map_rows = round_up(5 * tight + 8 * tails, 16)
        args = (
            primal,
            adjoint,
            source,
            coefficient.reshape(1, cells),
            levels.reshape(1, cells),
            recon.transpose(2, 0, 1),
            stiffness.T,
            interp.T,
            flux,
            face_eval,
            child_interp.transpose(1, 0, 2),
            neighbor_slot,
            neighbor_child,
            hang_recv,
            ghost_send,
            edge_send,
            hang_send,
        )
        raw = pl.pallas_call(
            functools.partial(compute_kernel, dims, len(args)),
            out_shape=pltpu.VMEM((2 * fields, cells), F32),
            in_specs=[pl.BlockSpec(memory_space=pltpu.MemorySpace.HBM)] * len(args),
            out_specs=pl.BlockSpec(memory_space=pltpu.VMEM),
            scratch_shapes=[pltpu.VMEM(x.shape, x.dtype) for x in args]
            + [
                pltpu.VMEM((8 * rows, quad_rows), F32),
                pltpu.VMEM((form_rows, quad_rows), F32),
                pltpu.VMEM((6 * rows, LANES), F32),
                pltpu.VMEM((6 * rows, quad_rows), F32),
                pltpu.VMEM((4 * rows, LANES), F32),
                pltpu.VMEM((map_rows, LANES), F32),
                pltpu.VMEM((4 * rows, LANES), F32),
                pltpu.VMEM((rows, round_up(6 * rows, LANES)), F32),
                pltpu.VMEM((rows, 6 * LANES), F32),
                pltpu.VMEM((2 * form_rows, 7 * rows), BF16),
                pltpu.VMEM((6, map_rows, LANES), BF16),
                pltpu.VMEM((2 * rows, round_up(6 * rows, LANES)), BF16),
                pltpu.VMEM((2 * rows, 4 * rows), BF16),
                pltpu.VMEM((8, hang_pad), jnp.int32),
                pltpu.VMEM((fields, 7 * rows, cells), BF16),
                pltpu.VMEM((fields, 7 * rows, cells), BF16),
                pltpu.VMEM((fields, 6, 3 * rows, cells), BF16),
                pltpu.VMEM((wide, cells), F32),
                pltpu.VMEM((max(cells, main_pad) // LANES, wide, LANES), F32),
                pltpu.VMEM((cells // LANES, fields * rows, LANES), F32),
                pltpu.VMEM((fields * rows, hang_pad), F32),
                pltpu.VMEM((6, wide, cells), F32),
                pltpu.VMEM((6, 2 * main_pad, cells), BF16),
                pltpu.VMEM((6, 2 * hang_rows, cells), BF16),
                pltpu.VMEM((fields, 6 * tight, chunk), F32),
                pltpu.VMEM((fields, max(8 * tails, 8), chunk), F32),
            ]
            + [
                pltpu.VMEM((bits, ghosts + hangs, wide // 2), F32),
                pltpu.VMEM((2, edges, wide // 2), F32),
                pltpu.VMEM((bits, ghosts, wide // 2), F32),
                pltpu.VMEM((2, edges, wide // 2), F32),
            ]
            * 2
            + [
                pltpu.VMEM((8, main_pad + hang_pad), jnp.int32),
                pltpu.VMEM((wide, LANES), F32),
                pltpu.SemaphoreType.DMA((len(args),)),
                pltpu.SemaphoreType.DMA((2, bits)),
                pltpu.SemaphoreType.DMA((2, bits)),
                pltpu.SemaphoreType.DMA((2, 2)),
                pltpu.SemaphoreType.DMA((2, 2)),
            ],
            compiler_params=pltpu.CompilerParams(collective_id=0, has_side_effects=True),
            name="indicators",
        )(*args)
        return raw[:fields], raw[fields:]

    split_all = ("gx", "gy")
    placed = (
        P(None, None, split_all),
        P(None, None, split_all),
        P(None, None, split_all),
        P(split_all),
        P(split_all),
        P(),
        P(),
        P(),
        P(),
        P(),
        P(),
        P(split_all, None, None),
        P(split_all, None, None),
        P(None, split_all),
        P(None, split_all),
        P(None, split_all, None, None),
        P(None, split_all, None, None),
    )
    return jax.shard_map(
        shards,
        mesh=mesh,
        in_specs=placed,
        out_specs=(P(None, split_all), P(None, split_all)),
        check_vma=False,
    )
```

```python
import functools
import math

import jax
import jax.numpy as jnp
from jax import lax
from jax.experimental import pallas as pl
from jax.experimental.pallas import tpu as pltpu
from jax.sharding import PartitionSpec as P

LANES = 128
F32 = jnp.float32
BF16 = jnp.bfloat16
MESH = pl.DeviceIdType.MESH
DOT_FACES = 4
FAR_DOT_FACES = 3


def round_up(value, unit):
    return -(-value // unit) * unit


def split(x):
    hi = x.astype(BF16)
    lo = (x - hi.astype(F32)).astype(BF16)
    return hi, lo


def both(x):
    return jnp.concatenate(split(x), 0)


def mm(a, b):
    return jnp.dot(a, b, preferred_element_type=F32)


def mm_nt(a, b):
    return lax.dot_general(a, b, (((1,), (1,)), ((), ())), preferred_element_type=F32)


def dot3(a_both, b_hi, b_lo, dot=mm):
    rows = a_both.shape[0] // 2
    first = dot(a_both, b_hi)
    return first[:rows] + first[rows:] + dot(a_both[:rows], b_lo)


def fill_flat(flat, ref, base, width):
    dofs, fields, cells = ref.shape
    used = dofs * fields
    for i in range(cells // LANES):
        for j in range(dofs):
            row = base + j * fields
            flat[i, row : row + fields, :] = ref[j, :, i * LANES : (i + 1) * LANES]
        flat[i, base + used : base + width, :] = jnp.zeros((width - used, LANES), F32)


def lane_gather(blocks, lane, block_id):
    total = jnp.zeros(blocks[0].shape, F32)
    for i, block in enumerate(blocks):
        got = jnp.take_along_axis(block, lane, axis=1)
        total = jnp.where(block_id == i, got, total)
    return total


def one_hot(index, rows):
    parts = []
    for first in range(0, rows, 256):
        count = min(256, rows - first)
        wide = jnp.broadcast_to((index - first).astype(F32), (count, index.shape[1])).astype(BF16)
        ids = lax.broadcasted_iota(jnp.int32, wide.shape, 0).astype(F32).astype(BF16)
        parts.append(jnp.where(wide == ids, jnp.ones_like(wide), jnp.zeros_like(wide)))
    return parts[0] if len(parts) == 1 else jnp.concatenate(parts, 0)


def compute_kernel(dims, n_args, *refs):
    n_gx, n_gy, bits, ghosts, edges, hangs, fields, rows, hang_rows, chunk_lanes = dims
    hbm = refs[:n_args]
    out_ref = refs[n_args]
    local = refs[n_args + 1 : 2 * n_args + 1]
    (
        op_recon,
        op_left,
        op_flux_rows,
        op_face_rows,
        op_child,
        op_child_tight,
        child_flat,
        op_flux,
        op_rep,
        op_z,
        op_u,
        op_trace,
        op_back,
        maps,
        z_hi,
        z_lo,
        u_all,
        sources,
        flat,
        source_flat,
        hang_flat,
        near,
        hot,
        scatter,
        part_z,
        part_x,
        from_gy_u,
        from_gx_u,
        from_gy_z,
        from_gx_z,
        to_gy_u,
        to_gx_u,
        to_gy_z,
        to_gx_z,
        ids,
        packed,
        in_sems,
        send_gy,
        recv_gy,
        send_gx,
        recv_gx,
        ready,
    ) = refs[2 * n_args + 1 :]
    (
        primal_ref,
        adjoint_ref,
        source_ref,
        coef_ref,
        levels_ref,
        recon_ref,
        stiffness_ref,
        interp_ref,
        flux_ref,
        face_eval_ref,
        child_interp_ref,
        slot_ref,
        child_ref,
        hang_ref,
        ghost_ref,
        edge_ref,
        hang_send_ref,
    ) = local
    gx = lax.axis_index("gx")
    gy = lax.axis_index("gy")
    dofs, _, cells = primal_ref.shape
    width = fields * rows
    wide = 2 * width
    partners = [jnp.bitwise_xor(gy, 1 << b) for b in range(bits)]

    bit_of = [gy // (1 << b) % 2 for b in range(bits)]
    barrier = pltpu.get_barrier_semaphore()
    for b, partner in enumerate(partners):

        @pl.when(bit_of[b] == 0)
        def _():
            pl.semaphore_signal(barrier, inc=1, device_id=(gx, partner), device_id_type=MESH)

    @pl.when(gx < n_gx - 1)
    def _():
        pl.semaphore_signal(barrier, inc=1, device_id=(gx + 1, gy), device_id_type=MESH)

    order = [14, 15, 16, 1, 0, 11, 5, 6, 7, 8, 9, 10, 13, 12, 3, 4, 2]
    loads = [pltpu.make_async_copy(hbm[i], local[i], in_sems.at[i]) for i in range(n_args)]
    for i in order[:5]:
        loads[i].start()

    main = bits * ghosts + 2 * edges
    main_pad = round_up(main, LANES)
    hang_pad = round_up(bits * hangs, LANES)
    ids[...] = jnp.zeros_like(ids)
    for i in order[:4]:
        loads[i].wait()
    for i in order[5:]:
        loads[i].start()
    for b, partner in enumerate(partners):
        ids[0:1, b * ghosts : (b + 1) * ghosts] = ghost_ref[0, pl.ds(partner, 1), :]
        at = main_pad + b * hangs
        ids[0:1, at : at + hangs] = hang_send_ref[0, 0, pl.ds(partner, 1), :]
    for side in range(2):
        at = bits * ghosts + side * edges
        ids[0:1, at : at + edges] = edge_ref[0, side : side + 1, :]
    chosen = jnp.maximum(ids[0:1, :], 0)

    lower = sum(bit_of) + jnp.minimum(gx, 1)

    @pl.when(lower > 0)
    def _():
        pl.semaphore_wait(barrier, lower)

    for b, partner in enumerate(partners):

        @pl.when(bit_of[b] == 1)
        def _():
            pl.semaphore_signal(ready.at[b], inc=1, device_id=(gx, partner), device_id_type=MESH)

    @pl.when(gx > 0)
    def _():
        pl.semaphore_signal(ready.at[bits], inc=1, device_id=(gx - 1, gy), device_id_type=MESH)

    def pick(base, at):
        part = jnp.broadcast_to(chosen[:, at : at + LANES], (rows, LANES))
        lane = jnp.bitwise_and(part, LANES - 1)
        block_id = jnp.right_shift(part, 7)
        for k in range(fields):
            span = slice(base + k * rows, base + (k + 1) * rows)
            blocks = [flat[i, span, :] for i in range(cells // LANES)]
            packed[span, :] = lane_gather(blocks, lane, block_id)
        return packed[base : base + width, :].T

    def pack(base, to_gy, to_gx):
        for at in range(0, main_pad, LANES):
            turned = pick(base, at)
            for first in range(at, min(at + LANES, main), edges):
                chunk = turned[first - at : first - at + edges]
                if first < bits * ghosts:
                    to_gy[first // ghosts, pl.ds(first % ghosts, edges), :] = chunk
                else:
                    to_gx[(first - bits * ghosts) // edges] = chunk

    stages = [(to_gy_z, from_gy_z, to_gx_z, from_gx_z), (to_gy_u, from_gy_u, to_gx_u, from_gx_u)]

    def gy_copy(stage, b):
        src, dst, _, _ = stages[stage]
        return pltpu.make_async_remote_copy(
            src_ref=src.at[b],
            dst_ref=dst.at[b],
            send_sem=send_gy.at[stage, b],
            recv_sem=recv_gy.at[stage, b],
            device_id=(gx, partners[b]),
            device_id_type=MESH,
        )

    def low_copy(stage):
        _, _, src, dst = stages[stage]
        return pltpu.make_async_remote_copy(
            src_ref=src.at[0],
            dst_ref=dst.at[1],
            send_sem=send_gx.at[stage, 0],
            recv_sem=recv_gx.at[stage, 1],
            device_id=(gx - 1, gy),
            device_id_type=MESH,
        )

    def high_copy(stage):
        _, _, src, dst = stages[stage]
        return pltpu.make_async_remote_copy(
            src_ref=src.at[1],
            dst_ref=dst.at[0],
            send_sem=send_gx.at[stage, 1],
            recv_sem=recv_gx.at[stage, 0],
            device_id=(gx + 1, gy),
            device_id_type=MESH,
        )

    def send_lower(stage):
        for b in reversed(range(bits)):

            @pl.when(bit_of[b] == 1)
            def _():
                gy_copy(stage, b).start()

        @pl.when(gx > 0)
        def _():
            low_copy(stage).start()

    fill_flat(flat, adjoint_ref, width, width)
    pack(width, to_gy_z, to_gx_z)
    send_lower(0)
    loads[order[4]].wait()
    fill_flat(flat, primal_ref, 0, width)
    pack(0, to_gy_u, to_gx_u)
    for at in range(main_pad, main_pad + hang_pad, LANES):
        turned = pick(0, at)
        for b in range(bits):
            at_slot = b * hangs - (at - main_pad)
            if 0 <= at_slot < LANES:
                to_gy_u[b, ghosts : ghosts + hangs, :] = turned[at_slot : at_slot + hangs]
    send_lower(1)

    for b in range(bits):

        @pl.when(bit_of[b] == 0)
        def _():
            pl.semaphore_wait(ready.at[b], 1)
            for stage in range(2):
                gy_copy(stage, b).start()

    @pl.when(gx < n_gx - 1)
    def _():
        pl.semaphore_wait(ready.at[bits], 1)
        for stage in range(2):
            high_copy(stage).start()

    @pl.when(gx == 0)
    def _():
        from_gx_z[0] = jnp.zeros(from_gx_z.shape[1:], F32)
        from_gx_u[0] = jnp.zeros(from_gx_u.shape[1:], F32)

    @pl.when(gx == n_gx - 1)
    def _():
        from_gx_z[1] = jnp.zeros(from_gx_z.shape[1:], F32)
        from_gx_u[1] = jnp.zeros(from_gx_u.shape[1:], F32)

    def receive(stage):
        for b in range(bits):
            gy_copy(stage, b).wait()

        @pl.when(gx > 0)
        def _():
            low_copy(stage).wait_send()
            high_copy(stage).wait_recv()

        @pl.when(gx < n_gx - 1)
        def _():
            high_copy(stage).wait_send()
            low_copy(stage).wait_recv()

    quads = recon_ref.shape[2]
    own_blocks = cells // LANES
    points = flux_ref.shape[1]
    remote = bits * ghosts + 2 * edges
    remote_pad = round_up(remote, LANES)
    hang_count = bits * hangs
    children = 4
    tight = points // 8 * 8
    tails = points - tight
    form_rows = op_z.shape[0] // 2
    tail_at = 5 * tight

    for i in order[5:]:
        loads[i].wait()

    for i in range(own_blocks):
        for group in range(2 * fields):
            first = group // fields * width + group % fields
            sources[group * rows : (group + 1) * rows, i * LANES : (i + 1) * LANES] = flat[
                i, pl.ds(first, rows, stride=fields), :
            ]
    own_both = both(sources[...])
    slot = slot_ref[...]
    shifted = slot - cells
    log_ghosts = ghosts.bit_length() - 1
    peer = jnp.right_shift(shifted, log_ghosts)
    within = jnp.bitwise_and(shifted, ghosts - 1)
    differing = jnp.bitwise_xor(peer, gy)
    place_of = jnp.zeros_like(slot)
    for b in range(1, bits):
        place_of = jnp.where(differing == (1 << b), b, place_of)
    far = jnp.where(
        shifted < n_gy * ghosts, place_of * ghosts + within, shifted - (n_gy - bits) * ghosts
    )
    far = jnp.where(shifted < 0, -1, far)
    for f in range(DOT_FACES):
        for at in range(0, cells, chunk_lanes):
            cols = slice(at, at + chunk_lanes)
            got = mm(own_both, one_hot(slot[f : f + 1, cols], cells))
            near[f, :, cols] = got[:wide] + got[wide:]
    for f in range(DOT_FACES, 6):
        for at in range(0, cells, LANES):
            cols = slice(at, at + LANES)
            part = jnp.broadcast_to(slot[f : f + 1, cols], (rows, LANES))
            lane = jnp.bitwise_and(part, LANES - 1)
            block_id = jnp.right_shift(part, 7)
            for group in range(2 * fields):
                span = slice(group * rows, (group + 1) * rows)
                blocks = [sources[span, i * LANES : (i + 1) * LANES] for i in range(own_blocks)]
                near[f, span, cols] = lane_gather(blocks, lane, block_id)
    for f in range(FAR_DOT_FACES):
        for at in range(0, chunk_lanes, chunk_lanes):
            cols = slice(at, at + chunk_lanes)
            hot_part = one_hot(far[f : f + 1, cols], remote_pad)
            hot[f, 0:remote_pad, cols] = hot_part
            hot[f, remote_pad : 2 * remote_pad, cols] = hot_part

    op_recon[...] = jnp.zeros_like(op_recon)
    op_left[...] = jnp.zeros_like(op_left)
    op_flux_rows[...] = jnp.zeros_like(op_flux_rows)
    op_face_rows[...] = jnp.zeros_like(op_face_rows)
    op_child_tight[...] = jnp.zeros_like(op_child_tight)
    child_flat[...] = jnp.zeros_like(child_flat)
    op_flux[...] = jnp.zeros_like(op_flux)
    for j in range(dofs):
        op_recon[8 * j : 8 * j + 7, 0:quads] = recon_ref[j]
    op_left[0:dofs, 0:quads] = interp_ref[...]
    op_left[rows : rows + dofs, 0:quads] = stiffness_ref[...]
    for f in range(6):
        at = 3 * rows + f * tight
        op_left[at : at + tight, 0:quads] = face_eval_ref[f, 0:tight, :]
        for e in range(points - tight):
            at = 3 * rows + 6 * tight + 8 * e + f
            op_left[at : at + 1, 0:quads] = face_eval_ref[f, tight + e : tight + e + 1, :]
        op_face_rows[f * rows : f * rows + points, 0:quads] = face_eval_ref[f]
        op_flux_rows[f * rows : f * rows + points, 0:dofs] = flux_ref[f]
        op_flux[0:points, f * rows : f * rows + dofs] = flux_ref[f]
    for p in range(points):
        child_flat[children * p : children * (p + 1), 0:points] = child_interp_ref[p]
    for h in range(children):
        op_child[h * rows : (h + 1) * rows, :] = child_flat[pl.ds(h, rows, stride=children), :]
    flux_turned = op_flux_rows[...].T[0:rows]
    op_left[2 * rows : 3 * rows, :] = dot3(both(flux_turned), *split(op_face_rows[...]))
    recon_turned = jnp.concatenate([op_recon[pl.ds(f, rows, stride=8), :] for f in range(7)], 0)
    op_z[...] = both(dot3(both(op_left[...]), *split(recon_turned), dot=mm_nt))
    for f in range(6):
        single = op_flux_rows[f * rows : (f + 1) * rows, :]
        thrice = single + pltpu.roll(single, rows, 1) + pltpu.roll(single, 2 * rows, 1)
        op_rep[:, (f ^ 1) * LANES : ((f ^ 1) + 1) * LANES] = thrice
    for h in range(children):
        op_child_tight[h * tight : (h + 1) * tight, :] = op_child[h * rows : h * rows + tight, :]
        for e in range(tails):
            at = tail_at + 8 * e + h
            op_child_tight[at : at + 1, :] = op_child[h * rows + tight + e : h * rows + tight + e + 1, :]
    same = (tight, LANES)
    op_child_tight[children * tight : 5 * tight, :] = jnp.where(
        lax.broadcasted_iota(jnp.int32, same, 0) == lax.broadcasted_iota(jnp.int32, same, 1), 1.0, 0.0
    )
    for e in range(tails):
        at = tail_at + 8 * e + children
        op_child_tight[at : at + 1, :] = jnp.where(
            lax.broadcasted_iota(jnp.int32, (1, LANES), 1) == tight + e, 1.0, 0.0
        )
    mapped_ops = dot3(both(op_child_tight[...])[:, 0:rows], *split(op_rep[...]))
    high_lanes = lax.broadcasted_iota(jnp.int32, (op_u.shape[1], LANES), 1) < 2 * rows
    for f in range(6):
        hi, lo = split(mapped_ops[:, f * LANES : (f + 1) * LANES])
        op_u[f] = jnp.where(high_lanes, hi.astype(F32), lo.astype(F32)).astype(BF16)
    op_trace[...] = both(op_flux[...])
    op_back[...] = both(op_child[...].T[0:rows])

    maps[...] = jnp.full(maps.shape, -1, jnp.int32)
    for b in range(bits):
        partner = jnp.bitwise_xor(gy, 1 << b)
        for i in range(3):
            maps[i : i + 1, b * hangs : (b + 1) * hangs] = hang_ref[i, 0, pl.ds(partner, 1), :]
    live = maps[0:1, :] >= 0
    place = jnp.where(live, maps[0:1, :] + maps[1:2, :] * cells, -1).astype(F32)
    place_rows = jnp.broadcast_to(place, (LANES, hang_pad)).T[0:hang_rows, 0:1]
    column = lax.broadcasted_iota(jnp.int32, (hang_rows, cells), 1).astype(F32)
    place_wide = jnp.broadcast_to(place_rows, (hang_rows, cells))
    for f in range(6):
        hit = jnp.where(place_wide == column + float(f * cells), 1.0, 0.0).astype(BF16)
        scatter[f, 0:hang_rows] = hit
        scatter[f, hang_rows : 2 * hang_rows] = hit

    def spread(x):
        outs = []
        for first in range(0, fields * hang_rows, LANES):
            total = None
            for k in range(fields):
                at = k * hang_rows - first
                if 0 <= at < LANES:
                    piece = x[k][:, 0:LANES]
                    piece = pltpu.roll(piece, at, 1) if at else piece
                    total = piece if total is None else total + piece
            outs.append(total)
        return outs[0] if len(outs) == 1 else jnp.concatenate(outs, 1)

    maps_all = spread([maps[...] + 1] * fields) - 1
    hang_lanes = fields * hang_rows
    face_wide = jnp.broadcast_to(maps_all[1:2, :], (rows, hang_lanes))
    child_wide = jnp.broadcast_to(maps_all[2:3, :], (rows, hang_lanes))
    hang_zero = jnp.zeros((rows, hang_lanes), BF16)

    fill_flat(source_flat, source_ref, 0, width)
    for k in range(fields):
        own_hi, own_lo = split(sources[(fields + k) * rows : (fields + k + 1) * rows, :])
        z_hi[k, 0:rows, :] = own_hi
        z_lo[k, 0:rows, :] = own_lo
    coef = coef_ref[...]
    size = jnp.exp2(-levels_ref[...].astype(F32))

    far_lane = jnp.bitwise_and(far, LANES - 1)
    far_block = jnp.right_shift(far, 7)

    def turn(from_gy, from_gx):
        parts = [from_gy[b, 0:ghosts, :] for b in range(bits)] + [from_gx[0], from_gx[1]]
        if remote_pad > remote:
            parts.append(jnp.zeros((remote_pad - remote, width), F32))
        arrived = jnp.concatenate(parts, 0).T
        blocks = []
        for i in range(remote_pad // LANES):
            flat[i, 0:width, :] = arrived[:, i * LANES : (i + 1) * LANES]
            blocks.append(
                jnp.concatenate(
                    [flat[i, pl.ds(k, rows, stride=fields), :] for k in range(fields)], 0
                )
            )
        return blocks

    def far_gather(blocks, base, f, at):
        cols = slice(at, at + LANES)
        lane = jnp.broadcast_to(far_lane[f : f + 1, cols], (rows, LANES))
        block_id = jnp.broadcast_to(far_block[f : f + 1, cols], (rows, LANES))
        outs = []
        for k in range(fields):
            span = slice(base + k * rows, base + (k + 1) * rows)
            total = near[f, span, cols]
            for i, block in enumerate(blocks):
                got = jnp.take_along_axis(block[k * rows : (k + 1) * rows], lane, axis=1)
                total = jnp.where(block_id == i, got, total)
            outs.append(total)
        return jnp.concatenate(outs, 0)

    def put_z(f, cols, total):
        hi, lo = split(total)
        for k in range(fields):
            span = slice(k * rows, (k + 1) * rows)
            z_hi[k, (1 + f) * rows : (2 + f) * rows, cols] = hi[span]
            z_lo[k, (1 + f) * rows : (2 + f) * rows, cols] = lo[span]

    def gather_z(at, dot_faces):
        cols = slice(at, at + chunk_lanes)
        for f in range(dot_faces):
            put_z(f, cols, near[f, width:, cols] + mm(far_both, hot[f, :, cols]))
        for f in range(dot_faces, 6):
            for first in range(at, at + chunk_lanes, LANES):
                put_z(f, slice(first, first + LANES), far_gather(blocks_z, width, f, first))

    def gather_u(at):
        for f in range(6):
            for first in range(at, at + chunk_lanes, LANES):
                cols = slice(first, first + LANES)
                hi, lo = split(far_gather(blocks_u, 0, f, first))
                for k in range(fields):
                    span = slice(k * rows, (k + 1) * rows)
                    u_all[k, f, 0:rows, cols] = hi[span]
                    u_all[k, f, rows : 2 * rows, cols] = lo[span]
                    u_all[k, f, 2 * rows : 3 * rows, cols] = hi[span]

    receive(0)
    blocks_z = turn(from_gy_z, from_gx_z)
    halves = [split(block) for block in blocks_z]
    far_both = jnp.concatenate([h[0] for h in halves] + [h[1] for h in halves], 1)
    gather_z(0, FAR_DOT_FACES)

    receive(1)
    blocks_u = turn(from_gy_u, from_gx_u)
    parts = [from_gy_u[b, ghosts : ghosts + hangs, :] for b in range(bits)]
    parts.append(jnp.zeros((hang_pad - hang_count, width), F32))
    hang_flat[...] = jnp.concatenate(parts, 0).T
    live_lanes = lax.broadcasted_iota(jnp.int32, (rows, LANES), 1) < hang_rows
    hang_all = spread([hang_flat[pl.ds(k, rows, stride=fields), :] for k in range(fields)])
    hang_hi, hang_lo = [
        jnp.concatenate([jnp.where(face_wide == (f ^ 1), x, hang_zero) for f in range(6)], 0)
        for x in split(hang_all)
    ]

    def hang_traces():
        trace_parts = split(dot3(op_trace[:, 0 : 6 * rows], hang_hi, hang_lo))
        return [
            jnp.concatenate([jnp.where(child_wide == h, x, hang_zero) for h in range(children)], 0)
            for x in trace_parts
        ]

    def hang_lift(lifted):
        mains, ends = [], []
        for k in range(fields):
            at = k * hang_rows
            block = lifted[:, at // LANES * LANES : at // LANES * LANES + LANES]
            if at % LANES:
                block = pltpu.roll(block, LANES - at % LANES, 1)
            block = jnp.where(live_lanes, block, 0.0)
            mains.append(block[0:tight])
            ends.append(block[tight:rows])
        lift_hi, lift_lo = split(jnp.concatenate(mains + ends, 0))
        if 2 * hang_rows <= LANES:
            lift_lo = pltpu.roll(lift_lo.astype(F32), hang_rows, 1)
            lift = (lift_hi.astype(F32) + lift_lo).astype(BF16)[:, 0 : 2 * hang_rows]
        else:
            lift = jnp.concatenate([lift_hi[:, 0:hang_rows], lift_lo[:, 0:hang_rows]], 1)
        return lift

    end_rows = rows - tight

    for at in range(0, cells, chunk_lanes):
        cols = slice(at, at + chunk_lanes)
        totals, end_totals = [], []
        gather_u(at)
        if at + chunk_lanes < cells:
            gather_z(at + chunk_lanes, 0)
        for k in range(fields):
            forms = dot3(op_z[...], z_hi[k, :, cols], z_lo[k, :, cols])
            if at == 0 and k == fields // 2:
                traces = hang_traces()
            own_u = sources[k * rows : (k + 1) * rows, cols]
            src = jnp.concatenate(
                [
                    source_flat[i, pl.ds(k, rows, stride=fields), :]
                    for i in range(at // LANES, (at + chunk_lanes) // LANES)
                ],
                1,
            )
            cell_part = src * forms[0:rows] - coef[:, cols] * own_u * forms[rows : 2 * rows]
            cell_sum = jnp.sum(cell_part, axis=0, keepdims=True)
            out_ref[k : k + 1, cols] = size[:, cols] * cell_sum * (1.0 / math.sqrt(quads))
            part_z[k] = forms[3 * rows : 3 * rows + 6 * tight]
            part_x[k] = forms[3 * rows + 6 * tight : 3 * rows + 6 * tight + 8 * tails]
            own_part = own_u * forms[2 * rows : 3 * rows]
            end_totals.append(sum(own_part[i : i + 8] for i in range(8, rows, 8)) + own_part[0:8])
            totals.append(jnp.zeros((tight, chunk_lanes), F32))
        for f in range(6):
            child = jnp.broadcast_to(child_ref[f : f + 1, cols], (tight, chunk_lanes))
            masks = [child == h for h in range(children)]
            sub = lax.broadcasted_iota(jnp.int32, (8, chunk_lanes), 0)
            end_mask = sub == child[0:8]
            for k in range(fields):
                jumps = mm(op_u[f, :, 0 : 3 * rows], u_all[k, f, :, cols])
                jump = jumps[children * tight : 5 * tight]
                for h in range(children):
                    jump = jnp.where(masks[h], jumps[h * tight : (h + 1) * tight], jump)
                totals[k] = totals[k] + jump * part_z[k, f * tight : (f + 1) * tight]
                for e in range(tails):
                    block = jumps[tail_at + 8 * e : tail_at + 8 * (e + 1)]
                    block = jnp.where(end_mask, block, 0.0)
                    weight = jnp.broadcast_to(part_x[k, 8 * e + f : 8 * e + f + 1, :], block.shape)
                    end_totals[k] = end_totals[k] + block * weight
            if at == 0 and f == 2:
                lift = hang_lift(dot3(op_back[...], *traces))
        for f in range(6):
            returned = mm(lift, scatter[f, :, cols])
            for k in range(fields):
                back = returned[k * tight : (k + 1) * tight]
                totals[k] = totals[k] + back * part_z[k, f * tight : (f + 1) * tight]
                end_at = fields * tight + k * end_rows
                for e in range(tails):
                    back = returned[end_at + e // 8 * 8 : end_at + e // 8 * 8 + 8]
                    if tails > 1:
                        back = jnp.where(sub == e % 8, back, 0.0)
                    weight = jnp.broadcast_to(part_x[k, 8 * e + f : 8 * e + f + 1, :], back.shape)
                    end_totals[k] = end_totals[k] + back * weight
        for k in range(fields):
            face_sum = jnp.sum(jnp.concatenate([totals[k], end_totals[k]], 0), axis=0, keepdims=True)
            row = fields + k
            out_ref[row : row + 1, cols] = size[:, cols] * face_sum * (1.0 / math.sqrt(6 * points))


def solution(mesh):
    n_gx, n_gy = mesh.shape["gx"], mesh.shape["gy"]
    bits = n_gy.bit_length() - 1

    def shards(
        primal,
        adjoint,
        source,
        coefficient,
        levels,
        recon,
        stiffness,
        interp,
        flux,
        face_eval,
        child_interp,
        ghost_send,
        edge_send,
        neighbor_slot,
        neighbor_child,
        hang_send,
        hang_recv,
    ):
        fields, dofs, cells = primal.shape
        ghosts, edges, hangs = ghost_send.shape[2], edge_send.shape[2], hang_send.shape[3]
        rows = round_up(dofs, 32)
        quads = recon.shape[1]
        quad_rows = round_up(quads, LANES)
        hang_rows = max(32, 1 << (bits * hangs - 1).bit_length())
        chunk = min(cells, 256)
        dims = (n_gx, n_gy, bits, ghosts, edges, hangs, fields, rows, hang_rows, chunk)
        primal, adjoint, source = [x.transpose(1, 0, 2) for x in (primal, adjoint, source)]
        main_pad = round_up(bits * ghosts + 2 * edges, LANES)
        hang_pad = round_up(bits * hangs, LANES)
        wide = 2 * fields * rows
        points = flux.shape[1]
        tight, tails = points // 8 * 8, points % 8
        form_rows = round_up(3 * rows + 6 * tight + 8 * tails, 16)
        map_rows = round_up(5 * tight + 8 * tails, 16)
        args = (
            primal,
            adjoint,
            source,
            coefficient.reshape(1, cells),
            levels.reshape(1, cells),
            recon.transpose(2, 0, 1),
            stiffness.T,
            interp.T,
            flux,
            face_eval,
            child_interp.transpose(1, 0, 2),
            neighbor_slot,
            neighbor_child,
            hang_recv,
            ghost_send,
            edge_send,
            hang_send,
        )
        raw = pl.pallas_call(
            functools.partial(compute_kernel, dims, len(args)),
            out_shape=pltpu.VMEM((2 * fields, cells), F32),
            in_specs=[pl.BlockSpec(memory_space=pltpu.MemorySpace.HBM)] * len(args),
            out_specs=pl.BlockSpec(memory_space=pltpu.VMEM),
            scratch_shapes=[pltpu.VMEM(x.shape, x.dtype) for x in args]
            + [
                pltpu.VMEM((8 * rows, quad_rows), F32),
                pltpu.VMEM((form_rows, quad_rows), F32),
                pltpu.VMEM((6 * rows, LANES), F32),
                pltpu.VMEM((6 * rows, quad_rows), F32),
                pltpu.VMEM((4 * rows, LANES), F32),
                pltpu.VMEM((map_rows, LANES), F32),
                pltpu.VMEM((4 * rows, LANES), F32),
                pltpu.VMEM((rows, round_up(6 * rows, LANES)), F32),
                pltpu.VMEM((rows, 6 * LANES), F32),
                pltpu.VMEM((2 * form_rows, 7 * rows), BF16),
                pltpu.VMEM((6, map_rows, LANES), BF16),
                pltpu.VMEM((2 * rows, round_up(6 * rows, LANES)), BF16),
                pltpu.VMEM((2 * rows, 4 * rows), BF16),
                pltpu.VMEM((8, hang_pad), jnp.int32),
                pltpu.VMEM((fields, 7 * rows, cells), BF16),
                pltpu.VMEM((fields, 7 * rows, cells), BF16),
                pltpu.VMEM((fields, 6, 3 * rows, cells), BF16),
                pltpu.VMEM((wide, cells), F32),
                pltpu.VMEM((max(cells, main_pad) // LANES, wide, LANES), F32),
                pltpu.VMEM((cells // LANES, fields * rows, LANES), F32),
                pltpu.VMEM((fields * rows, hang_pad), F32),
                pltpu.VMEM((6, wide, cells), F32),
                pltpu.VMEM((6, 2 * main_pad, cells), BF16),
                pltpu.VMEM((6, 2 * hang_rows, cells), BF16),
                pltpu.VMEM((fields, 6 * tight, chunk), F32),
                pltpu.VMEM((fields, max(8 * tails, 8), chunk), F32),
            ]
            + [
                pltpu.VMEM((bits, ghosts + hangs, wide // 2), F32),
                pltpu.VMEM((2, edges, wide // 2), F32),
                pltpu.VMEM((bits, ghosts, wide // 2), F32),
                pltpu.VMEM((2, edges, wide // 2), F32),
            ]
            * 2
            + [
                pltpu.VMEM((8, main_pad + hang_pad), jnp.int32),
                pltpu.VMEM((wide, LANES), F32),
                pltpu.SemaphoreType.DMA((len(args),)),
                pltpu.SemaphoreType.DMA((2, bits)),
                pltpu.SemaphoreType.DMA((2, bits)),
                pltpu.SemaphoreType.DMA((2, 2)),
                pltpu.SemaphoreType.DMA((2, 2)),
                pltpu.SemaphoreType.REGULAR((bits + 1,)),
            ],
            compiler_params=pltpu.CompilerParams(collective_id=0, has_side_effects=True),
            name="indicators",
        )(*args)
        return raw[:fields], raw[fields:]

    split_all = ("gx", "gy")
    placed = (
        P(None, None, split_all),
        P(None, None, split_all),
        P(None, None, split_all),
        P(split_all),
        P(split_all),
        P(),
        P(),
        P(),
        P(),
        P(),
        P(),
        P(split_all, None, None),
        P(split_all, None, None),
        P(None, split_all),
        P(None, split_all),
        P(None, split_all, None, None),
        P(None, split_all, None, None),
    )
    return jax.shard_map(
        shards,
        mesh=mesh,
        in_specs=placed,
        out_specs=(P(None, split_all), P(None, split_all)),
        check_vma=False,
    )
```

```python
import functools
import math

import jax
import jax.numpy as jnp
from jax import lax
from jax.experimental import pallas as pl
from jax.experimental.pallas import tpu as pltpu
from jax.sharding import PartitionSpec as P

LANES = 128
F32 = jnp.float32
BF16 = jnp.bfloat16
MESH = pl.DeviceIdType.MESH
EARLY_FORMS = 2
DOT_FACES = 4
FAR_DOT_FACES = 3


def round_up(value, unit):
    return -(-value // unit) * unit


def split(x):
    hi = x.astype(BF16)
    lo = (x - hi.astype(F32)).astype(BF16)
    return hi, lo


def both(x):
    return jnp.concatenate(split(x), 0)


def mm(a, b):
    return jnp.dot(a, b, preferred_element_type=F32)


def mm_nt(a, b):
    return lax.dot_general(a, b, (((1,), (1,)), ((), ())), preferred_element_type=F32)


def dot3(a_both, b_hi, b_lo, dot=mm):
    rows = a_both.shape[0] // 2
    first = dot(a_both, b_hi)
    return first[:rows] + first[rows:] + dot(a_both[:rows], b_lo)


def fill_flat(flat, ref, base, width):
    dofs, fields, cells = ref.shape
    used = dofs * fields
    for i in range(cells // LANES):
        for j in range(dofs):
            row = base + j * fields
            flat[i, row : row + fields, :] = ref[j, :, i * LANES : (i + 1) * LANES]
        flat[i, base + used : base + width, :] = jnp.zeros((width - used, LANES), F32)


def lane_gather(blocks, lane, block_id):
    total = jnp.zeros(blocks[0].shape, F32)
    for i, block in enumerate(blocks):
        got = jnp.take_along_axis(block, lane, axis=1)
        total = jnp.where(block_id == i, got, total)
    return total


def one_hot(index, rows):
    parts = []
    for first in range(0, rows, 256):
        count = min(256, rows - first)
        wide = jnp.broadcast_to((index - first).astype(F32), (count, index.shape[1])).astype(BF16)
        ids = lax.broadcasted_iota(jnp.int32, wide.shape, 0).astype(F32).astype(BF16)
        parts.append(jnp.where(wide == ids, jnp.ones_like(wide), jnp.zeros_like(wide)))
    return parts[0] if len(parts) == 1 else jnp.concatenate(parts, 0)


def compute_kernel(dims, n_args, *refs):
    n_gx, n_gy, bits, ghosts, edges, hangs, fields, rows, hang_rows, chunk_lanes = dims
    hbm = refs[:n_args]
    out_ref = refs[n_args]
    local = refs[n_args + 1 : 2 * n_args + 1]
    (
        op_recon,
        op_left,
        op_flux_rows,
        op_face_rows,
        op_child,
        op_child_tight,
        child_flat,
        op_flux,
        op_rep,
        op_z,
        op_u,
        op_trace,
        op_back,
        maps,
        z_hi,
        z_lo,
        u_all,
        sources,
        flat,
        source_flat,
        hang_flat,
        near,
        hot,
        scatter,
        part_z,
        part_x,
        from_gy_u,
        from_gx_u,
        from_gy_z,
        from_gx_z,
        to_gy_u,
        to_gx_u,
        to_gy_z,
        to_gx_z,
        ids,
        packed,
        in_sems,
        send_gy,
        recv_gy,
        send_gx,
        recv_gx,
        ready,
    ) = refs[2 * n_args + 1 :]
    (
        primal_ref,
        adjoint_ref,
        source_ref,
        coef_ref,
        levels_ref,
        recon_ref,
        stiffness_ref,
        interp_ref,
        flux_ref,
        face_eval_ref,
        child_interp_ref,
        slot_ref,
        child_ref,
        hang_ref,
        ghost_ref,
        edge_ref,
        hang_send_ref,
    ) = local
    gx = lax.axis_index("gx")
    gy = lax.axis_index("gy")
    dofs, _, cells = primal_ref.shape
    width = fields * rows
    wide = 2 * width
    partners = [jnp.bitwise_xor(gy, 1 << b) for b in range(bits)]

    bit_of = [gy // (1 << b) % 2 for b in range(bits)]
    barrier = pltpu.get_barrier_semaphore()
    for b, partner in enumerate(partners):

        @pl.when(bit_of[b] == 0)
        def _():
            pl.semaphore_signal(barrier, inc=1, device_id=(gx, partner), device_id_type=MESH)

    @pl.when(gx < n_gx - 1)
    def _():
        pl.semaphore_signal(barrier, inc=1, device_id=(gx + 1, gy), device_id_type=MESH)

    order = [14, 15, 16, 1, 0, 11, 5, 6, 7, 8, 9, 10, 13, 12, 3, 4, 2]
    groups = [0 if i in order[:4] else 1 if i == order[4] else 2 for i in range(n_args)]
    loads = [pltpu.make_async_copy(hbm[i], local[i], in_sems.at[groups[i]]) for i in range(n_args)]
    for i in order[:5]:
        loads[i].start()

    main = bits * ghosts + 2 * edges
    main_pad = round_up(main, LANES)
    hang_pad = round_up(bits * hangs, LANES)
    ids[...] = jnp.zeros_like(ids)
    for i in order[:4]:
        loads[i].wait()
    for i in order[5:]:
        loads[i].start()
    lower = sum(bit_of) + jnp.minimum(gx, 1)

    @pl.when(lower > 0)
    def _():
        pl.semaphore_wait(barrier, lower)

    for b, partner in enumerate(partners):

        @pl.when(bit_of[b] == 1)
        def _():
            pl.semaphore_signal(ready.at[b], inc=1, device_id=(gx, partner), device_id_type=MESH)

    @pl.when(gx > 0)
    def _():
        pl.semaphore_signal(ready.at[bits], inc=1, device_id=(gx - 1, gy), device_id_type=MESH)

    for b, partner in enumerate(partners):
        ids[0:1, b * ghosts : (b + 1) * ghosts] = ghost_ref[0, pl.ds(partner, 1), :]
        at = main_pad + b * hangs
        ids[0:1, at : at + hangs] = hang_send_ref[0, 0, pl.ds(partner, 1), :]
    for side in range(2):
        at = bits * ghosts + side * edges
        ids[0:1, at : at + edges] = edge_ref[0, side : side + 1, :]
    chosen = jnp.maximum(ids[0:1, :], 0)

    def pick(base, at):
        part = jnp.broadcast_to(chosen[:, at : at + LANES], (rows, LANES))
        lane = jnp.bitwise_and(part, LANES - 1)
        block_id = jnp.right_shift(part, 7)
        for k in range(fields):
            span = slice(base + k * rows, base + (k + 1) * rows)
            blocks = [flat[i, span, :] for i in range(cells // LANES)]
            packed[span, :] = lane_gather(blocks, lane, block_id)
        return packed[base : base + width, :].T

    def pack(base, to_gy, to_gx):
        for at in range(0, main_pad, LANES):
            turned = pick(base, at)
            for first in range(at, min(at + LANES, main), edges):
                chunk = turned[first - at : first - at + edges]
                if first < bits * ghosts:
                    to_gy[first // ghosts, pl.ds(first % ghosts, edges), :] = chunk
                else:
                    to_gx[(first - bits * ghosts) // edges] = chunk

    stages = [(to_gy_z, from_gy_z, to_gx_z, from_gx_z), (to_gy_u, from_gy_u, to_gx_u, from_gx_u)]

    def gy_copy(stage, b):
        src, dst, _, _ = stages[stage]
        return pltpu.make_async_remote_copy(
            src_ref=src.at[b],
            dst_ref=dst.at[b],
            send_sem=send_gy.at[stage, b],
            recv_sem=recv_gy.at[stage, b],
            device_id=(gx, partners[b]),
            device_id_type=MESH,
        )

    def low_copy(stage):
        _, _, src, dst = stages[stage]
        return pltpu.make_async_remote_copy(
            src_ref=src.at[0],
            dst_ref=dst.at[1],
            send_sem=send_gx.at[stage, 0],
            recv_sem=recv_gx.at[stage, 1],
            device_id=(gx - 1, gy),
            device_id_type=MESH,
        )

    def high_copy(stage):
        _, _, src, dst = stages[stage]
        return pltpu.make_async_remote_copy(
            src_ref=src.at[1],
            dst_ref=dst.at[0],
            send_sem=send_gx.at[stage, 1],
            recv_sem=recv_gx.at[stage, 0],
            device_id=(gx + 1, gy),
            device_id_type=MESH,
        )

    def send_lower(stage):
        for b in reversed(range(bits)):

            @pl.when(bit_of[b] == 1)
            def _():
                gy_copy(stage, b).start()

        @pl.when(gx > 0)
        def _():
            low_copy(stage).start()

    fill_flat(flat, adjoint_ref, width, width)
    pack(width, to_gy_z, to_gx_z)
    send_lower(0)
    loads[order[4]].wait()
    fill_flat(flat, primal_ref, 0, width)
    pack(0, to_gy_u, to_gx_u)
    for at in range(main_pad, main_pad + hang_pad, LANES):
        turned = pick(0, at)
        for b in range(bits):
            at_slot = b * hangs - (at - main_pad)
            if 0 <= at_slot < LANES:
                to_gy_u[b, ghosts : ghosts + hangs, :] = turned[at_slot : at_slot + hangs]
    send_lower(1)

    @pl.when(gx == 0)
    def _():
        from_gx_z[0] = jnp.zeros(from_gx_z.shape[1:], F32)
        from_gx_u[0] = jnp.zeros(from_gx_u.shape[1:], F32)

    @pl.when(gx == n_gx - 1)
    def _():
        from_gx_z[1] = jnp.zeros(from_gx_z.shape[1:], F32)
        from_gx_u[1] = jnp.zeros(from_gx_u.shape[1:], F32)

    def receive(stage):
        for b in range(bits):
            gy_copy(stage, b).wait()

        @pl.when(gx > 0)
        def _():
            low_copy(stage).wait_send()
            high_copy(stage).wait_recv()

        @pl.when(gx < n_gx - 1)
        def _():
            high_copy(stage).wait_send()
            low_copy(stage).wait_recv()

    quads = recon_ref.shape[2]
    own_blocks = cells // LANES
    points = flux_ref.shape[1]
    remote = bits * ghosts + 2 * edges
    remote_pad = round_up(remote, LANES)
    hang_count = bits * hangs
    children = 4
    tight = points // 8 * 8
    tails = points - tight
    form_rows = op_z.shape[0] // 2
    tail_at = 5 * tight

    for i in order[5:]:
        loads[i].wait()

    for i in range(own_blocks):
        for group in range(2 * fields):
            first = group // fields * width + group % fields
            sources[group * rows : (group + 1) * rows, i * LANES : (i + 1) * LANES] = flat[
                i, pl.ds(first, rows, stride=fields), :
            ]
    slot = slot_ref[...]
    shifted = slot - cells
    log_ghosts = ghosts.bit_length() - 1
    peer = jnp.right_shift(shifted, log_ghosts)
    within = jnp.bitwise_and(shifted, ghosts - 1)
    differing = jnp.bitwise_xor(peer, gy)
    place_of = jnp.zeros_like(slot)
    for b in range(1, bits):
        place_of = jnp.where(differing == (1 << b), b, place_of)
    far = jnp.where(
        shifted < n_gy * ghosts, place_of * ghosts + within, shifted - (n_gy - bits) * ghosts
    )
    far = jnp.where(shifted < 0, -1, far)
    for f in range(FAR_DOT_FACES):
        for at in range(0, chunk_lanes, chunk_lanes):
            cols = slice(at, at + chunk_lanes)
            hot_part = one_hot(far[f : f + 1, cols], remote_pad)
            hot[f, 0:remote_pad, cols] = hot_part
            hot[f, remote_pad : 2 * remote_pad, cols] = hot_part

    op_recon[...] = jnp.zeros_like(op_recon)
    op_left[...] = jnp.zeros_like(op_left)
    op_flux_rows[...] = jnp.zeros_like(op_flux_rows)
    op_face_rows[...] = jnp.zeros_like(op_face_rows)
    op_child_tight[...] = jnp.zeros_like(op_child_tight)
    child_flat[...] = jnp.zeros_like(child_flat)
    op_flux[...] = jnp.zeros_like(op_flux)
    for j in range(dofs):
        op_recon[8 * j : 8 * j + 7, 0:quads] = recon_ref[j]
    op_left[0:dofs, 0:quads] = interp_ref[...]
    op_left[rows : rows + dofs, 0:quads] = stiffness_ref[...]
    for f in range(6):
        at = 3 * rows + f * tight
        op_left[at : at + tight, 0:quads] = face_eval_ref[f, 0:tight, :]
        for e in range(points - tight):
            at = 3 * rows + 6 * tight + 8 * e + f
            op_left[at : at + 1, 0:quads] = face_eval_ref[f, tight + e : tight + e + 1, :]
        op_face_rows[f * rows : f * rows + points, 0:quads] = face_eval_ref[f]
        op_flux_rows[f * rows : f * rows + points, 0:dofs] = flux_ref[f]
        op_flux[0:points, f * rows : f * rows + dofs] = flux_ref[f]
    for p in range(points):
        child_flat[children * p : children * (p + 1), 0:points] = child_interp_ref[p]
    for h in range(children):
        op_child[h * rows : (h + 1) * rows, :] = child_flat[pl.ds(h, rows, stride=children), :]
    flux_turned = op_flux_rows[...].T[0:rows]
    op_left[2 * rows : 3 * rows, :] = dot3(both(flux_turned), *split(op_face_rows[...]))
    recon_turned = jnp.concatenate([op_recon[pl.ds(f, rows, stride=8), :] for f in range(7)], 0)
    op_z[...] = both(dot3(both(op_left[...]), *split(recon_turned), dot=mm_nt))
    for f in range(6):
        single = op_flux_rows[f * rows : (f + 1) * rows, :]
        thrice = single + pltpu.roll(single, rows, 1) + pltpu.roll(single, 2 * rows, 1)
        op_rep[:, (f ^ 1) * LANES : ((f ^ 1) + 1) * LANES] = thrice
    for h in range(children):
        op_child_tight[h * tight : (h + 1) * tight, :] = op_child[h * rows : h * rows + tight, :]
        for e in range(tails):
            at = tail_at + 8 * e + h
            op_child_tight[at : at + 1, :] = op_child[h * rows + tight + e : h * rows + tight + e + 1, :]
    same = (tight, LANES)
    op_child_tight[children * tight : 5 * tight, :] = jnp.where(
        lax.broadcasted_iota(jnp.int32, same, 0) == lax.broadcasted_iota(jnp.int32, same, 1), 1.0, 0.0
    )
    for e in range(tails):
        at = tail_at + 8 * e + children
        op_child_tight[at : at + 1, :] = jnp.where(
            lax.broadcasted_iota(jnp.int32, (1, LANES), 1) == tight + e, 1.0, 0.0
        )
    mapped_ops = dot3(both(op_child_tight[...])[:, 0:rows], *split(op_rep[...]))
    high_lanes = lax.broadcasted_iota(jnp.int32, (op_u.shape[1], LANES), 1) < 2 * rows
    for f in range(6):
        hi, lo = split(mapped_ops[:, f * LANES : (f + 1) * LANES])
        op_u[f] = jnp.where(high_lanes, hi.astype(F32), lo.astype(F32)).astype(BF16)
    op_trace[...] = both(op_flux[...])
    op_back[...] = both(op_child[...].T[0:rows])

    maps[...] = jnp.full(maps.shape, -1, jnp.int32)
    for b in range(bits):
        partner = jnp.bitwise_xor(gy, 1 << b)
        for i in range(3):
            maps[i : i + 1, b * hangs : (b + 1) * hangs] = hang_ref[i, 0, pl.ds(partner, 1), :]

    def spread(x):
        outs = []
        for first in range(0, fields * hang_rows, LANES):
            total = None
            for k in range(fields):
                at = k * hang_rows - first
                if 0 <= at < LANES:
                    piece = x[k][:, 0:LANES]
                    piece = pltpu.roll(piece, at, 1) if at else piece
                    total = piece if total is None else total + piece
            outs.append(total)
        return outs[0] if len(outs) == 1 else jnp.concatenate(outs, 1)

    maps_all = spread([maps[...] + 1] * fields) - 1
    hang_lanes = fields * hang_rows
    face_wide = jnp.broadcast_to(maps_all[1:2, :], (rows, hang_lanes))
    child_wide = jnp.broadcast_to(maps_all[2:3, :], (rows, hang_lanes))
    hang_zero = jnp.zeros((rows, hang_lanes), BF16)
    hang_cells = maps_all[0:1, :]
    for first in range(0, hang_lanes, LANES):
        cell_col = jnp.broadcast_to(hang_cells[:, first : first + LANES].astype(F32), (LANES, LANES)).T
        for at in range(0, cells, LANES):
            column = lax.broadcasted_iota(jnp.int32, (LANES, LANES), 1).astype(F32) + float(at)
            hit = jnp.where(cell_col == column, 1.0, 0.0).astype(BF16)
            scatter[first : first + LANES, at : at + LANES] = hit

    fill_flat(source_flat, source_ref, 0, width)
    for k in range(fields):
        own_hi, own_lo = split(sources[(fields + k) * rows : (fields + k + 1) * rows, :])
        z_hi[k, 0:rows, :] = own_hi
        z_lo[k, 0:rows, :] = own_lo
    coef = coef_ref[...]
    size = jnp.exp2(-levels_ref[...].astype(F32))

    @pl.when(gx < n_gx - 1)
    def _():
        pl.semaphore_wait(ready.at[bits], 1)
        for stage in range(2):
            high_copy(stage).start()

    for b in range(bits):

        @pl.when(bit_of[b] == 0)
        def _():
            pl.semaphore_wait(ready.at[b], 1)
            for stage in range(2):
                gy_copy(stage, b).start()

    own_both = both(sources[...])
    for f in range(DOT_FACES):
        for at in range(0, cells, chunk_lanes):
            cols = slice(at, at + chunk_lanes)
            got = mm(own_both, one_hot(slot[f : f + 1, cols], cells))
            near[f, :, cols] = got[:wide] + got[wide:]
    for f in range(DOT_FACES, 6):
        for at in range(0, cells, LANES):
            cols = slice(at, at + LANES)
            part = jnp.broadcast_to(slot[f : f + 1, cols], (rows, LANES))
            lane = jnp.bitwise_and(part, LANES - 1)
            block_id = jnp.right_shift(part, 7)
            for group in range(2 * fields):
                span = slice(group * rows, (group + 1) * rows)
                blocks = [sources[span, i * LANES : (i + 1) * LANES] for i in range(own_blocks)]
                near[f, span, cols] = lane_gather(blocks, lane, block_id)
    far_lane = jnp.bitwise_and(far, LANES - 1)
    far_block = jnp.right_shift(far, 7)

    def turn(from_gy, from_gx):
        parts = [from_gy[b, 0:ghosts, :] for b in range(bits)] + [from_gx[0], from_gx[1]]
        if remote_pad > remote:
            parts.append(jnp.zeros((remote_pad - remote, width), F32))
        arrived = jnp.concatenate(parts, 0).T
        blocks = []
        for i in range(remote_pad // LANES):
            flat[i, 0:width, :] = arrived[:, i * LANES : (i + 1) * LANES]
            blocks.append(
                jnp.concatenate(
                    [flat[i, pl.ds(k, rows, stride=fields), :] for k in range(fields)], 0
                )
            )
        return blocks

    def far_gather(blocks, base, f, at):
        cols = slice(at, at + LANES)
        lane = jnp.broadcast_to(far_lane[f : f + 1, cols], (rows, LANES))
        block_id = jnp.broadcast_to(far_block[f : f + 1, cols], (rows, LANES))
        outs = []
        for k in range(fields):
            span = slice(base + k * rows, base + (k + 1) * rows)
            total = near[f, span, cols]
            for i, block in enumerate(blocks):
                got = jnp.take_along_axis(block[k * rows : (k + 1) * rows], lane, axis=1)
                total = jnp.where(block_id == i, got, total)
            outs.append(total)
        return jnp.concatenate(outs, 0)

    def put_z(f, cols, total):
        hi, lo = split(total)
        for k in range(fields):
            span = slice(k * rows, (k + 1) * rows)
            z_hi[k, (1 + f) * rows : (2 + f) * rows, cols] = hi[span]
            z_lo[k, (1 + f) * rows : (2 + f) * rows, cols] = lo[span]

    def gather_z(at, dot_faces):
        cols = slice(at, at + chunk_lanes)
        for f in range(dot_faces):
            put_z(f, cols, near[f, width:, cols] + mm(far_both, hot[f, :, cols]))
        for f in range(dot_faces, 6):
            for first in range(at, at + chunk_lanes, LANES):
                put_z(f, slice(first, first + LANES), far_gather(blocks_z, width, f, first))

    def gather_u(at):
        for f in range(6):
            for first in range(at, at + chunk_lanes, LANES):
                cols = slice(first, first + LANES)
                hi, lo = split(far_gather(blocks_u, 0, f, first))
                for k in range(fields):
                    span = slice(k * rows, (k + 1) * rows)
                    u_all[k, f, 0:rows, cols] = hi[span]
                    u_all[k, f, rows : 2 * rows, cols] = lo[span]
                    u_all[k, f, 2 * rows : 3 * rows, cols] = hi[span]

    totals = {at: [None] * fields for at in range(0, cells, chunk_lanes)}

    def forms_of(k, at):
        cols = slice(at, at + chunk_lanes)
        forms = dot3(op_z[...], z_hi[k, :, cols], z_lo[k, :, cols])
        own_u = sources[k * rows : (k + 1) * rows, cols]
        src = jnp.concatenate(
            [
                source_flat[i, pl.ds(k, rows, stride=fields), :]
                for i in range(at // LANES, (at + chunk_lanes) // LANES)
            ],
            1,
        )
        cell_part = src * forms[0:rows] - coef[:, cols] * own_u * forms[rows : 2 * rows]
        cell_sum = jnp.sum(cell_part, axis=0, keepdims=True)
        out_ref[k : k + 1, cols] = size[:, cols] * cell_sum * (1.0 / math.sqrt(quads))
        part_z[k, :, cols] = forms[3 * rows : 3 * rows + 6 * tight]
        part_x[k, 0 : 8 * tails, cols] = forms[3 * rows + 6 * tight : 3 * rows + 6 * tight + 8 * tails]
        own_part = own_u * forms[2 * rows : 3 * rows]
        totals[at][k] = sum(own_part[i : i + 8] for i in range(8, rows, 8)) + own_part[0:8]

    receive(0)
    blocks_z = turn(from_gy_z, from_gx_z)
    halves = [split(block) for block in blocks_z]
    far_both = jnp.concatenate([h[0] for h in halves] + [h[1] for h in halves], 1)
    gather_z(0, FAR_DOT_FACES)
    for k in range(EARLY_FORMS):
        forms_of(k, 0)
    for at in range(chunk_lanes, cells, chunk_lanes):
        gather_z(at, 0)

    receive(1)
    blocks_u = turn(from_gy_u, from_gx_u)
    parts = [from_gy_u[b, ghosts : ghosts + hangs, :] for b in range(bits)]
    parts.append(jnp.zeros((hang_pad - hang_count, width), F32))
    hang_flat[...] = jnp.concatenate(parts, 0).T
    hang_all = spread([hang_flat[pl.ds(k, rows, stride=fields), :] for k in range(fields)])
    hang_hi, hang_lo = [
        jnp.concatenate([jnp.where(face_wide == (f ^ 1), x, hang_zero) for f in range(6)], 0)
        for x in split(hang_all)
    ]

    def hang_traces():
        trace_parts = split(dot3(op_trace[:, 0 : 6 * rows], hang_hi, hang_lo))
        return [
            jnp.concatenate([jnp.where(child_wide == h, x, hang_zero) for h in range(children)], 0)
            for x in trace_parts
        ]

    def hang_terms(lifted):
        sub = lax.broadcasted_iota(jnp.int32, (8, LANES), 0)
        outs = []
        for first in range(0, hang_lanes, LANES):
            span = slice(first, first + LANES)
            safe = jnp.maximum(hang_cells[:, span], 0)
            face = maps_all[1:2, span]
            field = (lax.broadcasted_iota(jnp.int32, (1, LANES), 1) + first) // hang_rows
            live_fields = [k for k in range(fields) if first <= k * hang_rows < first + LANES]

            def weights(ref, count):
                lane = jnp.broadcast_to(jnp.bitwise_and(safe, LANES - 1), (count, LANES))
                block_id = jnp.broadcast_to(jnp.right_shift(safe, 7), (count, LANES))
                total = jnp.zeros((count, LANES), F32)
                for k in live_fields:
                    blocks = [ref[k, 0:count, i * LANES : (i + 1) * LANES] for i in range(own_blocks)]
                    mine = jnp.broadcast_to(field == k, (count, LANES))
                    total = jnp.where(mine, lane_gather(blocks, lane, block_id), total)
                return total

            main_weights = weights(part_z, 6 * tight)
            chosen_weights = jnp.zeros((tight, LANES), F32)
            for f in range(6):
                mine = jnp.broadcast_to(face == f, (tight, LANES))
                chosen_weights = jnp.where(
                    mine, main_weights[f * tight : (f + 1) * tight], chosen_weights
                )
            product = chosen_weights * lifted[0:tight, span]
            total = sum(product[i : i + 8] for i in range(0, tight, 8))
            if tails:
                end_weights = weights(part_x, 8 * tails)
                mine = sub == jnp.broadcast_to(face, (8, LANES))
                for e in range(tails):
                    row = jnp.broadcast_to(lifted[tight + e : tight + e + 1, span], (8, LANES))
                    picked = jnp.where(mine, end_weights[8 * e : 8 * (e + 1)], 0.0)
                    total = total + picked * row
            total = jnp.broadcast_to(jnp.sum(total, axis=0, keepdims=True), (8, LANES))
            outs.append(jnp.where(sub == jnp.broadcast_to(field, (8, LANES)), total, 0.0))
        return both(outs[0] if len(outs) == 1 else jnp.concatenate(outs, 1))


    def face_terms(f, at):
        cols = slice(at, at + chunk_lanes)
        child = jnp.broadcast_to(child_ref[f : f + 1, cols], (tight, chunk_lanes))
        masks = [child == h for h in range(children)]
        end_mask = lax.broadcasted_iota(jnp.int32, (8, chunk_lanes), 0) == child[0:8]
        for k in range(fields):
            jumps = mm(op_u[f, :, 0 : 3 * rows], u_all[k, f, :, cols])
            jump = jumps[children * tight : 5 * tight]
            for h in range(children):
                jump = jnp.where(masks[h], jumps[h * tight : (h + 1) * tight], jump)
            product = jump * part_z[k, f * tight : (f + 1) * tight, cols]
            for i in range(0, tight, 8):
                totals[at][k] = totals[at][k] + product[i : i + 8]
            for e in range(tails):
                block = jumps[tail_at + 8 * e : tail_at + 8 * (e + 1)]
                block = jnp.where(end_mask, block, 0.0)
                row = 8 * e + f
                weight = jnp.broadcast_to(part_x[k, row : row + 1, cols], block.shape)
                totals[at][k] = totals[at][k] + block * weight

    chunks = list(range(0, cells, chunk_lanes))
    for k in range(EARLY_FORMS, fields):
        forms_of(k, 0)
    for n, at in enumerate(chunks):
        gather_u(at)
        if n > 0:
            for k in range(fields):
                forms_of(k, at)
                if n == 1 and k == 1:
                    traces = hang_traces()
        if n == 1:
            lifted = dot3(op_back[...], *traces)
    terms = hang_terms(lifted)
    for at in chunks:
        for f in range(6):
            face_terms(f, at)
            if at == chunks[-1] and f == 2:
                back = mm(terms, scatter[...])
                returned = back[0:8] + back[8:16]
    for at in chunks:
        cols = slice(at, at + chunk_lanes)
        for k in range(fields):
            face_sum = jnp.sum(totals[at][k], axis=0, keepdims=True) + returned[k : k + 1, cols]
            row = fields + k
            out_ref[row : row + 1, cols] = size[:, cols] * face_sum * (1.0 / math.sqrt(6 * points))


def solution(mesh):
    n_gx, n_gy = mesh.shape["gx"], mesh.shape["gy"]
    bits = n_gy.bit_length() - 1

    def shards(
        primal,
        adjoint,
        source,
        coefficient,
        levels,
        recon,
        stiffness,
        interp,
        flux,
        face_eval,
        child_interp,
        ghost_send,
        edge_send,
        neighbor_slot,
        neighbor_child,
        hang_send,
        hang_recv,
    ):
        fields, dofs, cells = primal.shape
        ghosts, edges, hangs = ghost_send.shape[2], edge_send.shape[2], hang_send.shape[3]
        rows = round_up(dofs, 32)
        quads = recon.shape[1]
        quad_rows = round_up(quads, LANES)
        hang_rows = max(32, 1 << (bits * hangs - 1).bit_length())
        chunk = min(cells, 256)
        dims = (n_gx, n_gy, bits, ghosts, edges, hangs, fields, rows, hang_rows, chunk)
        primal, adjoint, source = [x.transpose(1, 0, 2) for x in (primal, adjoint, source)]
        main_pad = round_up(bits * ghosts + 2 * edges, LANES)
        hang_pad = round_up(bits * hangs, LANES)
        wide = 2 * fields * rows
        points = flux.shape[1]
        tight, tails = points // 8 * 8, points % 8
        form_rows = round_up(3 * rows + 6 * tight + 8 * tails, 16)
        map_rows = round_up(5 * tight + 8 * tails, 16)
        args = (
            primal,
            adjoint,
            source,
            coefficient.reshape(1, cells),
            levels.reshape(1, cells),
            recon.transpose(2, 0, 1),
            stiffness.T,
            interp.T,
            flux,
            face_eval,
            child_interp.transpose(1, 0, 2),
            neighbor_slot,
            neighbor_child,
            hang_recv,
            ghost_send,
            edge_send,
            hang_send,
        )
        raw = pl.pallas_call(
            functools.partial(compute_kernel, dims, len(args)),
            out_shape=pltpu.VMEM((2 * fields, cells), F32),
            in_specs=[pl.BlockSpec(memory_space=pltpu.MemorySpace.HBM)] * len(args),
            out_specs=pl.BlockSpec(memory_space=pltpu.VMEM),
            scratch_shapes=[pltpu.VMEM(x.shape, x.dtype) for x in args]
            + [
                pltpu.VMEM((8 * rows, quad_rows), F32),
                pltpu.VMEM((form_rows, quad_rows), F32),
                pltpu.VMEM((6 * rows, LANES), F32),
                pltpu.VMEM((6 * rows, quad_rows), F32),
                pltpu.VMEM((4 * rows, LANES), F32),
                pltpu.VMEM((map_rows, LANES), F32),
                pltpu.VMEM((4 * rows, LANES), F32),
                pltpu.VMEM((rows, round_up(6 * rows, LANES)), F32),
                pltpu.VMEM((rows, 6 * LANES), F32),
                pltpu.VMEM((2 * form_rows, 7 * rows), BF16),
                pltpu.VMEM((6, map_rows, LANES), BF16),
                pltpu.VMEM((2 * rows, round_up(6 * rows, LANES)), BF16),
                pltpu.VMEM((2 * rows, 4 * rows), BF16),
                pltpu.VMEM((8, hang_pad), jnp.int32),
                pltpu.VMEM((fields, 7 * rows, cells), BF16),
                pltpu.VMEM((fields, 7 * rows, cells), BF16),
                pltpu.VMEM((fields, 6, 3 * rows, cells), BF16),
                pltpu.VMEM((wide, cells), F32),
                pltpu.VMEM((max(cells, main_pad) // LANES, wide, LANES), F32),
                pltpu.VMEM((cells // LANES, fields * rows, LANES), F32),
                pltpu.VMEM((fields * rows, hang_pad), F32),
                pltpu.VMEM((6, wide, cells), F32),
                pltpu.VMEM((6, 2 * main_pad, cells), BF16),
                pltpu.VMEM((fields * hang_rows, cells), BF16),
                pltpu.VMEM((fields, 6 * tight, cells), F32),
                pltpu.VMEM((fields, max(8 * tails, 8), cells), F32),
            ]
            + [
                pltpu.VMEM((bits, ghosts + hangs, wide // 2), F32),
                pltpu.VMEM((2, edges, wide // 2), F32),
                pltpu.VMEM((bits, ghosts, wide // 2), F32),
                pltpu.VMEM((2, edges, wide // 2), F32),
            ]
            * 2
            + [
                pltpu.VMEM((8, main_pad + hang_pad), jnp.int32),
                pltpu.VMEM((wide, LANES), F32),
                pltpu.SemaphoreType.DMA((3,)),
                pltpu.SemaphoreType.DMA((2, bits)),
                pltpu.SemaphoreType.DMA((2, bits)),
                pltpu.SemaphoreType.DMA((2, 2)),
                pltpu.SemaphoreType.DMA((2, 2)),
                pltpu.SemaphoreType.REGULAR((bits + 1,)),
            ],
            compiler_params=pltpu.CompilerParams(collective_id=0, has_side_effects=True),
            name="indicators",
        )(*args)
        return raw[:fields], raw[fields:]

    split_all = ("gx", "gy")
    placed = (
        P(None, None, split_all),
        P(None, None, split_all),
        P(None, None, split_all),
        P(split_all),
        P(split_all),
        P(),
        P(),
        P(),
        P(),
        P(),
        P(),
        P(split_all, None, None),
        P(split_all, None, None),
        P(None, split_all),
        P(None, split_all),
        P(None, split_all, None, None),
        P(None, split_all, None, None),
    )
    return jax.shard_map(
        shards,
        mesh=mesh,
        in_specs=placed,
        out_specs=(P(None, split_all), P(None, split_all)),
        check_vma=False,
    )
```

```python
import functools
import math

import jax
import jax.numpy as jnp
from jax import lax
from jax.experimental import pallas as pl
from jax.experimental.pallas import tpu as pltpu
from jax.sharding import PartitionSpec as P

LANES = 128
F32 = jnp.float32
BF16 = jnp.bfloat16
MESH = pl.DeviceIdType.MESH
EARLY_FORMS = 2
DOT_FACES = 4
FAR_DOT_FACES = 3


def round_up(value, unit):
    return -(-value // unit) * unit


def split(x):
    hi = x.astype(BF16)
    lo = (x - hi.astype(F32)).astype(BF16)
    return hi, lo


def both(x):
    return jnp.concatenate(split(x), 0)


def mm(a, b):
    return jnp.dot(a, b, preferred_element_type=F32)


def mm_nt(a, b):
    return lax.dot_general(a, b, (((1,), (1,)), ((), ())), preferred_element_type=F32)


def dot3(a_both, b_hi, b_lo, dot=mm):
    rows = a_both.shape[0] // 2
    first = dot(a_both, b_hi)
    return first[:rows] + first[rows:] + dot(a_both[:rows], b_lo)


def fill_flat(flat, ref, base, width):
    dofs, fields, cells = ref.shape
    used = dofs * fields
    for i in range(cells // LANES):
        for j in range(dofs):
            row = base + j * fields
            flat[i, row : row + fields, :] = ref[j, :, i * LANES : (i + 1) * LANES]
        flat[i, base + used : base + width, :] = jnp.zeros((width - used, LANES), F32)


def lane_gather(blocks, lane, block_id):
    total = jnp.zeros(blocks[0].shape, F32)
    for i, block in enumerate(blocks):
        got = jnp.take_along_axis(block, lane, axis=1)
        total = jnp.where(block_id == i, got, total)
    return total


def one_hot(index, rows):
    parts = []
    for first in range(0, rows, 256):
        count = min(256, rows - first)
        wide = jnp.broadcast_to((index - first).astype(F32), (count, index.shape[1])).astype(BF16)
        ids = lax.broadcasted_iota(jnp.int32, wide.shape, 0).astype(F32).astype(BF16)
        parts.append(jnp.where(wide == ids, jnp.ones_like(wide), jnp.zeros_like(wide)))
    return parts[0] if len(parts) == 1 else jnp.concatenate(parts, 0)


def compute_kernel(dims, n_args, *refs):
    n_gx, n_gy, bits, ghosts, edges, hangs, fields, rows, hang_rows, chunk_lanes = dims
    hbm = refs[:n_args]
    out_ref = refs[n_args]
    local = refs[n_args + 1 : 2 * n_args + 1]
    (
        op_recon,
        op_left,
        op_flux_rows,
        op_face_rows,
        op_child,
        op_child_tight,
        child_flat,
        op_flux,
        op_rep,
        op_near,
        op_own,
        op_u,
        op_trace,
        op_back,
        maps,
        z_near,
        own_forms,
        u_all,
        sources,
        flat,
        source_flat,
        hang_flat,
        near,
        hot,
        scatter,
        part_z,
        part_x,
        from_gy_u,
        from_gx_u,
        from_gy_z,
        from_gx_z,
        to_gy_u,
        to_gx_u,
        to_gy_z,
        to_gx_z,
        ids,
        packed,
        in_sems,
        send_sems,
        recv_sems,
        ready,
    ) = refs[2 * n_args + 1 :]
    (
        primal_ref,
        adjoint_ref,
        source_ref,
        coef_ref,
        levels_ref,
        recon_ref,
        stiffness_ref,
        interp_ref,
        flux_ref,
        face_eval_ref,
        child_interp_ref,
        slot_ref,
        child_ref,
        hang_ref,
        ghost_ref,
        edge_ref,
        hang_send_ref,
    ) = local
    gx = lax.axis_index("gx")
    gy = lax.axis_index("gy")
    dofs, _, cells = primal_ref.shape
    width = fields * rows
    wide = 2 * width
    partners = [jnp.bitwise_xor(gy, 1 << b) for b in range(bits)]

    bit_of = [gy // (1 << b) % 2 for b in range(bits)]
    barrier = pltpu.get_barrier_semaphore()
    for b, partner in enumerate(partners):

        @pl.when(bit_of[b] == 0)
        def _():
            pl.semaphore_signal(barrier, inc=1, device_id=(gx, partner), device_id_type=MESH)

    @pl.when(gx < n_gx - 1)
    def _():
        pl.semaphore_signal(barrier, inc=1, device_id=(gx + 1, gy), device_id_type=MESH)

    order = [14, 15, 16, 1, 0, 11, 5, 6, 7, 8, 9, 10, 13, 12, 3, 4, 2]
    groups = [0 if i in order[:4] else 1 if i == order[4] else 2 for i in range(n_args)]
    loads = [pltpu.make_async_copy(hbm[i], local[i], in_sems.at[groups[i]]) for i in range(n_args)]
    for i in order[:5]:
        loads[i].start()

    main = bits * ghosts + 2 * edges
    main_pad = round_up(main, LANES)
    hang_pad = round_up(bits * hangs, LANES)
    ids[...] = jnp.zeros_like(ids)
    for i in order[:4]:
        loads[i].wait()
    for i in order[5:]:
        loads[i].start()
    lower = sum(bit_of) + jnp.minimum(gx, 1)

    @pl.when(lower > 0)
    def _():
        pl.semaphore_wait(barrier, lower)

    for b, partner in enumerate(partners):

        @pl.when(bit_of[b] == 1)
        def _():
            pl.semaphore_signal(ready.at[b], inc=1, device_id=(gx, partner), device_id_type=MESH)

    @pl.when(gx > 0)
    def _():
        pl.semaphore_signal(ready.at[bits], inc=1, device_id=(gx - 1, gy), device_id_type=MESH)

    for b, partner in enumerate(partners):
        ids[0:1, b * ghosts : (b + 1) * ghosts] = ghost_ref[0, pl.ds(partner, 1), :]
        at = main_pad + b * hangs
        ids[0:1, at : at + hangs] = hang_send_ref[0, 0, pl.ds(partner, 1), :]
    for side in range(2):
        at = bits * ghosts + side * edges
        ids[0:1, at : at + edges] = edge_ref[0, side : side + 1, :]
    chosen = jnp.maximum(ids[0:1, :], 0)

    def pick(base, at):
        part = jnp.broadcast_to(chosen[:, at : at + LANES], (rows, LANES))
        lane = jnp.bitwise_and(part, LANES - 1)
        block_id = jnp.right_shift(part, 7)
        for k in range(fields):
            span = slice(base + k * rows, base + (k + 1) * rows)
            blocks = [flat[i, span, :] for i in range(cells // LANES)]
            packed[span, :] = lane_gather(blocks, lane, block_id)
        return packed[base : base + width, :].T

    def pack(base, to_gy, to_gx):
        for at in range(0, main_pad, LANES):
            turned = pick(base, at)
            for first in range(at, min(at + LANES, main), edges):
                chunk = turned[first - at : first - at + edges]
                if first < bits * ghosts:
                    to_gy[first // ghosts, pl.ds(first % ghosts, edges), :] = chunk
                else:
                    to_gx[(first - bits * ghosts) // edges] = chunk

    stages = [(to_gy_z, from_gy_z, to_gx_z, from_gx_z), (to_gy_u, from_gy_u, to_gx_u, from_gx_u)]

    def gy_copy(stage, b):
        src, dst, _, _ = stages[stage]
        return pltpu.make_async_remote_copy(
            src_ref=src.at[b],
            dst_ref=dst.at[b],
            send_sem=send_sems.at[stage, 0],
            recv_sem=recv_sems.at[stage, 0],
            device_id=(gx, partners[b]),
            device_id_type=MESH,
        )

    def low_copy(stage):
        _, _, src, dst = stages[stage]
        return pltpu.make_async_remote_copy(
            src_ref=src.at[0],
            dst_ref=dst.at[1],
            send_sem=send_sems.at[stage, 1],
            recv_sem=recv_sems.at[stage, 1],
            device_id=(gx - 1, gy),
            device_id_type=MESH,
        )

    def high_copy(stage):
        _, _, src, dst = stages[stage]
        return pltpu.make_async_remote_copy(
            src_ref=src.at[1],
            dst_ref=dst.at[0],
            send_sem=send_sems.at[stage, 1],
            recv_sem=recv_sems.at[stage, 1],
            device_id=(gx + 1, gy),
            device_id_type=MESH,
        )

    def send_lower(stage):
        for b in reversed(range(bits)):

            @pl.when(bit_of[b] == 1)
            def _():
                gy_copy(stage, b).start()

        @pl.when(gx > 0)
        def _():
            low_copy(stage).start()

    fill_flat(flat, adjoint_ref, width, width)
    pack(width, to_gy_z, to_gx_z)
    send_lower(0)
    loads[order[4]].wait()
    fill_flat(flat, primal_ref, 0, width)
    pack(0, to_gy_u, to_gx_u)
    for at in range(main_pad, main_pad + hang_pad, LANES):
        turned = pick(0, at)
        for b in range(bits):
            at_slot = b * hangs - (at - main_pad)
            if 0 <= at_slot < LANES:
                to_gy_u[b, ghosts : ghosts + hangs, :] = turned[at_slot : at_slot + hangs]
    send_lower(1)

    @pl.when(gx == 0)
    def _():
        from_gx_z[0] = jnp.zeros(from_gx_z.shape[1:], F32)
        from_gx_u[0] = jnp.zeros(from_gx_u.shape[1:], F32)

    @pl.when(gx == n_gx - 1)
    def _():
        from_gx_z[1] = jnp.zeros(from_gx_z.shape[1:], F32)
        from_gx_u[1] = jnp.zeros(from_gx_u.shape[1:], F32)

    def wait_all(gy_ref, gx_ref, sems):
        def wait(ref, sem):
            pltpu.make_async_copy(ref, ref, sem).wait()

        wait(gy_ref, sems.at[0])

        @pl.when((gx > 0) & (gx < n_gx - 1))
        def _():
            wait(gx_ref, sems.at[1])

        if n_gx > 1:

            @pl.when((gx == 0) | (gx == n_gx - 1))
            def _():
                wait(gx_ref.at[0], sems.at[1])

    def receive(stage):
        _, dst, _, far_gx = stages[stage]
        wait_all(dst, far_gx, recv_sems.at[stage])

    quads = recon_ref.shape[2]
    own_blocks = cells // LANES
    points = flux_ref.shape[1]
    remote = bits * ghosts + 2 * edges
    remote_pad = round_up(remote, LANES)
    hang_count = bits * hangs
    children = 4
    tight = points // 8 * 8
    tails = points - tight
    dof_tight = dofs // 8 * 8
    form_rows = op_own.shape[0]
    pack_rows = 6 * dof_tight + 24
    cut_row = 256 - pack_rows - pack_rows % 16
    tail_at = 5 * tight

    for i in order[5:]:
        loads[i].wait()

    for i in range(own_blocks):
        for group in range(2 * fields):
            first = group // fields * width + group % fields
            sources[group * rows : (group + 1) * rows, i * LANES : (i + 1) * LANES] = flat[
                i, pl.ds(first, rows, stride=fields), :
            ]
    slot = slot_ref[...]
    shifted = slot - cells
    log_ghosts = ghosts.bit_length() - 1
    peer = jnp.right_shift(shifted, log_ghosts)
    within = jnp.bitwise_and(shifted, ghosts - 1)
    differing = jnp.bitwise_xor(peer, gy)
    place_of = jnp.zeros_like(slot)
    for b in range(1, bits):
        place_of = jnp.where(differing == (1 << b), b, place_of)
    far = jnp.where(
        shifted < n_gy * ghosts, place_of * ghosts + within, shifted - (n_gy - bits) * ghosts
    )
    far = jnp.where(shifted < 0, -1, far)
    for f in range(FAR_DOT_FACES):
        for at in range(0, cells, chunk_lanes):
            cols = slice(at, at + chunk_lanes)
            hot_part = one_hot(far[f : f + 1, cols], remote_pad)
            hot[f, 0:remote_pad, cols] = hot_part
            hot[f, remote_pad : 2 * remote_pad, cols] = hot_part

    def pack_near(piece):
        mains = [piece(f)[0:dof_tight] for f in range(6)]
        ends = [
            piece(f)[dof_tight:rows] + pltpu.roll(piece(f + 1)[dof_tight:rows], 4, 0)
            for f in range(0, 6, 2)
        ]
        return jnp.concatenate(mains + ends, 0)

    op_recon[...] = jnp.zeros_like(op_recon)
    op_left[...] = jnp.zeros_like(op_left)
    op_flux_rows[...] = jnp.zeros_like(op_flux_rows)
    op_face_rows[...] = jnp.zeros_like(op_face_rows)
    op_child_tight[...] = jnp.zeros_like(op_child_tight)
    child_flat[...] = jnp.zeros_like(child_flat)
    op_flux[...] = jnp.zeros_like(op_flux)
    for j in range(dofs):
        op_recon[8 * j : 8 * j + 7, 0:quads] = recon_ref[j]
    op_left[0:dofs, 0:quads] = interp_ref[...]
    op_left[rows : rows + dofs, 0:quads] = stiffness_ref[...]
    for f in range(6):
        at = 3 * rows + f * tight
        op_left[at : at + tight, 0:quads] = face_eval_ref[f, 0:tight, :]
        for e in range(points - tight):
            at = 3 * rows + 6 * tight + 8 * e + f
            op_left[at : at + 1, 0:quads] = face_eval_ref[f, tight + e : tight + e + 1, :]
        op_face_rows[f * rows : f * rows + points, 0:quads] = face_eval_ref[f]
        op_flux_rows[f * rows : f * rows + points, 0:dofs] = flux_ref[f]
        op_flux[0:points, f * rows : f * rows + dofs] = flux_ref[f]
    for p in range(points):
        child_flat[children * p : children * (p + 1), 0:points] = child_interp_ref[p]
    for h in range(children):
        op_child[h * rows : (h + 1) * rows, :] = child_flat[pl.ds(h, rows, stride=children), :]
    flux_turned = op_flux_rows[...].T[0:rows]
    op_left[2 * rows : 3 * rows, :] = dot3(both(flux_turned), *split(op_face_rows[...]))
    turned = [op_recon[pl.ds(f, rows, stride=8), :] for f in range(7)]
    order_near = pack_near(lambda f: turned[1 + f])
    spare = jnp.zeros((256 - pack_rows - cut_row, op_recon.shape[1]), F32)
    order_all = jnp.concatenate(
        [order_near, order_near[0:cut_row], spare, order_near, order_near[cut_row:]]
        + [turned[0]] * 3
        + [jnp.zeros((LANES - 3 * rows, op_recon.shape[1]), F32)],
        0,
    )
    ops_hi, ops_lo = split(dot3(both(op_left[...]), *split(order_all), dot=mm_nt))
    op_near[0] = ops_hi[:, 0:256]
    lane_of = lax.broadcasted_iota(jnp.int32, (form_rows, 256), 1)
    mixed = jnp.where(lane_of < pack_rows, ops_lo[:, 256:512].astype(F32), ops_hi[:, 256:512].astype(F32))
    op_near[1] = mixed.astype(BF16)
    mixed = jnp.where(
        lane_of[:, 0:LANES] < 2 * rows, ops_hi[:, 512:].astype(F32), ops_lo[:, 512:].astype(F32)
    )
    op_own[...] = mixed.astype(BF16)
    for f in range(6):
        single = op_flux_rows[f * rows : (f + 1) * rows, :]
        thrice = single + pltpu.roll(single, rows, 1) + pltpu.roll(single, 2 * rows, 1)
        op_rep[:, (f ^ 1) * LANES : ((f ^ 1) + 1) * LANES] = thrice
    for h in range(children):
        op_child_tight[h * tight : (h + 1) * tight, :] = op_child[h * rows : h * rows + tight, :]
        for e in range(tails):
            at = tail_at + 8 * e + h
            op_child_tight[at : at + 1, :] = op_child[h * rows + tight + e : h * rows + tight + e + 1, :]
    same = (tight, LANES)
    op_child_tight[children * tight : 5 * tight, :] = jnp.where(
        lax.broadcasted_iota(jnp.int32, same, 0) == lax.broadcasted_iota(jnp.int32, same, 1), 1.0, 0.0
    )
    for e in range(tails):
        at = tail_at + 8 * e + children
        op_child_tight[at : at + 1, :] = jnp.where(
            lax.broadcasted_iota(jnp.int32, (1, LANES), 1) == tight + e, 1.0, 0.0
        )
    mapped_ops = dot3(both(op_child_tight[...])[:, 0:rows], *split(op_rep[...]))
    high_lanes = lax.broadcasted_iota(jnp.int32, (op_u.shape[1], LANES), 1) < 2 * rows
    for f in range(6):
        hi, lo = split(mapped_ops[:, f * LANES : (f + 1) * LANES])
        op_u[f] = jnp.where(high_lanes, hi.astype(F32), lo.astype(F32)).astype(BF16)
    op_trace[...] = both(op_flux[...])
    op_back[...] = both(op_child[...].T[0:rows])

    maps[...] = jnp.full(maps.shape, -1, jnp.int32)
    for b in range(bits):
        partner = jnp.bitwise_xor(gy, 1 << b)
        for i in range(3):
            maps[i : i + 1, b * hangs : (b + 1) * hangs] = hang_ref[i, 0, pl.ds(partner, 1), :]

    def spread(x):
        outs = []
        for first in range(0, fields * hang_rows, LANES):
            total = None
            for k in range(fields):
                at = k * hang_rows - first
                if 0 <= at < LANES:
                    piece = x[k][:, 0:LANES]
                    piece = pltpu.roll(piece, at, 1) if at else piece
                    total = piece if total is None else total + piece
            outs.append(total)
        return outs[0] if len(outs) == 1 else jnp.concatenate(outs, 1)

    maps_all = spread([maps[...] + 1] * fields) - 1
    hang_lanes = fields * hang_rows
    face_wide = jnp.broadcast_to(maps_all[1:2, :], (rows, hang_lanes))
    child_wide = jnp.broadcast_to(maps_all[2:3, :], (rows, hang_lanes))
    hang_zero = jnp.zeros((rows, hang_lanes), BF16)
    hang_cells = maps_all[0:1, :]
    for first in range(0, hang_lanes, LANES):
        cell_col = jnp.broadcast_to(hang_cells[:, first : first + LANES].astype(F32), (LANES, LANES)).T
        for at in range(0, cells, LANES):
            column = lax.broadcasted_iota(jnp.int32, (LANES, LANES), 1).astype(F32) + float(at)
            hit = jnp.where(cell_col == column, 1.0, 0.0).astype(BF16)
            scatter[first : first + LANES, at : at + LANES] = hit

    fill_flat(source_flat, source_ref, 0, width)
    coef = coef_ref[...]
    size = jnp.exp2(-levels_ref[...].astype(F32))

    @pl.when(gx < n_gx - 1)
    def _():
        pl.semaphore_wait(ready.at[bits], 1)
        for stage in range(2):
            high_copy(stage).start()

    for b in range(bits):

        @pl.when(bit_of[b] == 0)
        def _():
            pl.semaphore_wait(ready.at[b], 1)
            for stage in range(2):
                gy_copy(stage, b).start()

    own_both = both(sources[...])
    for f in range(DOT_FACES):
        for at in range(0, cells, chunk_lanes):
            cols = slice(at, at + chunk_lanes)
            got = mm(own_both, one_hot(slot[f : f + 1, cols], cells))
            near[f, :, cols] = got[:wide] + got[wide:]
    for f in range(DOT_FACES, 6):
        for at in range(0, cells, LANES):
            cols = slice(at, at + LANES)
            part = jnp.broadcast_to(slot[f : f + 1, cols], (rows, LANES))
            lane = jnp.bitwise_and(part, LANES - 1)
            block_id = jnp.right_shift(part, 7)
            for group in range(2 * fields):
                span = slice(group * rows, (group + 1) * rows)
                blocks = [sources[span, i * LANES : (i + 1) * LANES] for i in range(own_blocks)]
                near[f, span, cols] = lane_gather(blocks, lane, block_id)
    for k in range(fields):
        own_hi, own_lo = split(sources[(fields + k) * rows : (fields + k + 1) * rows, :])
        for at in range(0, cells, chunk_lanes):
            cols = slice(at, at + chunk_lanes)
            thrice = jnp.concatenate([own_hi[:, cols], own_lo[:, cols], own_hi[:, cols]], 0)
            own_forms[k, :, cols] = mm(op_own[:, 0 : 3 * rows], thrice)
    far_lane = jnp.bitwise_and(far, LANES - 1)
    far_block = jnp.right_shift(far, 7)

    def turn(from_gy, from_gx):
        parts = [from_gy[b, 0:ghosts, :] for b in range(bits)] + [from_gx[0], from_gx[1]]
        if remote_pad > remote:
            parts.append(jnp.zeros((remote_pad - remote, width), F32))
        arrived = jnp.concatenate(parts, 0).T
        blocks = []
        for i in range(remote_pad // LANES):
            flat[i, 0:width, :] = arrived[:, i * LANES : (i + 1) * LANES]
            blocks.append(
                jnp.concatenate(
                    [flat[i, pl.ds(k, rows, stride=fields), :] for k in range(fields)], 0
                )
            )
        return blocks

    def far_gather(blocks, base, f, at):
        cols = slice(at, at + LANES)
        lane = jnp.broadcast_to(far_lane[f : f + 1, cols], (rows, LANES))
        block_id = jnp.broadcast_to(far_block[f : f + 1, cols], (rows, LANES))
        outs = []
        for k in range(fields):
            span = slice(base + k * rows, base + (k + 1) * rows)
            total = near[f, span, cols]
            for i, block in enumerate(blocks):
                got = jnp.take_along_axis(block[k * rows : (k + 1) * rows], lane, axis=1)
                total = jnp.where(block_id == i, got, total)
            outs.append(total)
        return jnp.concatenate(outs, 0)

    def put_z(f, cols, total):
        for k in range(fields):
            z_near[k, f * rows : (f + 1) * rows, cols] = total[k * rows : (k + 1) * rows]

    def gather_z(at, dot_faces):
        cols = slice(at, at + chunk_lanes)
        for f in range(dot_faces):
            put_z(f, cols, near[f, width:, cols] + mm(far_both, hot[f, :, cols]))
        for f in range(dot_faces, 6):
            for first in range(at, at + chunk_lanes, LANES):
                put_z(f, slice(first, first + LANES), far_gather(blocks_z, width, f, first))

    def gather_u(at):
        for f in range(6):
            for first in range(at, at + chunk_lanes, LANES):
                cols = slice(first, first + LANES)
                hi, lo = split(far_gather(blocks_u, 0, f, first))
                for k in range(fields):
                    span = slice(k * rows, (k + 1) * rows)
                    u_all[k, f, 0:rows, cols] = hi[span]
                    u_all[k, f, rows : 2 * rows, cols] = lo[span]

    totals = {at: [None] * fields for at in range(0, cells, chunk_lanes)}

    form_lanes = cells

    def forms_of(k, at):
        cols = slice(at, at + form_lanes)
        packed_z = pack_near(lambda f: z_near[k, f * rows : (f + 1) * rows, cols])
        high = packed_z.astype(BF16).astype(F32)
        low = packed_z - high
        fill = jnp.zeros((256 - pack_rows - cut_row, form_lanes), F32)
        first = jnp.concatenate([high, low[0:cut_row], fill], 0).astype(BF16)
        second = jnp.concatenate([high, low[cut_row:]], 0).astype(BF16)
        forms = mm(op_near[0], first) + mm(op_near[1], second) + own_forms[k, :, cols]
        own_u = sources[k * rows : (k + 1) * rows, cols]
        src = jnp.concatenate(
            [
                source_flat[i, pl.ds(k, rows, stride=fields), :]
                for i in range(at // LANES, (at + form_lanes) // LANES)
            ],
            1,
        )
        cell_part = src * forms[0:rows] - coef[:, cols] * own_u * forms[rows : 2 * rows]
        cell_sum = jnp.sum(cell_part, axis=0, keepdims=True)
        out_ref[k : k + 1, cols] = size[:, cols] * cell_sum * (1.0 / math.sqrt(quads))
        part_z[k, :, cols] = forms[3 * rows : 3 * rows + 6 * tight]
        part_x[k, 0 : 8 * tails, cols] = forms[3 * rows + 6 * tight : 3 * rows + 6 * tight + 8 * tails]
        own_part = own_u * forms[2 * rows : 3 * rows]
        own_sum = sum(own_part[i : i + 8] for i in range(8, rows, 8)) + own_part[0:8]
        for first in range(at, at + form_lanes, chunk_lanes):
            totals[first][k] = own_sum[:, first - at : first - at + chunk_lanes]

    for stage in range(2):
        wait_all(stages[stage][0], stages[stage][2], send_sems.at[stage])
    receive(0)
    blocks_z = turn(from_gy_z, from_gx_z)
    halves = [split(block) for block in blocks_z]
    far_both = jnp.concatenate([h[0] for h in halves] + [h[1] for h in halves], 1)
    for at in range(0, cells, chunk_lanes):
        gather_z(at, FAR_DOT_FACES)
    for k in range(EARLY_FORMS):
        forms_of(k, 0)

    receive(1)
    blocks_u = turn(from_gy_u, from_gx_u)
    parts = [from_gy_u[b, ghosts : ghosts + hangs, :] for b in range(bits)]
    parts.append(jnp.zeros((hang_pad - hang_count, width), F32))
    hang_flat[...] = jnp.concatenate(parts, 0).T
    hang_all = spread([hang_flat[pl.ds(k, rows, stride=fields), :] for k in range(fields)])
    hang_hi, hang_lo = [
        jnp.concatenate([jnp.where(face_wide == (f ^ 1), x, hang_zero) for f in range(6)], 0)
        for x in split(hang_all)
    ]

    def hang_traces():
        trace_parts = split(dot3(op_trace[:, 0 : 6 * rows], hang_hi, hang_lo))
        return [
            jnp.concatenate([jnp.where(child_wide == h, x, hang_zero) for h in range(children)], 0)
            for x in trace_parts
        ]

    def hang_terms(lifted):
        sub = lax.broadcasted_iota(jnp.int32, (8, LANES), 0)
        outs = []
        for first in range(0, hang_lanes, LANES):
            span = slice(first, first + LANES)
            safe = jnp.maximum(hang_cells[:, span], 0)
            face = maps_all[1:2, span]
            field = (lax.broadcasted_iota(jnp.int32, (1, LANES), 1) + first) // hang_rows
            live_fields = [k for k in range(fields) if first <= k * hang_rows < first + LANES]

            def weights(ref, count):
                lane = jnp.broadcast_to(jnp.bitwise_and(safe, LANES - 1), (count, LANES))
                block_id = jnp.broadcast_to(jnp.right_shift(safe, 7), (count, LANES))
                total = jnp.zeros((count, LANES), F32)
                for k in live_fields:
                    blocks = [ref[k, 0:count, i * LANES : (i + 1) * LANES] for i in range(own_blocks)]
                    mine = jnp.broadcast_to(field == k, (count, LANES))
                    total = jnp.where(mine, lane_gather(blocks, lane, block_id), total)
                return total

            main_weights = weights(part_z, 6 * tight)
            chosen_weights = jnp.zeros((tight, LANES), F32)
            for f in range(6):
                mine = jnp.broadcast_to(face == f, (tight, LANES))
                chosen_weights = jnp.where(
                    mine, main_weights[f * tight : (f + 1) * tight], chosen_weights
                )
            product = chosen_weights * lifted[0:tight, span]
            total = sum(product[i : i + 8] for i in range(0, tight, 8))
            if tails:
                end_weights = weights(part_x, 8 * tails)
                mine = sub == jnp.broadcast_to(face, (8, LANES))
                for e in range(tails):
                    row = jnp.broadcast_to(lifted[tight + e : tight + e + 1, span], (8, LANES))
                    picked = jnp.where(mine, end_weights[8 * e : 8 * (e + 1)], 0.0)
                    total = total + picked * row
            total = jnp.broadcast_to(jnp.sum(total, axis=0, keepdims=True), (8, LANES))
            outs.append(jnp.where(sub == jnp.broadcast_to(field, (8, LANES)), total, 0.0))
        return both(outs[0] if len(outs) == 1 else jnp.concatenate(outs, 1))


    def face_terms(f, at):
        cols = slice(at, at + chunk_lanes)
        child = jnp.broadcast_to(child_ref[f : f + 1, cols], (tight, chunk_lanes))
        masks = [child == h for h in range(children)]
        end_mask = lax.broadcasted_iota(jnp.int32, (8, chunk_lanes), 0) == child[0:8]
        for k in range(fields):
            pair = u_all[k, f, :, cols]
            jumps = mm(op_u[f, :, 0 : 3 * rows], jnp.concatenate([pair, pair[0:rows]], 0))
            jump = jumps[children * tight : 5 * tight]
            for h in range(children):
                jump = jnp.where(masks[h], jumps[h * tight : (h + 1) * tight], jump)
            product = jump * part_z[k, f * tight : (f + 1) * tight, cols]
            for i in range(0, tight, 8):
                totals[at][k] = totals[at][k] + product[i : i + 8]
            for e in range(tails):
                block = jumps[tail_at + 8 * e : tail_at + 8 * (e + 1)]
                block = jnp.where(end_mask, block, 0.0)
                row = 8 * e + f
                weight = jnp.broadcast_to(part_x[k, row : row + 1, cols], block.shape)
                totals[at][k] = totals[at][k] + block * weight

    chunks = list(range(0, cells, chunk_lanes))
    for k in range(EARLY_FORMS, fields):
        forms_of(k, 0)
        if k == max(EARLY_FORMS, fields - 3):
            traces = hang_traces()
        if k == fields - 1:
            lifted = dot3(op_back[...], *traces)
    for at in chunks:
        gather_u(at)
    terms = hang_terms(lifted)
    for at in chunks:
        for f in range(6):
            face_terms(f, at)
            if at == chunks[-1] and f == 2:
                back = mm(terms, scatter[...])
                returned = back[0:8] + back[8:16]
    for at in chunks:
        cols = slice(at, at + chunk_lanes)
        for k in range(fields):
            face_sum = jnp.sum(totals[at][k], axis=0, keepdims=True) + returned[k : k + 1, cols]
            row = fields + k
            out_ref[row : row + 1, cols] = size[:, cols] * face_sum * (1.0 / math.sqrt(6 * points))


def solution(mesh):
    n_gx, n_gy = mesh.shape["gx"], mesh.shape["gy"]
    bits = n_gy.bit_length() - 1

    def shards(
        primal,
        adjoint,
        source,
        coefficient,
        levels,
        recon,
        stiffness,
        interp,
        flux,
        face_eval,
        child_interp,
        ghost_send,
        edge_send,
        neighbor_slot,
        neighbor_child,
        hang_send,
        hang_recv,
    ):
        fields, dofs, cells = primal.shape
        ghosts, edges, hangs = ghost_send.shape[2], edge_send.shape[2], hang_send.shape[3]
        rows = round_up(dofs, 32)
        quads = recon.shape[1]
        quad_rows = round_up(quads, LANES)
        hang_rows = max(32, 1 << (bits * hangs - 1).bit_length())
        chunk = min(cells, 256)
        dims = (n_gx, n_gy, bits, ghosts, edges, hangs, fields, rows, hang_rows, chunk)
        primal, adjoint, source = [x.transpose(1, 0, 2) for x in (primal, adjoint, source)]
        main_pad = round_up(bits * ghosts + 2 * edges, LANES)
        hang_pad = round_up(bits * hangs, LANES)
        wide = 2 * fields * rows
        points = flux.shape[1]
        tight, tails = points // 8 * 8, points % 8
        form_rows = round_up(3 * rows + 6 * tight + 8 * tails, 16)
        map_rows = round_up(5 * tight + 8 * tails, 16)
        args = (
            primal,
            adjoint,
            source,
            coefficient.reshape(1, cells),
            levels.reshape(1, cells),
            recon.transpose(2, 0, 1),
            stiffness.T,
            interp.T,
            flux,
            face_eval,
            child_interp.transpose(1, 0, 2),
            neighbor_slot,
            neighbor_child,
            hang_recv,
            ghost_send,
            edge_send,
            hang_send,
        )
        raw = pl.pallas_call(
            functools.partial(compute_kernel, dims, len(args)),
            out_shape=pltpu.VMEM((2 * fields, cells), F32),
            in_specs=[pl.BlockSpec(memory_space=pltpu.MemorySpace.HBM)] * len(args),
            out_specs=pl.BlockSpec(memory_space=pltpu.VMEM),
            scratch_shapes=[pltpu.VMEM(x.shape, x.dtype) for x in args]
            + [
                pltpu.VMEM((8 * rows, quad_rows), F32),
                pltpu.VMEM((form_rows, quad_rows), F32),
                pltpu.VMEM((6 * rows, LANES), F32),
                pltpu.VMEM((6 * rows, quad_rows), F32),
                pltpu.VMEM((4 * rows, LANES), F32),
                pltpu.VMEM((map_rows, LANES), F32),
                pltpu.VMEM((4 * rows, LANES), F32),
                pltpu.VMEM((rows, round_up(6 * rows, LANES)), F32),
                pltpu.VMEM((rows, 6 * LANES), F32),
                pltpu.VMEM((2, form_rows, 256), BF16),
                pltpu.VMEM((form_rows, LANES), BF16),
                pltpu.VMEM((6, map_rows, LANES), BF16),
                pltpu.VMEM((2 * rows, round_up(6 * rows, LANES)), BF16),
                pltpu.VMEM((2 * rows, 4 * rows), BF16),
                pltpu.VMEM((8, hang_pad), jnp.int32),
                pltpu.VMEM((fields, 6 * rows, cells), F32),
                pltpu.VMEM((fields, form_rows, cells), F32),
                pltpu.VMEM((fields, 6, 2 * rows, cells), BF16),
                pltpu.VMEM((wide, cells), F32),
                pltpu.VMEM((max(cells, main_pad) // LANES, wide, LANES), F32),
                pltpu.VMEM((cells // LANES, fields * rows, LANES), F32),
                pltpu.VMEM((fields * rows, hang_pad), F32),
                pltpu.VMEM((6, wide, cells), F32),
                pltpu.VMEM((6, 2 * main_pad, cells), BF16),
                pltpu.VMEM((fields * hang_rows, cells), BF16),
                pltpu.VMEM((fields, 6 * tight, cells), F32),
                pltpu.VMEM((fields, max(8 * tails, 8), cells), F32),
            ]
            + [
                pltpu.VMEM((bits, ghosts + hangs, wide // 2), F32),
                pltpu.VMEM((2, edges, wide // 2), F32),
                pltpu.VMEM((bits, ghosts, wide // 2), F32),
                pltpu.VMEM((2, edges, wide // 2), F32),
            ]
            * 2
            + [
                pltpu.VMEM((8, main_pad + hang_pad), jnp.int32),
                pltpu.VMEM((wide, LANES), F32),
                pltpu.SemaphoreType.DMA((3,)),
                pltpu.SemaphoreType.DMA((2, 2)),
                pltpu.SemaphoreType.DMA((2, 2)),
                pltpu.SemaphoreType.REGULAR((bits + 1,)),
            ],
            compiler_params=pltpu.CompilerParams(collective_id=0, has_side_effects=True),
            name="indicators",
        )(*args)
        return raw[:fields], raw[fields:]

    split_all = ("gx", "gy")
    placed = (
        P(None, None, split_all),
        P(None, None, split_all),
        P(None, None, split_all),
        P(split_all),
        P(split_all),
        P(),
        P(),
        P(),
        P(),
        P(),
        P(),
        P(split_all, None, None),
        P(split_all, None, None),
        P(None, split_all),
        P(None, split_all),
        P(None, split_all, None, None),
        P(None, split_all, None, None),
    )
    return jax.shard_map(
        shards,
        mesh=mesh,
        in_specs=placed,
        out_specs=(P(None, split_all), P(None, split_all)),
        check_vma=False,
    )
```

```python
import functools
import math

import jax
import jax.numpy as jnp
from jax import lax
from jax.experimental import pallas as pl
from jax.experimental.pallas import tpu as pltpu
from jax.sharding import PartitionSpec as P

LANES = 128
F32 = jnp.float32
BF16 = jnp.bfloat16
MESH = pl.DeviceIdType.MESH
EARLY_FORMS = 2
DOT_FACES = 4
FAR_DOT_FACES = 3


def round_up(value, unit):
    return -(-value // unit) * unit


def split(x):
    hi = x.astype(BF16)
    lo = (x - hi.astype(F32)).astype(BF16)
    return hi, lo


def both(x):
    return jnp.concatenate(split(x), 0)


def mm(a, b):
    return jnp.dot(a, b, preferred_element_type=F32)


def mm_nt(a, b):
    return lax.dot_general(a, b, (((1,), (1,)), ((), ())), preferred_element_type=F32)


def dot3(a_both, b_hi, b_lo, dot=mm):
    rows = a_both.shape[0] // 2
    first = dot(a_both, b_hi)
    return first[:rows] + first[rows:] + dot(a_both[:rows], b_lo)


def fill_flat(flat, ref, base, width):
    dofs, fields, cells = ref.shape
    used = dofs * fields
    for i in range(cells // LANES):
        for j in range(dofs):
            row = base + j * fields
            flat[i, row : row + fields, :] = ref[j, :, i * LANES : (i + 1) * LANES]
        flat[i, base + used : base + width, :] = jnp.zeros((width - used, LANES), F32)


def lane_gather(blocks, lane, block_id):
    total = jnp.zeros(blocks[0].shape, F32)
    for i, block in enumerate(blocks):
        got = jnp.take_along_axis(block, lane, axis=1)
        total = jnp.where(block_id == i, got, total)
    return total


def one_hot(index, rows):
    parts = []
    for first in range(0, rows, 256):
        count = min(256, rows - first)
        wide = jnp.broadcast_to((index - first).astype(F32), (count, index.shape[1])).astype(BF16)
        ids = lax.broadcasted_iota(jnp.int32, wide.shape, 0).astype(F32).astype(BF16)
        parts.append(jnp.where(wide == ids, jnp.ones_like(wide), jnp.zeros_like(wide)))
    return parts[0] if len(parts) == 1 else jnp.concatenate(parts, 0)


def compute_kernel(dims, n_args, *refs):
    n_gx, n_gy, bits, ghosts, edges, hangs, fields, rows, hang_rows, chunk_lanes = dims
    hbm = refs[:n_args]
    out_ref = refs[n_args]
    local = refs[n_args + 1 : 2 * n_args + 1]
    (
        op_recon,
        op_left,
        op_flux_rows,
        op_face_rows,
        op_child,
        op_child_tight,
        child_flat,
        op_flux,
        op_rep,
        op_near,
        op_own,
        op_u,
        op_trace,
        op_back,
        maps,
        z_near,
        own_forms,
        u_all,
        sources,
        flat,
        source_flat,
        hang_flat,
        near,
        hot,
        scatter,
        part_z,
        part_x,
        from_gy_u,
        from_gx_u,
        from_gy_z,
        from_gx_z,
        to_gy_u,
        to_gx_u,
        to_gy_z,
        to_gx_z,
        ids,
        packed,
        in_sems,
        send_sems,
        recv_sems,
        ready,
    ) = refs[2 * n_args + 1 :]
    (
        primal_ref,
        adjoint_ref,
        source_ref,
        coef_ref,
        levels_ref,
        recon_ref,
        stiffness_ref,
        interp_ref,
        flux_ref,
        face_eval_ref,
        child_interp_ref,
        slot_ref,
        child_ref,
        hang_ref,
        ghost_ref,
        edge_ref,
        hang_send_ref,
    ) = local
    gx = lax.axis_index("gx")
    gy = lax.axis_index("gy")
    dofs, _, cells = primal_ref.shape
    width = fields * rows
    wide = 2 * width
    partners = [jnp.bitwise_xor(gy, 1 << b) for b in range(bits)]

    bit_of = [gy // (1 << b) % 2 for b in range(bits)]
    barrier = pltpu.get_barrier_semaphore()
    for b, partner in enumerate(partners):

        @pl.when(bit_of[b] == 0)
        def _():
            pl.semaphore_signal(barrier, inc=1, device_id=(gx, partner), device_id_type=MESH)

    @pl.when(gx < n_gx - 1)
    def _():
        pl.semaphore_signal(barrier, inc=1, device_id=(gx + 1, gy), device_id_type=MESH)

    order = [14, 15, 16, 1, 0, 11, 5, 6, 7, 8, 9, 10, 13, 12, 3, 4, 2]
    groups = [0 if i in order[:4] else 1 if i == order[4] else 2 for i in range(n_args)]
    loads = [pltpu.make_async_copy(hbm[i], local[i], in_sems.at[groups[i]]) for i in range(n_args)]
    for i in order[:5]:
        loads[i].start()

    main = bits * ghosts + 2 * edges
    main_pad = round_up(main, LANES)
    hang_pad = round_up(bits * hangs, LANES)
    ids[...] = jnp.zeros_like(ids)
    for i in order[:4]:
        loads[i].wait()
    for b, partner in enumerate(partners):
        ids[0:1, b * ghosts : (b + 1) * ghosts] = ghost_ref[0, pl.ds(partner, 1), :]
        at = main_pad + b * hangs
        ids[0:1, at : at + hangs] = hang_send_ref[0, 0, pl.ds(partner, 1), :]
    for side in range(2):
        at = bits * ghosts + side * edges
        ids[0:1, at : at + edges] = edge_ref[0, side : side + 1, :]
    chosen = jnp.maximum(ids[0:1, :], 0)

    def pick(base, at):
        part = jnp.broadcast_to(chosen[:, at : at + LANES], (rows, LANES))
        lane = jnp.bitwise_and(part, LANES - 1)
        block_id = jnp.right_shift(part, 7)
        for k in range(fields):
            span = slice(base + k * rows, base + (k + 1) * rows)
            blocks = [flat[i, span, :] for i in range(cells // LANES)]
            packed[span, :] = lane_gather(blocks, lane, block_id)
        return packed[base : base + width, :].T

    def pack(base, to_gy, to_gx):
        for at in range(0, main_pad, LANES):
            turned = pick(base, at)
            for first in range(at, min(at + LANES, main), edges):
                chunk = turned[first - at : first - at + edges]
                if first < bits * ghosts:
                    to_gy[first // ghosts, pl.ds(first % ghosts, edges), :] = chunk
                else:
                    to_gx[(first - bits * ghosts) // edges] = chunk

    stages = [(to_gy_z, from_gy_z, to_gx_z, from_gx_z), (to_gy_u, from_gy_u, to_gx_u, from_gx_u)]

    def gy_copy(stage, b):
        src, dst, _, _ = stages[stage]
        return pltpu.make_async_remote_copy(
            src_ref=src.at[b],
            dst_ref=dst.at[b],
            send_sem=send_sems.at[stage, 0],
            recv_sem=recv_sems.at[stage, 0],
            device_id=(gx, partners[b]),
            device_id_type=MESH,
        )

    def low_copy(stage):
        _, _, src, dst = stages[stage]
        return pltpu.make_async_remote_copy(
            src_ref=src.at[0],
            dst_ref=dst.at[1],
            send_sem=send_sems.at[stage, 1],
            recv_sem=recv_sems.at[stage, 1],
            device_id=(gx - 1, gy),
            device_id_type=MESH,
        )

    def high_copy(stage):
        _, _, src, dst = stages[stage]
        return pltpu.make_async_remote_copy(
            src_ref=src.at[1],
            dst_ref=dst.at[0],
            send_sem=send_sems.at[stage, 1],
            recv_sem=recv_sems.at[stage, 1],
            device_id=(gx + 1, gy),
            device_id_type=MESH,
        )

    def send_lower(stage):
        for b in reversed(range(bits)):

            @pl.when(bit_of[b] == 1)
            def _():
                gy_copy(stage, b).start()

        @pl.when(gx > 0)
        def _():
            low_copy(stage).start()

    fill_flat(flat, adjoint_ref, width, width)
    pack(width, to_gy_z, to_gx_z)
    lower = sum(bit_of) + jnp.minimum(gx, 1)

    @pl.when(lower > 0)
    def _():
        pl.semaphore_wait(barrier, lower)

    send_lower(0)
    for b, partner in enumerate(partners):

        @pl.when(bit_of[b] == 1)
        def _():
            pl.semaphore_signal(ready.at[b], inc=1, device_id=(gx, partner), device_id_type=MESH)

    @pl.when(gx > 0)
    def _():
        pl.semaphore_signal(ready.at[bits], inc=1, device_id=(gx - 1, gy), device_id_type=MESH)

    for i in order[5:]:
        loads[i].start()
    loads[order[4]].wait()
    fill_flat(flat, primal_ref, 0, width)
    pack(0, to_gy_u, to_gx_u)
    for at in range(main_pad, main_pad + hang_pad, LANES):
        turned = pick(0, at)
        for b in range(bits):
            at_slot = b * hangs - (at - main_pad)
            if 0 <= at_slot < LANES:
                to_gy_u[b, ghosts : ghosts + hangs, :] = turned[at_slot : at_slot + hangs]
    send_lower(1)

    @pl.when(gx == 0)
    def _():
        from_gx_z[0] = jnp.zeros(from_gx_z.shape[1:], F32)
        from_gx_u[0] = jnp.zeros(from_gx_u.shape[1:], F32)

    @pl.when(gx == n_gx - 1)
    def _():
        from_gx_z[1] = jnp.zeros(from_gx_z.shape[1:], F32)
        from_gx_u[1] = jnp.zeros(from_gx_u.shape[1:], F32)

    def wait_all(gy_ref, gx_ref, sems):
        def wait(ref, sem):
            pltpu.make_async_copy(ref, ref, sem).wait()

        wait(gy_ref, sems.at[0])

        @pl.when((gx > 0) & (gx < n_gx - 1))
        def _():
            wait(gx_ref, sems.at[1])

        if n_gx > 1:

            @pl.when((gx == 0) | (gx == n_gx - 1))
            def _():
                wait(gx_ref.at[0], sems.at[1])

    def receive(stage):
        _, dst, _, far_gx = stages[stage]
        wait_all(dst, far_gx, recv_sems.at[stage])

    quads = recon_ref.shape[2]
    own_blocks = cells // LANES
    points = flux_ref.shape[1]
    remote = bits * ghosts + 2 * edges
    remote_pad = round_up(remote, LANES)
    hang_count = bits * hangs
    children = 4
    tight = points // 8 * 8
    tails = points - tight
    dof_tight = dofs // 8 * 8
    form_rows = op_own.shape[0]
    pack_rows = 6 * dof_tight + 24
    cut_row = 256 - pack_rows - pack_rows % 16
    tail_at = 5 * tight

    for i in order[5:]:
        loads[i].wait()

    for i in range(own_blocks):
        for group in range(2 * fields):
            first = group // fields * width + group % fields
            sources[group * rows : (group + 1) * rows, i * LANES : (i + 1) * LANES] = flat[
                i, pl.ds(first, rows, stride=fields), :
            ]
    slot = slot_ref[...]
    shifted = slot - cells
    log_ghosts = ghosts.bit_length() - 1
    peer = jnp.right_shift(shifted, log_ghosts)
    within = jnp.bitwise_and(shifted, ghosts - 1)
    differing = jnp.bitwise_xor(peer, gy)
    place_of = jnp.zeros_like(slot)
    for b in range(1, bits):
        place_of = jnp.where(differing == (1 << b), b, place_of)
    far = jnp.where(
        shifted < n_gy * ghosts, place_of * ghosts + within, shifted - (n_gy - bits) * ghosts
    )
    far = jnp.where(shifted < 0, -1, far)
    for f in range(FAR_DOT_FACES):
        for at in range(0, cells, chunk_lanes):
            cols = slice(at, at + chunk_lanes)
            hot_part = one_hot(far[f : f + 1, cols], remote_pad)
            hot[f, 0:remote_pad, cols] = hot_part
            hot[f, remote_pad : 2 * remote_pad, cols] = hot_part

    def pack_near(piece):
        mains = [piece(f)[0:dof_tight] for f in range(6)]
        ends = [
            piece(f)[dof_tight:rows] + pltpu.roll(piece(f + 1)[dof_tight:rows], 4, 0)
            for f in range(0, 6, 2)
        ]
        return jnp.concatenate(mains + ends, 0)

    op_recon[...] = jnp.zeros_like(op_recon)
    op_left[...] = jnp.zeros_like(op_left)
    op_flux_rows[...] = jnp.zeros_like(op_flux_rows)
    op_face_rows[...] = jnp.zeros_like(op_face_rows)
    op_child_tight[...] = jnp.zeros_like(op_child_tight)
    child_flat[...] = jnp.zeros_like(child_flat)
    op_flux[...] = jnp.zeros_like(op_flux)
    for j in range(dofs):
        op_recon[8 * j : 8 * j + 7, 0:quads] = recon_ref[j]
    op_left[0:dofs, 0:quads] = interp_ref[...]
    op_left[rows : rows + dofs, 0:quads] = stiffness_ref[...]
    for f in range(6):
        at = 3 * rows + f * tight
        op_left[at : at + tight, 0:quads] = face_eval_ref[f, 0:tight, :]
        for e in range(points - tight):
            at = 3 * rows + 6 * tight + 8 * e + f
            op_left[at : at + 1, 0:quads] = face_eval_ref[f, tight + e : tight + e + 1, :]
        op_face_rows[f * rows : f * rows + points, 0:quads] = face_eval_ref[f]
        op_flux_rows[f * rows : f * rows + points, 0:dofs] = flux_ref[f]
        op_flux[0:points, f * rows : f * rows + dofs] = flux_ref[f]
    for p in range(points):
        child_flat[children * p : children * (p + 1), 0:points] = child_interp_ref[p]
    for h in range(children):
        op_child[h * rows : (h + 1) * rows, :] = child_flat[pl.ds(h, rows, stride=children), :]
    flux_turned = op_flux_rows[...].T[0:rows]
    op_left[2 * rows : 3 * rows, :] = dot3(both(flux_turned), *split(op_face_rows[...]))
    turned = [op_recon[pl.ds(f, rows, stride=8), :] for f in range(7)]
    order_near = pack_near(lambda f: turned[1 + f])
    spare = jnp.zeros((256 - pack_rows - cut_row, op_recon.shape[1]), F32)
    order_all = jnp.concatenate(
        [order_near, order_near[0:cut_row], spare, order_near, order_near[cut_row:]]
        + [turned[0]] * 3
        + [jnp.zeros((LANES - 3 * rows, op_recon.shape[1]), F32)],
        0,
    )
    ops_hi, ops_lo = split(dot3(both(op_left[...]), *split(order_all), dot=mm_nt))
    op_near[0] = ops_hi[:, 0:256]
    lane_of = lax.broadcasted_iota(jnp.int32, (form_rows, 256), 1)
    mixed = jnp.where(lane_of < pack_rows, ops_lo[:, 256:512].astype(F32), ops_hi[:, 256:512].astype(F32))
    op_near[1] = mixed.astype(BF16)
    mixed = jnp.where(
        lane_of[:, 0:LANES] < 2 * rows, ops_hi[:, 512:].astype(F32), ops_lo[:, 512:].astype(F32)
    )
    op_own[...] = mixed.astype(BF16)
    for f in range(6):
        single = op_flux_rows[f * rows : (f + 1) * rows, :]
        thrice = single + pltpu.roll(single, rows, 1) + pltpu.roll(single, 2 * rows, 1)
        op_rep[:, (f ^ 1) * LANES : ((f ^ 1) + 1) * LANES] = thrice
    for h in range(children):
        op_child_tight[h * tight : (h + 1) * tight, :] = op_child[h * rows : h * rows + tight, :]
        for e in range(tails):
            at = tail_at + 8 * e + h
            op_child_tight[at : at + 1, :] = op_child[h * rows + tight + e : h * rows + tight + e + 1, :]
    same = (tight, LANES)
    op_child_tight[children * tight : 5 * tight, :] = jnp.where(
        lax.broadcasted_iota(jnp.int32, same, 0) == lax.broadcasted_iota(jnp.int32, same, 1), 1.0, 0.0
    )
    for e in range(tails):
        at = tail_at + 8 * e + children
        op_child_tight[at : at + 1, :] = jnp.where(
            lax.broadcasted_iota(jnp.int32, (1, LANES), 1) == tight + e, 1.0, 0.0
        )
    mapped_ops = dot3(both(op_child_tight[...])[:, 0:rows], *split(op_rep[...]))
    high_lanes = lax.broadcasted_iota(jnp.int32, (op_u.shape[1], LANES), 1) < 2 * rows
    for f in range(6):
        hi, lo = split(mapped_ops[:, f * LANES : (f + 1) * LANES])
        op_u[f] = jnp.where(high_lanes, hi.astype(F32), lo.astype(F32)).astype(BF16)
    op_trace[...] = both(op_flux[...])
    op_back[...] = both(op_child[...].T[0:rows])

    maps[...] = jnp.full(maps.shape, -1, jnp.int32)
    for b in range(bits):
        partner = jnp.bitwise_xor(gy, 1 << b)
        for i in range(3):
            maps[i : i + 1, b * hangs : (b + 1) * hangs] = hang_ref[i, 0, pl.ds(partner, 1), :]

    def spread(x):
        outs = []
        for first in range(0, fields * hang_rows, LANES):
            total = None
            for k in range(fields):
                at = k * hang_rows - first
                if 0 <= at < LANES:
                    piece = x[k][:, 0:LANES]
                    piece = pltpu.roll(piece, at, 1) if at else piece
                    total = piece if total is None else total + piece
            outs.append(total)
        return outs[0] if len(outs) == 1 else jnp.concatenate(outs, 1)

    maps_all = spread([maps[...] + 1] * fields) - 1
    hang_lanes = fields * hang_rows
    face_wide = jnp.broadcast_to(maps_all[1:2, :], (rows, hang_lanes))
    child_wide = jnp.broadcast_to(maps_all[2:3, :], (rows, hang_lanes))
    hang_zero = jnp.zeros((rows, hang_lanes), BF16)
    hang_cells = maps_all[0:1, :]
    for first in range(0, hang_lanes, LANES):
        cell_col = jnp.broadcast_to(hang_cells[:, first : first + LANES].astype(F32), (LANES, LANES)).T
        for at in range(0, cells, LANES):
            column = lax.broadcasted_iota(jnp.int32, (LANES, LANES), 1).astype(F32) + float(at)
            hit = jnp.where(cell_col == column, 1.0, 0.0).astype(BF16)
            scatter[first : first + LANES, at : at + LANES] = hit

    fill_flat(source_flat, source_ref, 0, width)
    coef = coef_ref[...]
    size = jnp.exp2(-levels_ref[...].astype(F32))

    @pl.when(gx < n_gx - 1)
    def _():
        pl.semaphore_wait(ready.at[bits], 1)
        for stage in range(2):
            high_copy(stage).start()

    for b in range(bits):

        @pl.when(bit_of[b] == 0)
        def _():
            pl.semaphore_wait(ready.at[b], 1)
            for stage in range(2):
                gy_copy(stage, b).start()

    own_both = both(sources[...])
    for f in range(DOT_FACES):
        for at in range(0, cells, chunk_lanes):
            cols = slice(at, at + chunk_lanes)
            got = mm(own_both, one_hot(slot[f : f + 1, cols], cells))
            near[f, :, cols] = got[:wide] + got[wide:]
    for f in range(DOT_FACES, 6):
        for at in range(0, cells, LANES):
            cols = slice(at, at + LANES)
            part = jnp.broadcast_to(slot[f : f + 1, cols], (rows, LANES))
            lane = jnp.bitwise_and(part, LANES - 1)
            block_id = jnp.right_shift(part, 7)
            for group in range(2 * fields):
                span = slice(group * rows, (group + 1) * rows)
                blocks = [sources[span, i * LANES : (i + 1) * LANES] for i in range(own_blocks)]
                near[f, span, cols] = lane_gather(blocks, lane, block_id)
    for k in range(fields):
        own_hi, own_lo = split(sources[(fields + k) * rows : (fields + k + 1) * rows, :])
        for at in range(0, cells, chunk_lanes):
            cols = slice(at, at + chunk_lanes)
            thrice = jnp.concatenate([own_hi[:, cols], own_lo[:, cols], own_hi[:, cols]], 0)
            own_forms[k, :, cols] = mm(op_own[:, 0 : 3 * rows], thrice)
    far_lane = jnp.bitwise_and(far, LANES - 1)
    far_block = jnp.right_shift(far, 7)

    def turn(from_gy, from_gx):
        parts = [from_gy[b, 0:ghosts, :] for b in range(bits)] + [from_gx[0], from_gx[1]]
        if remote_pad > remote:
            parts.append(jnp.zeros((remote_pad - remote, width), F32))
        arrived = jnp.concatenate(parts, 0).T
        blocks = []
        for i in range(remote_pad // LANES):
            flat[i, 0:width, :] = arrived[:, i * LANES : (i + 1) * LANES]
            blocks.append(
                jnp.concatenate(
                    [flat[i, pl.ds(k, rows, stride=fields), :] for k in range(fields)], 0
                )
            )
        return blocks

    def far_gather(blocks, base, f, at):
        cols = slice(at, at + LANES)
        lane = jnp.broadcast_to(far_lane[f : f + 1, cols], (rows, LANES))
        block_id = jnp.broadcast_to(far_block[f : f + 1, cols], (rows, LANES))
        outs = []
        for k in range(fields):
            span = slice(base + k * rows, base + (k + 1) * rows)
            total = near[f, span, cols]
            for i, block in enumerate(blocks):
                got = jnp.take_along_axis(block[k * rows : (k + 1) * rows], lane, axis=1)
                total = jnp.where(block_id == i, got, total)
            outs.append(total)
        return jnp.concatenate(outs, 0)

    def put_z(f, cols, total):
        for k in range(fields):
            z_near[k, f * rows : (f + 1) * rows, cols] = total[k * rows : (k + 1) * rows]

    def gather_z(at, dot_faces):
        cols = slice(at, at + chunk_lanes)
        for f in range(dot_faces):
            put_z(f, cols, near[f, width:, cols] + mm(far_both, hot[f, :, cols]))
        for f in range(dot_faces, 6):
            for first in range(at, at + chunk_lanes, LANES):
                put_z(f, slice(first, first + LANES), far_gather(blocks_z, width, f, first))

    def gather_u(at):
        for f in range(6):
            for first in range(at, at + chunk_lanes, LANES):
                cols = slice(first, first + LANES)
                hi, lo = split(far_gather(blocks_u, 0, f, first))
                for k in range(fields):
                    span = slice(k * rows, (k + 1) * rows)
                    u_all[k, f, 0:rows, cols] = hi[span]
                    u_all[k, f, rows : 2 * rows, cols] = lo[span]

    totals = {at: [None] * fields for at in range(0, cells, chunk_lanes)}

    form_lanes = cells

    def forms_of(k, at):
        cols = slice(at, at + form_lanes)
        packed_z = pack_near(lambda f: z_near[k, f * rows : (f + 1) * rows, cols])
        high = packed_z.astype(BF16).astype(F32)
        low = packed_z - high
        fill = jnp.zeros((256 - pack_rows - cut_row, form_lanes), F32)
        first = jnp.concatenate([high, low[0:cut_row], fill], 0).astype(BF16)
        second = jnp.concatenate([high, low[cut_row:]], 0).astype(BF16)
        forms = mm(op_near[0], first) + mm(op_near[1], second) + own_forms[k, :, cols]
        own_u = sources[k * rows : (k + 1) * rows, cols]
        src = jnp.concatenate(
            [
                source_flat[i, pl.ds(k, rows, stride=fields), :]
                for i in range(at // LANES, (at + form_lanes) // LANES)
            ],
            1,
        )
        cell_part = src * forms[0:rows] - coef[:, cols] * own_u * forms[rows : 2 * rows]
        cell_sum = jnp.sum(cell_part, axis=0, keepdims=True)
        out_ref[k : k + 1, cols] = size[:, cols] * cell_sum * (1.0 / math.sqrt(quads))
        part_z[k, :, cols] = forms[3 * rows : 3 * rows + 6 * tight]
        part_x[k, 0 : 8 * tails, cols] = forms[3 * rows + 6 * tight : 3 * rows + 6 * tight + 8 * tails]
        own_part = own_u * forms[2 * rows : 3 * rows]
        own_sum = sum(own_part[i : i + 8] for i in range(8, rows, 8)) + own_part[0:8]
        for first in range(at, at + form_lanes, chunk_lanes):
            totals[first][k] = own_sum[:, first - at : first - at + chunk_lanes]

    for stage in range(2):
        wait_all(stages[stage][0], stages[stage][2], send_sems.at[stage])
    receive(0)
    blocks_z = turn(from_gy_z, from_gx_z)
    halves = [split(block) for block in blocks_z]
    far_both = jnp.concatenate([h[0] for h in halves] + [h[1] for h in halves], 1)
    for at in range(0, cells, chunk_lanes):
        gather_z(at, FAR_DOT_FACES)
    for k in range(EARLY_FORMS):
        forms_of(k, 0)

    receive(1)
    blocks_u = turn(from_gy_u, from_gx_u)
    parts = [from_gy_u[b, ghosts : ghosts + hangs, :] for b in range(bits)]
    parts.append(jnp.zeros((hang_pad - hang_count, width), F32))
    hang_flat[...] = jnp.concatenate(parts, 0).T
    hang_all = spread([hang_flat[pl.ds(k, rows, stride=fields), :] for k in range(fields)])
    hang_hi, hang_lo = [
        jnp.concatenate([jnp.where(face_wide == (f ^ 1), x, hang_zero) for f in range(6)], 0)
        for x in split(hang_all)
    ]

    def hang_traces():
        trace_parts = split(dot3(op_trace[:, 0 : 6 * rows], hang_hi, hang_lo))
        return [
            jnp.concatenate([jnp.where(child_wide == h, x, hang_zero) for h in range(children)], 0)
            for x in trace_parts
        ]

    def hang_terms(lifted):
        sub = lax.broadcasted_iota(jnp.int32, (8, LANES), 0)
        outs = []
        for first in range(0, hang_lanes, LANES):
            span = slice(first, first + LANES)
            safe = jnp.maximum(hang_cells[:, span], 0)
            face = maps_all[1:2, span]
            field = (lax.broadcasted_iota(jnp.int32, (1, LANES), 1) + first) // hang_rows
            live_fields = [k for k in range(fields) if first <= k * hang_rows < first + LANES]

            def weights(ref, count):
                lane = jnp.broadcast_to(jnp.bitwise_and(safe, LANES - 1), (count, LANES))
                block_id = jnp.broadcast_to(jnp.right_shift(safe, 7), (count, LANES))
                total = jnp.zeros((count, LANES), F32)
                for k in live_fields:
                    blocks = [ref[k, 0:count, i * LANES : (i + 1) * LANES] for i in range(own_blocks)]
                    mine = jnp.broadcast_to(field == k, (count, LANES))
                    total = jnp.where(mine, lane_gather(blocks, lane, block_id), total)
                return total

            main_weights = weights(part_z, 6 * tight)
            chosen_weights = jnp.zeros((tight, LANES), F32)
            for f in range(6):
                mine = jnp.broadcast_to(face == f, (tight, LANES))
                chosen_weights = jnp.where(
                    mine, main_weights[f * tight : (f + 1) * tight], chosen_weights
                )
            product = chosen_weights * lifted[0:tight, span]
            total = sum(product[i : i + 8] for i in range(0, tight, 8))
            if tails:
                end_weights = weights(part_x, 8 * tails)
                mine = sub == jnp.broadcast_to(face, (8, LANES))
                for e in range(tails):
                    row = jnp.broadcast_to(lifted[tight + e : tight + e + 1, span], (8, LANES))
                    picked = jnp.where(mine, end_weights[8 * e : 8 * (e + 1)], 0.0)
                    total = total + picked * row
            total = jnp.broadcast_to(jnp.sum(total, axis=0, keepdims=True), (8, LANES))
            outs.append(jnp.where(sub == jnp.broadcast_to(field, (8, LANES)), total, 0.0))
        return both(outs[0] if len(outs) == 1 else jnp.concatenate(outs, 1))


    def face_terms(f, at):
        cols = slice(at, at + chunk_lanes)
        child = jnp.broadcast_to(child_ref[f : f + 1, cols], (tight, chunk_lanes))
        masks = [child == h for h in range(children)]
        end_mask = lax.broadcasted_iota(jnp.int32, (8, chunk_lanes), 0) == child[0:8]
        for k in range(fields):
            pair = u_all[k, f, :, cols]
            jumps = mm(op_u[f, :, 0 : 3 * rows], jnp.concatenate([pair, pair[0:rows]], 0))
            jump = jumps[children * tight : 5 * tight]
            for h in range(children):
                jump = jnp.where(masks[h], jumps[h * tight : (h + 1) * tight], jump)
            product = jump * part_z[k, f * tight : (f + 1) * tight, cols]
            for i in range(0, tight, 8):
                totals[at][k] = totals[at][k] + product[i : i + 8]
            for e in range(tails):
                block = jumps[tail_at + 8 * e : tail_at + 8 * (e + 1)]
                block = jnp.where(end_mask, block, 0.0)
                row = 8 * e + f
                weight = jnp.broadcast_to(part_x[k, row : row + 1, cols], block.shape)
                totals[at][k] = totals[at][k] + block * weight

    chunks = list(range(0, cells, chunk_lanes))
    for k in range(EARLY_FORMS, fields):
        forms_of(k, 0)
        if k == max(EARLY_FORMS, fields - 3):
            traces = hang_traces()
        if k == fields - 1:
            lifted = dot3(op_back[...], *traces)
    for at in chunks:
        gather_u(at)
    for at in chunks:
        for f in range(6):
            face_terms(f, at)
            if at == chunks[0] and f == 3:
                terms = hang_terms(lifted)
            if at == chunks[-1] and f == 4:
                back = mm(terms, scatter[...])
                returned = back[0:8] + back[8:16]
    for at in chunks:
        cols = slice(at, at + chunk_lanes)
        for k in range(fields):
            face_sum = jnp.sum(totals[at][k], axis=0, keepdims=True) + returned[k : k + 1, cols]
            row = fields + k
            out_ref[row : row + 1, cols] = size[:, cols] * face_sum * (1.0 / math.sqrt(6 * points))


def solution(mesh):
    n_gx, n_gy = mesh.shape["gx"], mesh.shape["gy"]
    bits = n_gy.bit_length() - 1

    def shards(
        primal,
        adjoint,
        source,
        coefficient,
        levels,
        recon,
        stiffness,
        interp,
        flux,
        face_eval,
        child_interp,
        ghost_send,
        edge_send,
        neighbor_slot,
        neighbor_child,
        hang_send,
        hang_recv,
    ):
        fields, dofs, cells = primal.shape
        ghosts, edges, hangs = ghost_send.shape[2], edge_send.shape[2], hang_send.shape[3]
        rows = round_up(dofs, 32)
        quads = recon.shape[1]
        quad_rows = round_up(quads, LANES)
        hang_rows = max(32, 1 << (bits * hangs - 1).bit_length())
        chunk = min(cells, 256)
        dims = (n_gx, n_gy, bits, ghosts, edges, hangs, fields, rows, hang_rows, chunk)
        primal, adjoint, source = [x.transpose(1, 0, 2) for x in (primal, adjoint, source)]
        main_pad = round_up(bits * ghosts + 2 * edges, LANES)
        hang_pad = round_up(bits * hangs, LANES)
        wide = 2 * fields * rows
        points = flux.shape[1]
        tight, tails = points // 8 * 8, points % 8
        form_rows = round_up(3 * rows + 6 * tight + 8 * tails, 16)
        map_rows = round_up(5 * tight + 8 * tails, 16)
        args = (
            primal,
            adjoint,
            source,
            coefficient.reshape(1, cells),
            levels.reshape(1, cells),
            recon.transpose(2, 0, 1),
            stiffness.T,
            interp.T,
            flux,
            face_eval,
            child_interp.transpose(1, 0, 2),
            neighbor_slot,
            neighbor_child,
            hang_recv,
            ghost_send,
            edge_send,
            hang_send,
        )
        raw = pl.pallas_call(
            functools.partial(compute_kernel, dims, len(args)),
            out_shape=pltpu.VMEM((2 * fields, cells), F32),
            in_specs=[pl.BlockSpec(memory_space=pltpu.MemorySpace.HBM)] * len(args),
            out_specs=pl.BlockSpec(memory_space=pltpu.VMEM),
            scratch_shapes=[pltpu.VMEM(x.shape, x.dtype) for x in args]
            + [
                pltpu.VMEM((8 * rows, quad_rows), F32),
                pltpu.VMEM((form_rows, quad_rows), F32),
                pltpu.VMEM((6 * rows, LANES), F32),
                pltpu.VMEM((6 * rows, quad_rows), F32),
                pltpu.VMEM((4 * rows, LANES), F32),
                pltpu.VMEM((map_rows, LANES), F32),
                pltpu.VMEM((4 * rows, LANES), F32),
                pltpu.VMEM((rows, round_up(6 * rows, LANES)), F32),
                pltpu.VMEM((rows, 6 * LANES), F32),
                pltpu.VMEM((2, form_rows, 256), BF16),
                pltpu.VMEM((form_rows, LANES), BF16),
                pltpu.VMEM((6, map_rows, LANES), BF16),
                pltpu.VMEM((2 * rows, round_up(6 * rows, LANES)), BF16),
                pltpu.VMEM((2 * rows, 4 * rows), BF16),
                pltpu.VMEM((8, hang_pad), jnp.int32),
                pltpu.VMEM((fields, 6 * rows, cells), F32),
                pltpu.VMEM((fields, form_rows, cells), F32),
                pltpu.VMEM((fields, 6, 2 * rows, cells), BF16),
                pltpu.VMEM((wide, cells), F32),
                pltpu.VMEM((max(cells, main_pad) // LANES, wide, LANES), F32),
                pltpu.VMEM((cells // LANES, fields * rows, LANES), F32),
                pltpu.VMEM((fields * rows, hang_pad), F32),
                pltpu.VMEM((6, wide, cells), F32),
                pltpu.VMEM((6, 2 * main_pad, cells), BF16),
                pltpu.VMEM((fields * hang_rows, cells), BF16),
                pltpu.VMEM((fields, 6 * tight, cells), F32),
                pltpu.VMEM((fields, max(8 * tails, 8), cells), F32),
            ]
            + [
                pltpu.VMEM((bits, ghosts + hangs, wide // 2), F32),
                pltpu.VMEM((2, edges, wide // 2), F32),
                pltpu.VMEM((bits, ghosts, wide // 2), F32),
                pltpu.VMEM((2, edges, wide // 2), F32),
            ]
            * 2
            + [
                pltpu.VMEM((8, main_pad + hang_pad), jnp.int32),
                pltpu.VMEM((wide, LANES), F32),
                pltpu.SemaphoreType.DMA((3,)),
                pltpu.SemaphoreType.DMA((2, 2)),
                pltpu.SemaphoreType.DMA((2, 2)),
                pltpu.SemaphoreType.REGULAR((bits + 1,)),
            ],
            compiler_params=pltpu.CompilerParams(collective_id=0, has_side_effects=True),
            name="indicators",
        )(*args)
        return raw[:fields], raw[fields:]

    split_all = ("gx", "gy")
    placed = (
        P(None, None, split_all),
        P(None, None, split_all),
        P(None, None, split_all),
        P(split_all),
        P(split_all),
        P(),
        P(),
        P(),
        P(),
        P(),
        P(),
        P(split_all, None, None),
        P(split_all, None, None),
        P(None, split_all),
        P(None, split_all),
        P(None, split_all, None, None),
        P(None, split_all, None, None),
    )
    return jax.shard_map(
        shards,
        mesh=mesh,
        in_specs=placed,
        out_specs=(P(None, split_all), P(None, split_all)),
        check_vma=False,
    )
```
